8 devices in a mesh: inst: 1 (over z), qy: 2 (over y), qx: 4 (over x, core).
Axes of the slice: x: 2, y: 2, z: 1, core: 2. Of those that a mesh axis runs over, the one named last changes fastest.
Arguments:
- cost_diag: float32 [2097152], P(('inst', 'qx', 'qy'))
- gammas: float32 [2], replicated
- betas: float32 [2], replicated
Outputs:
- output 1: float32 [1], P('inst')
- output 2: float32 [2097152], P(('inst', 'qx', 'qy'))
- output 3: float32 [2097152], P(('inst', 'qx', 'qy'))
All inputs are finite; a program needn't handle non-finite values.
Results may differ from the reference program's by a relative error of at most 0.001.
Values sent between devices are 32-bit elements.
A program may use at most 1 GiB of HBM per device.

```python
import math
import jax
import jax.numpy as jnp
from jax import lax

STATE = 2097152
LAYERS = 2
DEGREE = 2

QUBITS = int(math.log2(STATE))
EDGES = DEGREE * QUBITS // 2


def setup_inputs(seed: int = 0, part: int = 0) -> dict:
    base_key = jax.random.key(seed)
    part_key = jax.random.fold_in(base_key, part)
    key_offset, key_weight = jax.random.split(part_key)
    first_node = jnp.arange(EDGES, dtype=jnp.int32) % QUBITS
    offsets = jax.random.randint(key_offset, (EDGES,), 1, QUBITS, dtype=jnp.int32)
    second_node = (first_node + offsets) % QUBITS
    weights = jax.random.uniform(key_weight, (EDGES,), jnp.float32, 0.5, 1.5) * (2.0 / math.sqrt(EDGES))
    basis_index = jnp.arange(STATE, dtype=jnp.int32)

    def add_edge(edge_id, cost_acc):
        cut_bit = ((basis_index >> first_node[edge_id]) ^ (basis_index >> second_node[edge_id])) & 1
        return cost_acc + weights[edge_id] * cut_bit.astype(jnp.float32)

    cost_diag = lax.fori_loop(0, EDGES, add_edge, jnp.zeros((STATE,), jnp.float32))
    key_gamma, key_beta = jax.random.split(jax.random.key(seed + 1))
    gammas = jax.random.uniform(key_gamma, (LAYERS,), jnp.float32, 0.3, 1.0)
    betas = jax.random.uniform(key_beta, (LAYERS,), jnp.float32, 0.4, 1.2)
    return {'cost_diag': cost_diag, 'gammas': gammas, 'betas': betas}


def apply_mixer(state_re, state_im, cos_half, sin_half):
    for qubit_id in range(QUBITS):
        view_shape = (STATE >> (qubit_id + 1), 2, 1 << qubit_id)
        view_re = state_re.reshape(view_shape)
        view_im = state_im.reshape(view_shape)
        flip_re = jnp.flip(view_re, axis=1)
        flip_im = jnp.flip(view_im, axis=1)
        state_re = (cos_half * view_re + sin_half * flip_im).reshape(STATE)
        state_im = (cos_half * view_im - sin_half * flip_re).reshape(STATE)
    return state_re, state_im


def reference(cost_diag, gammas, betas):
    def layer_step(scan_carry, angles):
        state_re, state_im = scan_carry
        layer_gamma, layer_beta = angles
        phase_angle = layer_gamma * cost_diag
        cos_phase = jnp.cos(phase_angle)
        sin_phase = jnp.sin(phase_angle)
        new_re = state_re * cos_phase + state_im * sin_phase
        new_im = state_im * cos_phase - state_re * sin_phase
        cos_half = jnp.cos(0.5 * layer_beta)
        sin_half = jnp.sin(0.5 * layer_beta)
        return apply_mixer(new_re, new_im, cos_half, sin_half), None

    init_state = (jnp.ones((STATE,), jnp.float32), jnp.zeros((STATE,), jnp.float32))
    final_state, layer_outs = lax.scan(layer_step, init_state, (gammas, betas))
    state_re, state_im = final_state
    energy = jnp.sum(cost_diag * (state_re * state_re + state_im * state_im)) / STATE
    return energy.reshape(1), state_re, state_im
```

```python
import math
import jax
import jax.numpy as jnp
import numpy as np
from jax import lax
from jax.experimental import pallas as pl
from jax.experimental.pallas import tpu as pltpu
from jax.sharding import PartitionSpec as P

LANES = 128
MESH = pl.DeviceIdType.MESH
HIGHEST = lax.Precision.HIGHEST
ANGLE_MAX = 131072.0
INV_TURN = float(np.float32(1.0 / (2.0 * math.pi)))
TURN_HI = 6.28125
TURN_LO = float(np.float32(2.0 * math.pi - 6.28125))
MAGIC = 12582912.0
CHUNKS = 4
PART = 64

SIN_COEFS = [2 * v / 4.0 ** (2 * k + 1) for k, v in enumerate(
    [1.0, -1.6666654611e-1, 8.3321608736e-3, -1.9515295891e-4])]
COS_COEFS = [2 * v / 16.0 ** k for k, v in enumerate(
    [1.0, -0.5, 4.166664568298827e-2, -1.388731625493765e-3, 2.443315711809948e-5])]


def horner(coefs, z):
    acc = coefs[-1] * z + coefs[-2]
    for v in coefs[-3::-1]:
        acc = acc * z + v
    return acc


def double_phase(angle, quarter=None, offset=None):
    turns = angle * INV_TURN
    if quarter is not None:
        turns = turns - quarter
    n = (turns + MAGIC) - MAGIC
    r = (n * TURN_HI - angle) + n * TURN_LO
    if offset is not None:
        r = r + offset
    z = r * r
    s = r * horner(SIN_COEFS, z)
    c = horner(COS_COEFS, z)
    s2 = s * c
    c2 = 2.0 - s * s
    return 2.0 - s2 * s2, s2 * c2


def rotate_pair(x00, x01, x10, x11, cos_full, sin_full):
    u, v = x00 - x11, x00 + x11
    w, y = x01 + x10, x01 - x10
    u, w = cos_full * u - sin_full * w, sin_full * u + cos_full * w
    return v + u, w + y, w - y, v - u


def popcount_small(k, bits):
    total = k % 2
    for b in range(1, bits):
        total = total + (k // (1 << b)) % 2
    return total


def rotation_power(cos_half, sin_half, bits, scale):
    n = 1 << bits
    row = lax.broadcasted_iota(jnp.int32, (n, n), 0)
    col = lax.broadcasted_iota(jnp.int32, (n, n), 1)
    acc = jnp.full((n, n), scale, jnp.float32)
    for b in range(bits):
        rb, cb = (row >> b) & 1, (col >> b) & 1
        acc = acc * jnp.where(rb == cb, cos_half, jnp.where(rb > cb, sin_half, -sin_half))
    return acc


def gather_kernel(c_hbm, g_ref, b_ref, out_re, out_im, out_energy, out_max,
                  cost, psi_re, psi_im, trig_re, trig_im, wave_re, wave_im, part_re, part_im,
                  w1l, w1r, w2l, w2r, tab_q, tab_o, cmax, ebuf,
                  own_sem, sx, sy, sc, srx, sry, rx, ry, rd, rc, swave, rwave, se, re_sem):
    qx, qy = lax.axis_index("qx"), lax.axis_index("qy")
    x, core = qx // 2, qx % 2
    rows = c_hbm.shape[0]
    chunk = rows // CHUNKS
    half = chunk // 2

    def dev(dx, dy, dc):
        return {"qx": lax.rem(x + dx, 2) * 2 + lax.rem(core + dc, 2), "qy": lax.rem(qy + dy, 2)}

    xn, yn, cn = dev(1, 0, 0), dev(0, 1, 0), dev(0, 0, 1)
    block = [x * 2 + qy, (1 - x) * 2 + qy, x * 2 + (1 - qy), (1 - x) * 2 + (1 - qy)]

    own_copy = pltpu.make_async_copy(c_hbm, cost.at[block[0], core], own_sem)
    own_copy.start()
    barrier = pltpu.get_barrier_semaphore()
    for neighbour in (xn, yn, cn):
        pl.semaphore_signal(barrier, inc=1, device_id=neighbour, device_id_type=MESH)

    tile = (8, LANES)
    cb1, sb1 = jnp.cos(jnp.full(tile, 0.5 * b_ref[0])), jnp.sin(jnp.full(tile, 0.5 * b_ref[0]))
    cb2, sb2 = jnp.cos(jnp.full(tile, 0.5 * b_ref[1])), jnp.sin(jnp.full(tile, 0.5 * b_ref[1]))
    cf1, sf1 = jnp.cos(jnp.full(tile, b_ref[0])), jnp.sin(jnp.full(tile, b_ref[0]))
    cf2, sf2 = jnp.cos(jnp.full(tile, b_ref[1])), jnp.sin(jnp.full(tile, b_ref[1]))
    g1, g2 = g_ref[0], g_ref[1]
    low = (lax.broadcasted_iota(jnp.int32, (PART, LANES), 0) * LANES
           + lax.broadcasted_iota(jnp.int32, (PART, LANES), 1))
    pop = popcount(low, 13)
    for k in range(4):
        q = ((pop + k) & 3).astype(jnp.float32)
        tab_q[k] = 0.25 * q
        tab_o[k] = q * float(np.float32(0.5 * math.pi))

    own_copy.wait()
    pl.semaphore_wait(barrier, 3)

    def remote(src, dst, ssem, rsem, device):
        return pltpu.make_async_remote_copy(src_ref=src, dst_ref=dst, send_sem=ssem, recv_sem=rsem,
                                            device_id=device, device_id_type=MESH)

    def piece(b, k, c):
        return cost.at[b, k, pl.ds(c * chunk, chunk)]

    def to_x(c):
        return remote(piece(block[0], core, c), piece(block[0], core, c), sx.at[c], rx.at[c], xn)

    def to_y(c):
        return remote(piece(block[0], core, c), piece(block[0], core, c), sy.at[c], ry.at[c], yn)

    def relay_x(c):
        return remote(piece(block[2], core, c), piece(block[2], core, c), srx.at[c], rd.at[c], xn)

    def relay_y(c):
        return remote(piece(block[1], core, c), piece(block[1], core, c), sry.at[c], rd.at[c], yn)

    def to_core(i, c):
        return remote(piece(block[i], core, c), piece(block[i], core, c), sc.at[i, c], rc.at[i, c], cn)

    for c in (0, 1, 2):
        to_x(c).start()
        to_y((c + 2) % 4).start()
    for c in range(CHUNKS):
        to_core(0, c).start()

    w1l[...] = rotation_power(cb1[0:1, 0:1], sb1[0:1, 0:1], 8, 1.0)
    w1r[...] = rotation_power(cb1[0:1, 0:1], -sb1[0:1, 0:1], 8, 0.125)
    w2l[...] = rotation_power(cb2[0:1, 0:1], sb2[0:1, 0:1], 8, 1.0)
    w2r[...] = rotation_power(cb2[0:1, 0:1], -sb2[0:1, 0:1], 8, 0.25)
    cmax[...] = jnp.zeros(tile, jnp.float32)

    coref = core.astype(jnp.float32)
    core_sin1 = (2.0 * coref - 1.0) * sb1
    core_sin2 = (2.0 * coref - 1.0) * sb2

    def bit_coef(have, want):
        hf, wf = have.astype(jnp.float32), want.astype(jnp.float32)
        same = 1.0 - (hf - wf) * (hf - wf)
        return same * cb2 + (wf - hf) * sb2

    def mix(ref_re, ref_im, b, c, wl, wr):
        for ref in (ref_re, ref_im):
            lo = ref[b, pl.ds(c * chunk, half)]
            hi = ref[b, pl.ds(c * chunk + half, half)]
            t = jnp.dot(jnp.concatenate([lo, hi], axis=1), wr[...], precision=HIGHEST,
                        preferred_element_type=jnp.float32)
            t = jnp.dot(wl[...], t, precision=HIGHEST, preferred_element_type=jnp.float32)
            ref[b, pl.ds(c * chunk, half)] = t[:, :LANES]
            ref[b, pl.ds(c * chunk + half, half)] = t[:, LANES:]

    def unit(i, c):
        b = block[i]
        bx, by = b // 2, b % 2
        coef = bit_coef(bx, x) * bit_coef(by, qy)

        def body(p, carry):
            r0 = c * chunk + p * PART
            base = popcount_small(p, 3) + (c % 2) + (c // 2) + bx + by
            k_own, k_par = lax.rem(base + core, 4), lax.rem(base + 1 - core, 4)
            own = cost[b, core, pl.ds(r0, PART)]
            par = cost[b, 1 - core, pl.ds(r0, PART)]
            three = (PART // 8, 8, LANES)
            m = jnp.maximum(jnp.abs(own), jnp.abs(par)).reshape(three).max(axis=0)
            cmax[...] = jnp.maximum(cmax[...], m)
            pr, pi = double_phase(g1 * own, tab_q[k_own], tab_o[k_own])
            qr, qi = double_phase(g1 * par, tab_q[k_par], tab_o[k_par])
            psi_re[b, pl.ds(r0, PART)] = (cb1 * pr.reshape(three) + core_sin1 * qr.reshape(three)).reshape(PART, LANES)
            psi_im[b, pl.ds(r0, PART)] = (cb1 * pi.reshape(three) + core_sin1 * qi.reshape(three)).reshape(PART, LANES)
            ar, ai = double_phase(g2 * own)
            trig_re[b, pl.ds(r0, PART)] = (coef * ar.reshape(three)).reshape(PART, LANES)
            trig_im[b, pl.ds(r0, PART)] = (coef * ai.reshape(three)).reshape(PART, LANES)
            return carry

        lax.fori_loop(0, chunk // PART, body, 0)
        mix(psi_re, psi_im, b, c, w1l, w1r)

    for c in range(CHUNKS):
        to_core(0, c).wait_recv()
        unit(0, c)

    slots = [((1, 0), (2, 2)), ((1, 1), (2, 3)), ((1, 2), (2, 0)), ((3, 2), (3, 0)), ((1, 3), (2, 1)), ((3, 3), (3, 1))]
    arrive = {1: to_x, 2: to_y, 3: relay_x}
    for n, slot in enumerate(slots):
        for i, c in slot:
            arrive[i](c).wait_recv()
            to_core(i, c).start()
        if n == 0:
            relay_x(2).start()
            relay_y(0).start()
            to_x(3).start()
            to_y(1).start()
        if n == 1:
            relay_x(3).start()
            relay_y(1).start()
        for i, c in slot:
            to_core(i, c).wait_recv()
            unit(i, c)

    def tail(p, carry):
        r = [pl.ds(pl.multiple_of(c * chunk + p * 8, 8), 8) for c in range(CHUNKS)]
        mixed = []
        for ref in (psi_re, psi_im):
            v = [[ref[b, r[c]] for c in range(CHUNKS)] for b in range(4)]
            v = [list(rotate_pair(*v[b], cf1, sf1)) for b in range(4)]
            cols = [rotate_pair(*[v[b][c] for b in range(4)], cf1, sf1) for c in range(CHUNKS)]
            mixed.append(cols)
        zr, zi = [], []
        for c in range(CHUNKS):
            ar = ai = None
            for b in range(4):
                vr, vi = mixed[0][c][b], mixed[1][c][b]
                tr, ti = trig_re[b, r[c]], trig_im[b, r[c]]
                yr, yi = vr * tr - vi * ti, vr * ti + vi * tr
                ar, ai = (yr, yi) if ar is None else (ar + yr, ai + yi)
            zr.append(ar)
            zi.append(ai)
        zr, zi = rotate_pair(*zr, cf2, sf2), rotate_pair(*zi, cf2, sf2)
        for c in range(CHUNKS):
            wave_re[0, r[c]] = zr[c]
            wave_im[0, r[c]] = zi[c]
        return carry

    lax.fori_loop(0, chunk // 8, tail, 0)

    swap = [remote(wave_re.at[0], part_re, swave.at[0], rwave.at[0], cn),
            remote(wave_im.at[0], part_im, swave.at[1], rwave.at[1], cn)]
    for cp in swap:
        cp.start()
    for cp in swap:
        cp.wait()

    def join(p, carry):
        r = pl.ds(pl.multiple_of(p * PART, PART), PART)
        three = (PART // 8, 8, LANES)
        for ref, part in ((wave_re, part_re), (wave_im, part_im)):
            ref[0, r] = (cb2 * ref[0, r].reshape(three) + core_sin2 * part[r].reshape(three)).reshape(PART, LANES)
        return carry

    lax.fori_loop(0, rows // PART, join, 0)
    for c in range(CHUNKS):
        mix(wave_re, wave_im, 0, c, w2l, w2r)

    def energy(p, acc):
        r = pl.ds(pl.multiple_of(p * PART, PART), PART)
        vr, vi = wave_re[0, r], wave_im[0, r]
        out_re[r] = vr
        out_im[r] = vi
        e = cost[block[0], core, r] * (vr * vr + vi * vi)
        return acc + e.reshape(PART // 8, 8, LANES).sum(axis=0)

    me = qy * 4 + qx
    ebuf[me] = lax.fori_loop(0, rows // PART, energy, jnp.zeros(tile, jnp.float32))
    sends = []
    for n in range(1, 8):
        dx, dy, dc = n // 4, (n // 2) % 2, n % 2
        d = dev(dx, dy, dc)
        sends.append(remote(ebuf.at[me], ebuf.at[me], se.at[n], re_sem.at[n], d))
    for cp in sends:
        cp.start()
    for cp in sends:
        cp.wait()
    total = ebuf[0]
    for n in range(1, 8):
        total = total + ebuf[n]
    out_energy[...] = jnp.broadcast_to(jnp.sum(total, keepdims=True), tile)
    out_max[...] = jnp.broadcast_to(jnp.max(cmax[...], keepdims=True), tile)

    for c in range(CHUNKS):
        to_x(c).wait_send()
        to_y(c).wait_send()
        for i in range(4):
            to_core(i, c).wait_send()
    for c in (2, 3):
        relay_x(c).wait_send()
    for c in (0, 1):
        relay_y(c).wait_send()


def fast_program(cost_rows, gammas, betas):
    rows = cost_rows.shape[0]
    f32 = jnp.float32
    vm = pl.BlockSpec(memory_space=pltpu.VMEM)
    sm = pl.BlockSpec(memory_space=pltpu.SMEM)
    dma = pltpu.SemaphoreType.DMA
    big = pltpu.VMEM((4, rows, LANES), f32)
    return pl.pallas_call(
        gather_kernel,
        out_shape=(jax.ShapeDtypeStruct((rows, LANES), f32), jax.ShapeDtypeStruct((rows, LANES), f32),
                   jax.ShapeDtypeStruct((8, LANES), f32), jax.ShapeDtypeStruct((8, LANES), f32)),
        in_specs=[pl.BlockSpec(memory_space=pl.ANY), sm, sm],
        out_specs=(vm, vm, vm, vm),
        scratch_shapes=[
            pltpu.VMEM((4, 2, rows, LANES), f32), big, big, big, big,
            pltpu.VMEM((1, rows, LANES), f32), pltpu.VMEM((1, rows, LANES), f32),
            pltpu.VMEM((rows, LANES), f32), pltpu.VMEM((rows, LANES), f32),
            pltpu.VMEM((256, 256), f32), pltpu.VMEM((256, 256), f32),
            pltpu.VMEM((256, 256), f32), pltpu.VMEM((256, 256), f32),
            pltpu.VMEM((4, PART, LANES), f32), pltpu.VMEM((4, PART, LANES), f32),
            pltpu.VMEM((8, LANES), f32), pltpu.VMEM((8, 8, LANES), f32),
            dma, dma((4,)), dma((4,)), dma((4, 4)), dma((4,)), dma((4,)),
            dma((4,)), dma((4,)), dma((4,)), dma((4, 4)), dma((2,)), dma((2,)), dma((8,)), dma((8,))],
        compiler_params=pltpu.CompilerParams(collective_id=0, has_side_effects=True,
                                             vmem_limit_bytes=60 << 20),
    )(cost_rows, gammas, betas)


def popcount(values, bits):
    return sum((values >> b) & 1 for b in range(bits))


def solution(mesh):
    size_x, size_y = mesh.shape['qx'], mesh.shape['qy']
    state_spec = P(('inst', 'qx', 'qy'))

    def turn_back(v_re, v_im, rows):
        index = (lax.broadcasted_iota(jnp.int32, (rows, LANES), 0) * LANES
                 + lax.broadcasted_iota(jnp.int32, (rows, LANES), 1))
        dev_id = lax.axis_index('qx') * size_y + lax.axis_index('qy')
        q = (popcount(index, 18) + popcount(dev_id, 3)) & 3
        odd = (q & 1) == 1
        r = jnp.where(odd, v_im, v_re)
        i = jnp.where(odd, v_re, v_im)
        r = jnp.where((q & 2) == 2, -r, r)
        i = jnp.where(((q + 1) & 2) == 2, -i, i)
        return r, i

    def slow_program(cost_rows, gammas, betas):
        rows = cost_rows.shape[0]
        index = (lax.broadcasted_iota(jnp.int32, (rows, LANES), 0) * LANES
                 + lax.broadcasted_iota(jnp.int32, (rows, LANES), 1))
        dev_id = lax.axis_index('qx') * size_y + lax.axis_index('qy')
        q = (popcount(index, 18) + popcount(dev_id, 3)) & 3
        v_re = jnp.where(q == 0, 1.0, jnp.where(q == 2, -1.0, 0.0))
        v_im = jnp.where(q == 1, 1.0, jnp.where(q == 3, -1.0, 0.0))

        def rotate(v, axis, bit, size, ch, sh):
            perm = [(d, d ^ (1 << bit)) for d in range(size)]
            mine = ((lax.axis_index(axis) >> bit) & 1).astype(jnp.float32)
            return ch * v + (2.0 * mine - 1.0) * sh * lax.ppermute(v, axis, perm)

        for layer in range(2):
            t = gammas[layer] * cost_rows
            a, s = jnp.cos(t), jnp.sin(t)
            v_re, v_im = v_re * a + v_im * s, v_im * a - v_re * s
            ch, sh = jnp.cos(0.5 * betas[layer]), jnp.sin(0.5 * betas[layer])
            u7, u4 = rotation_power(ch, sh, 7, 1.0), rotation_power(ch, sh, 4, 1.0)
            v = jnp.stack([v_re, v_im]).reshape(2, 16, 128, 128)
            v = jnp.einsum('pijk,ck->pijc', v, u7, precision=HIGHEST)
            v = jnp.einsum('pijc,bj->pibc', v, u7, precision=HIGHEST)
            v = jnp.einsum('pibc,ai->pabc', v, u4, precision=HIGHEST)
            v = rotate(v, 'qy', 0, size_y, ch, sh)
            v = rotate(v, 'qx', 0, size_x, ch, sh)
            v = rotate(v, 'qx', 1, size_x, ch, sh)
            v_re, v_im = v[0].reshape(rows, LANES), v[1].reshape(rows, LANES)
        energy = jnp.sum(cost_rows * (v_re * v_re + v_im * v_im))
        for axis, bit, size in (('qy', 0, size_y), ('qx', 0, size_x), ('qx', 1, size_x)):
            energy = energy + lax.ppermute(energy, axis, [(d, d ^ (1 << bit)) for d in range(size)])
        return (energy,) + turn_back(v_re, v_im, rows)

    def device_body(cost_local, gammas, betas):
        local_len = cost_local.shape[0]
        rows = local_len // LANES
        cost_rows = cost_local.reshape(rows, LANES)
        v_re, v_im, energy, cost_max = fast_program(cost_rows, gammas, betas)
        large = cost_max[0, 0] * jnp.max(jnp.abs(gammas)) > ANGLE_MAX
        energy, s_re, s_im = lax.cond(
            large, lambda: slow_program(cost_rows, gammas, betas),
            lambda: (energy[0, 0],) + turn_back(v_re, v_im, rows))
        energy = energy / (local_len * size_x * size_y)
        return energy.reshape(1), s_re.reshape(local_len), s_im.reshape(local_len)

    return jax.shard_map(device_body, mesh=mesh, in_specs=(state_spec, P(), P()),
                         out_specs=(P('inst'), state_spec, state_spec), check_vma=False)
```

```python
import math
import jax
import jax.numpy as jnp
import numpy as np
from jax import lax
from jax.experimental import pallas as pl
from jax.experimental.pallas import tpu as pltpu
from jax.sharding import PartitionSpec as P

LANES = 128
MESH = pl.DeviceIdType.MESH
HIGHEST = lax.Precision.HIGHEST
ANGLE_MAX = 131072.0
INV_TURN = float(np.float32(1.0 / (2.0 * math.pi)))
TURN_HI = 6.28125
TURN_LO = float(np.float32(2.0 * math.pi - 6.28125))
CHUNKS = 4
PART = 64

SIN_COEFS = [2 * v / 4.0 ** (2 * k + 1) for k, v in enumerate(
    [1.0, -1.6666654611e-1, 8.3321608736e-3, -1.9515295891e-4])]
COS_COEFS = [2 * v / 16.0 ** k for k, v in enumerate(
    [1.0, -0.5, 4.166664568298827e-2, -1.388731625493765e-3, 2.443315711809948e-5])]


def horner(coefs, z):
    acc = coefs[-1] * z + coefs[-2]
    for v in coefs[-3::-1]:
        acc = acc * z + v
    return acc


def double_phase(angle, quarter=None, offset=None):
    turns = angle * INV_TURN
    if quarter is not None:
        turns = turns - quarter
    n = lax.round(turns, lax.RoundingMethod.TO_NEAREST_EVEN)
    r = (n * TURN_HI - angle) + n * TURN_LO
    if offset is not None:
        r = r + offset
    z = r * r
    s = r * horner(SIN_COEFS, z)
    c = horner(COS_COEFS, z)
    s2 = s * c
    c2 = 2.0 - s * s
    return 2.0 - s2 * s2, s2 * c2


def rotate_pair(x00, x01, x10, x11, cos_full, sin_full):
    u, v = x00 - x11, x00 + x11
    w, y = x01 + x10, x01 - x10
    u, w = cos_full * u - sin_full * w, sin_full * u + cos_full * w
    return v + u, w + y, w - y, v - u


def popcount_small(k, bits):
    total = k % 2
    for b in range(1, bits):
        total = total + (k // (1 << b)) % 2
    return total


def rotation_power(cos_half, sin_half, bits, scale):
    n = 1 << bits
    row = lax.broadcasted_iota(jnp.int32, (n, n), 0)
    col = lax.broadcasted_iota(jnp.int32, (n, n), 1)
    acc = jnp.full((n, n), scale, jnp.float32)
    for b in range(bits):
        rb, cb = (row >> b) & 1, (col >> b) & 1
        acc = acc * jnp.where(rb == cb, cos_half, jnp.where(rb > cb, sin_half, -sin_half))
    return acc


def row_gates(arr, cos_half, signed, lower, cos_full, sin_full):
    for b in range(3):
        k = 1 << b
        if k == 4:
            other = pltpu.roll(arr, 4, 1)
        else:
            other = jnp.where(lower[b], pltpu.roll(arr, 8 - k, 1), pltpu.roll(arr, k, 1))
        arr = cos_half * arr + signed[b] * other
    v = [arr[k] for k in range(32)]
    for q in (1, 4):
        for k in range(32):
            if (k // q) % 4 == 0:
                quad = (k, k + q, k + 2 * q, k + 3 * q)
                for d, value in zip(quad, rotate_pair(*[v[d] for d in quad], cos_full, sin_full)):
                    v[d] = value
    for k in range(16):
        lo, hi = v[k], v[k + 16]
        v[k], v[k + 16] = cos_half * lo - signed[3] * hi, signed[3] * lo + cos_half * hi
    return v


def run_rows(views, c, chunk, consts):
    half = chunk // 2
    for ref in views:
        def body(g, carry):
            r = pl.ds(pl.multiple_of(c * chunk + g * half, half), half)
            v = row_gates(ref[r].reshape(half // 8, 8, LANES), *consts)
            for k in range(half // 8):
                ref[pl.ds(pl.multiple_of(c * chunk + g * half + k * 8, 8), 8)] = v[k]
            return carry
        lax.fori_loop(0, 2, body, 0)


def run_lanes(views, chunk, w):
    half = chunk // 2
    spans = [(ref, pl.ds(pl.multiple_of(c * chunk, half), half), pl.ds(pl.multiple_of(c * chunk + half, half), half))
             for ref, c in views]
    lhs = [jnp.concatenate([ref[lo], ref[hi]], axis=1) for ref, lo, hi in spans]
    t = jnp.dot(jnp.concatenate(lhs, axis=0), w[...], precision=HIGHEST, preferred_element_type=jnp.float32)
    for n, (ref, lo, hi) in enumerate(spans):
        ref[lo] = t[n * half:(n + 1) * half, :LANES]
        ref[hi] = t[n * half:(n + 1) * half, LANES:]


def cos_sin(v):
    v = jnp.full((8, LANES), v)
    return jnp.cos(v), jnp.sin(v)


def sublane_masks():
    sub = lax.broadcasted_iota(jnp.int32, (8, LANES), 0)
    return [(sub & (1 << b)) == 0 for b in range(3)]


def signed_sines(sin_half, lower):
    return [jnp.where(m, -sin_half, sin_half) for m in lower] + [sin_half]


def quarter_tables(tab_a, tab_b):
    low = (lax.broadcasted_iota(jnp.int32, (PART, LANES), 0) * LANES
           + lax.broadcasted_iota(jnp.int32, (PART, LANES), 1))
    pop = popcount(low, 13)
    for k in range(4):
        q = (pop + k) & 3
        tab_a[k] = jnp.where(q == 0, 1.0, jnp.where(q == 2, -1.0, 0.0))
        tab_b[k] = jnp.where(q == 1, 1.0, jnp.where(q == 3, -1.0, 0.0))
    return pop


def gather_kernel(c_hbm, g_ref, b_ref, out_re, out_im, out_cost, out_pair,
                  cost, psi, trig, pre_a, pre_p, pre_q, wave, part, w1, w2, tab_q, tab_o, tab_a, tab_b, cmax, ebuf,
                  own_sem, out_sem, keep_sem, sx, sy, sr, sc, rx, ry, rd, rc, swave, rwave, se, re_sem):
    qx, qy = lax.axis_index("qx"), lax.axis_index("qy")
    x, core = qx // 2, qx % 2
    rows = c_hbm.shape[0]
    chunk = rows // CHUNKS

    def dev(dx, dy, dc):
        return {"qx": lax.rem(x + dx, 2) * 2 + lax.rem(core + dc, 2), "qy": lax.rem(qy + dy, 2)}

    xn, yn, cn = dev(1, 0, 0), dev(0, 1, 0), dev(0, 0, 1)

    own_copy = pltpu.make_async_copy(c_hbm, cost.at[0, 0], own_sem)
    own_copy.start()
    barrier = pltpu.get_barrier_semaphore()
    for neighbour in (xn, yn, cn):
        pl.semaphore_signal(barrier, inc=1, device_id=neighbour, device_id_type=MESH)

    tile = (8, LANES)
    three = (PART // 8, 8, LANES)

    ch1, sh1 = cos_sin(0.5 * b_ref[0])
    ch2, sh2 = cos_sin(0.5 * b_ref[1])
    cf1, sf1 = cos_sin(b_ref[0])
    cf2, sf2 = cos_sin(b_ref[1])
    g1, g2 = g_ref[0], g_ref[1]
    pop = quarter_tables(tab_a, tab_b)
    for k in range(4):
        q = ((pop + k) & 3).astype(jnp.float32)
        tab_q[k] = 0.25 * q
        tab_o[k] = q * float(np.float32(0.5 * math.pi))
    lower = sublane_masks()
    signed1, signed2 = signed_sines(sh1, lower), signed_sines(sh2, lower)

    own_copy.wait()
    pl.semaphore_wait(barrier, 3)

    def remote(src, dst, ssem, rsem, device):
        return pltpu.make_async_remote_copy(src_ref=src, dst_ref=dst, send_sem=ssem, recv_sem=rsem,
                                            device_id=device, device_id_type=MESH)

    def rows_of(c):
        return pl.ds(c * chunk, chunk)

    def to_x(c):
        return remote(cost.at[0, 0, rows_of(c)], cost.at[1, 0, rows_of(c)], sx.at[c], rx.at[c], xn)

    def to_y(c):
        return remote(cost.at[0, 0, rows_of(c)], cost.at[2, 0, rows_of(c)], sy.at[c], ry.at[c], yn)

    def relay(c):
        if c >= 2:
            return remote(cost.at[2, 0, rows_of(c)], cost.at[3, 0, rows_of(c)], sr.at[c], rd.at[c], xn)
        return remote(cost.at[1, 0, rows_of(c)], cost.at[3, 0, rows_of(c)], sr.at[c], rd.at[c], yn)

    def to_core(i, c):
        return remote(cost.at[i, 0, rows_of(c)], cost.at[i, 1, rows_of(c)], sc.at[i, c], rc.at[i, c], cn)

    def keep(i, k, c):
        return pltpu.make_async_copy(cost.at[i, k, rows_of(c)], out_cost.at[i, k, rows_of(c)], keep_sem.at[i, k, c])

    for c in range(CHUNKS):
        to_x(c).start()
        to_y((c + 2) % 4).start()
    for c in range(CHUNKS):
        to_core(0, c).start()

    w1[...] = rotation_power(ch1[0:1, 0:1], -sh1[0:1, 0:1], 8, 2.0 ** -6)
    w2[...] = rotation_power(ch2[0:1, 0:1], -sh2[0:1, 0:1], 8, 2.0 ** -3)
    cmax[...] = jnp.zeros(tile, jnp.float32)

    xf, yf, kf = x.astype(jnp.float32), qy.astype(jnp.float32), core.astype(jnp.float32)
    sign_x, sign_y, sign_k = 2.0 * xf - 1.0, 2.0 * yf - 1.0, 2.0 * kf - 1.0
    flip = sign_x * sign_y
    sx1 = -sign_x * sf1
    sx2, sy2 = sign_x * sh2, sign_y * sh2
    contract = [ch2 * ch2, sx2 * ch2, flip * (ch2 * sy2), flip * (sx2 * sy2)]
    spread = [1.0, 1.0, flip, flip]

    def phases(i, c):
        bx = x if i % 2 == 0 else 1 - x
        by = qy if i < 2 else 1 - qy
        ca, cb = spread[i] * ch1, spread[i] * sign_k * sh1

        def first(p, carry):
            r = pl.ds(pl.multiple_of(c * chunk + p * PART, PART), PART)
            own = cost[i, 0, r]
            k = lax.rem(popcount_small(p, 3) + c % 2 + c // 2 + bx + by + core, 4)
            pr, pi = double_phase(g1 * own, tab_q[k], tab_o[k])
            psi[0, i, r] = (ca * pr.reshape(three)).reshape(PART, LANES)
            psi[1, i, r] = (ca * pi.reshape(three)).reshape(PART, LANES)
            ar, ai = double_phase(g2 * own)
            trig[0, i, r] = (contract[i] * ar.reshape(three)).reshape(PART, LANES)
            trig[1, i, r] = (contract[i] * ai.reshape(three)).reshape(PART, LANES)
            cmax[...] = jnp.maximum(cmax[...], jnp.abs(own).reshape(three).max(axis=0))
            return carry

        def second(p, carry):
            r = pl.ds(pl.multiple_of(c * chunk + p * PART, PART), PART)
            other = cost[i, 1, r]
            k = lax.rem(popcount_small(p, 3) + c % 2 + c // 2 + bx + by + 1 - core, 4)
            pr, pi = double_phase(g1 * other, tab_q[k], tab_o[k])
            psi[0, i, r] = psi[0, i, r] + (cb * pr.reshape(three)).reshape(PART, LANES)
            psi[1, i, r] = psi[1, i, r] + (cb * pi.reshape(three)).reshape(PART, LANES)
            cmax[...] = jnp.maximum(cmax[...], jnp.abs(other).reshape(three).max(axis=0))
            return carry

        return first, second

    consts1 = (ch1, signed1, lower, cf1, sf1)
    consts2 = (ch2, signed2, lower, cf2, sf2)
    parts = chunk // PART

    def mix1(units):
        for i, c in units:
            run_rows([psi.at[0, i], psi.at[1, i]], c, chunk, consts1)
        run_lanes([(psi.at[k, i], c) for i, c in units for k in range(2)], chunk, w1)

    for n in range(2):
        units = [(0, 2 * n), (0, 2 * n + 1)]
        for i, c in units:
            lax.fori_loop(0, parts, phases(i, c)[0], 0)
        for i, c in units:
            keep(i, 0, c).start()
            to_core(i, c).wait_recv()
            keep(i, 1, c).start()
            lax.fori_loop(0, parts, phases(i, c)[1], 0)
        mix1(units)

    def pre(p, carry):
        r = [pl.ds(pl.multiple_of(c * chunk + p * 8, 8), 8) for c in range(CHUNKS)]
        mixed = []
        for k in range(2):
            v = [rotate_pair(*[psi[k, i, r[c]] for c in range(CHUNKS)], cf1, sf1) for i in range(3)]
            cols = []
            for c in range(CHUNKS):
                own, w, y = v[0][c], v[2][c] + v[1][c], v[2][c] - v[1][c]
                u, w = cf1 * own - sx1 * w, sx1 * own + cf1 * w
                cols.append((own + u, w - y, w + y, own - u))
            mixed.append(cols)
        for c in range(CHUNKS):
            tr = [trig[0, i, r[c]] for i in range(3)]
            ti = [trig[1, i, r[c]] for i in range(3)]
            re, im = mixed[0][c], mixed[1][c]
            ar = ai = None
            for i in range(3):
                yr, yi = re[i] * tr[i] - im[i] * ti[i], re[i] * ti[i] + im[i] * tr[i]
                ar, ai = (yr, yi) if ar is None else (ar + yr, ai + yi)
            pre_a[0, r[c]], pre_a[1, r[c]] = ar, ai
            pre_p[0, r[c]], pre_p[1, r[c]] = re[3], im[3]
            pre_q[0, r[c]] = (1.0 - cf1) * tr[0] - sx1 * (tr[1] + tr[2])
            pre_q[1, r[c]] = (1.0 - cf1) * ti[0] - sx1 * (ti[1] + ti[2])
        return carry

    slots = [((1, 0), (2, 2)), ((1, 1), (2, 3)), ((1, 2), (2, 0)), ((1, 3), (2, 1)), ((3, 2), (3, 0)), ((3, 3), (3, 1))]
    arrive = {1: to_x, 2: to_y, 3: relay}
    for n, slot in enumerate(slots):
        for i, c in slot:
            arrive[i](c).wait_recv()
            to_core(i, c).start()
            keep(i, 0, c).start()
            if n < 2:
                relay(c).start()
        for i, c in slot:
            lax.fori_loop(0, parts, phases(i, c)[0], 0)
        for i, c in slot:
            to_core(i, c).wait_recv()
            keep(i, 1, c).start()
            lax.fori_loop(0, parts, phases(i, c)[1], 0)
        mix1(slot)
        if n == 3:
            lax.fori_loop(0, chunk // 8, pre, 0)

    def tail(p, carry):
        r = [pl.ds(pl.multiple_of(c * chunk + p * 8, 8), 8) for c in range(CHUNKS)]
        vr = rotate_pair(*[psi[0, 3, r[c]] for c in range(CHUNKS)], cf1, sf1)
        vi = rotate_pair(*[psi[1, 3, r[c]] for c in range(CHUNKS)], cf1, sf1)
        zr, zi = [], []
        for c in range(CHUNKS):
            tr, ti = trig[0, 3, r[c]], trig[1, 3, r[c]]
            pr, pi = pre_p[0, r[c]], pre_p[1, r[c]]
            qr, qi = pre_q[0, r[c]] + (1.0 + cf1) * tr, pre_q[1, r[c]] + (1.0 + cf1) * ti
            zr.append(pre_a[0, r[c]] + (pr * tr - pi * ti) + (vr[c] * qr - vi[c] * qi))
            zi.append(pre_a[1, r[c]] + (pr * ti + pi * tr) + (vr[c] * qi + vi[c] * qr))
        zr, zi = rotate_pair(*zr, cf2, sf2), rotate_pair(*zi, cf2, sf2)
        for c in range(CHUNKS):
            wave[0, r[c]] = zr[c]
            wave[1, r[c]] = zi[c]
        return carry

    lax.fori_loop(0, chunk // 8, tail, 0)

    def swap(c):
        return remote(wave.at[:, rows_of(c)], part.at[:, rows_of(c)], swave.at[c], rwave.at[c], cn)

    for c in range(CHUNKS):
        run_rows([wave.at[0], wave.at[1]], c, chunk, consts2)
        run_lanes([(wave.at[0], c), (wave.at[1], c)], chunk, w2)
        swap(c).start()

    sk2 = sign_k * sh2
    energy = jnp.zeros(tile, jnp.float32)
    outs = []
    for c in range(CHUNKS):
        swap(c).wait_recv()

        def last(p, acc):
            r = pl.ds(pl.multiple_of(c * chunk + p * PART, PART), PART)
            vr = ch2 * wave[0, r].reshape(three) + sk2 * part[0, r].reshape(three)
            vi = ch2 * wave[1, r].reshape(three) + sk2 * part[1, r].reshape(three)
            k = lax.rem(popcount_small(p, 3) + c % 2 + c // 2 + x + qy + core, 4)
            ta, tb = tab_a[k].reshape(three), tab_b[k].reshape(three)
            part[0, r] = (ta * vr + tb * vi).reshape(PART, LANES)
            part[1, r] = (ta * vi - tb * vr).reshape(PART, LANES)
            return acc + (cost[0, 0, r].reshape(three) * (vr * vr + vi * vi)).sum(axis=0)

        energy = lax.fori_loop(0, parts, last, energy)
        for k, out in enumerate((out_re, out_im)):
            cp = pltpu.make_async_copy(part.at[k, rows_of(c)], out.at[rows_of(c)], out_sem.at[k, c])
            cp.start()
            outs.append(cp)

    me = qy * 4 + qx
    ebuf[me] = energy
    sends = []
    for n in range(1, 8):
        d = dev(n // 4, (n // 2) % 2, n % 2)
        sends.append(remote(ebuf.at[me], ebuf.at[me], se.at[n], re_sem.at[n], d))
    for cp in sends:
        cp.start()
    for c in range(CHUNKS):
        to_x(c).wait_send()
        to_y(c).wait_send()
        relay(c).wait_send()
        swap(c).wait_send()
        for i in range(4):
            to_core(i, c).wait_send()
            for k in range(2):
                keep(i, k, c).wait()
    for cp in outs:
        cp.wait()
    for cp in sends:
        cp.wait()
    total = ebuf[0]
    for n in range(1, 8):
        total = total + ebuf[n]
    out_pair[0] = jnp.sum(total)
    out_pair[1] = jnp.max(cmax[...]) * jnp.maximum(jnp.abs(g1), jnp.abs(g2))


def final_kernel(in_re, in_im, in_cost, pair, g_ref, b_ref, out_re, out_im, out_energy,
                 state, cost, psi, w, tab_a, tab_b, in_sem, out_sem, cost_sem):
    rows = in_re.shape[0]
    chunk = rows // CHUNKS
    parts = rows // PART
    three = (PART // 8, 8, LANES)
    small = pair[1] <= ANGLE_MAX

    def rows_of(c):
        return pl.ds(c * chunk, chunk)

    def put(k, c):
        out = (out_re, out_im)[k]
        return pltpu.make_async_copy(state.at[k, rows_of(c)], out.at[rows_of(c)], out_sem.at[k, c])

    @pl.when(small)
    def _():
        def get(k, c):
            return pltpu.make_async_copy((in_re, in_im)[k].at[rows_of(c)], state.at[k, rows_of(c)], in_sem.at[k, c])

        pieces = [(k, c) for c in range(CHUNKS) for k in range(2)]
        for k, c in pieces:
            get(k, c).start()
        for k, c in pieces:
            get(k, c).wait()
            put(k, c).start()
        out_energy[0] = pair[0] * (1.0 / (8 * rows * LANES))

    @pl.when(jnp.logical_not(small))
    def _():
        qx, qy = lax.axis_index("qx"), lax.axis_index("qy")
        copies = []
        for a in range(8):
            i = lax.rem(a // 4 + qx // 2, 2) + 2 * lax.rem(a % 2 + qy, 2)
            k = lax.rem((a // 2) % 2 + qx, 2)
            copies.append(pltpu.make_async_copy(in_cost.at[i, k], cost.at[a], cost_sem.at[a]))
        for cp in copies:
            cp.start()
        quarter_tables(tab_a, tab_b)
        for cp in copies:
            cp.wait()
        lower = sublane_masks()

        def part_of(n):
            a, p = n // parts, n % parts
            return a, pl.ds(pl.multiple_of(p * PART, PART), PART), lax.rem(popcount_small(p, 5) + popcount_small(a, 3), 4)

        for layer in range(2):
            ch, sh = cos_sin(0.5 * b_ref[layer])
            cf, sf = cos_sin(b_ref[layer])
            gamma = g_ref[layer]

            def phase(n, carry):
                a, r, k = part_of(n)
                t = gamma * cost[a, r]
                vr, vi = jnp.cos(t), -jnp.sin(t)
                qr, qi = (tab_a[k], tab_b[k]) if layer == 0 else (psi[0, a, r], psi[1, a, r])
                psi[0, a, r] = vr * qr - vi * qi
                psi[1, a, r] = vr * qi + vi * qr
                return carry

            lax.fori_loop(0, 8 * parts, phase, 0)
            w[...] = rotation_power(ch[0:1, 0:1], -sh[0:1, 0:1], 8, 2.0 ** -4)
            consts = (ch, signed_sines(sh, lower), lower, cf, sf)

            def within(n, carry):
                a, c = n // CHUNKS, n % CHUNKS
                run_rows([psi.at[0, a], psi.at[1, a]], c, chunk, consts)
                run_lanes([(psi.at[0, a], c), (psi.at[1, a], c)], chunk, w)
                return carry

            lax.fori_loop(0, 8 * CHUNKS, within, 0)

            def chunk_bits(n, carry):
                k, a, p = n // (chunk // 8 * 8), (n // (chunk // 8)) % 8, n % (chunk // 8)
                r = [pl.ds(pl.multiple_of(c * chunk + p * 8, 8), 8) for c in range(CHUNKS)]
                for c, value in enumerate(rotate_pair(*[psi[k, a, r[c]] for c in range(CHUNKS)], cf, sf)):
                    psi[k, a, r[c]] = value
                return carry

            lax.fori_loop(0, 16 * (chunk // 8), chunk_bits, 0)

            def top_bits(n, carry):
                k, p = n // (rows // 8), n % (rows // 8)
                r = pl.ds(pl.multiple_of(p * 8, 8), 8)
                v = [psi[k, a, r] for a in range(8)]
                v = list(rotate_pair(*v[:4], cf, sf)) + list(rotate_pair(*v[4:], cf, sf))
                for a in range(4):
                    psi[k, a, r] = ch * v[a] - sh * v[a + 4]
                    psi[k, a + 4, r] = sh * v[a] + ch * v[a + 4]
                return carry

            lax.fori_loop(0, 2 * (rows // 8), top_bits, 0)

        def add(n, acc):
            a, r, _ = part_of(n)
            vr, vi = psi[0, a, r], psi[1, a, r]
            return acc + (cost[a, r] * (vr * vr + vi * vi)).reshape(three).sum(axis=0)

        total = jnp.sum(lax.fori_loop(0, 8 * parts, add, jnp.zeros((8, LANES), jnp.float32)))
        out_energy[0] = total * (1.0 / (8 * rows * LANES))
        me = qx * 2 + qy

        def turn(p, carry):
            _, r, k = part_of(me * parts + p)
            vr, vi, ta, tb = psi[0, me, r], psi[1, me, r], tab_a[k], tab_b[k]
            state[0, r] = ta * vr + tb * vi
            state[1, r] = ta * vi - tb * vr
            return carry

        lax.fori_loop(0, parts, turn, 0)
        for c in range(CHUNKS):
            for k in range(2):
                put(k, c).start()

    for c in range(CHUNKS):
        for k in range(2):
            put(k, c).wait()


def simulate(cost_rows, gammas, betas):
    rows = cost_rows.shape[0]
    f32 = jnp.float32
    state = jax.ShapeDtypeStruct((rows, LANES), f32)
    sm = pl.BlockSpec(memory_space=pltpu.SMEM)
    anyspace = pl.BlockSpec(memory_space=pl.ANY)
    dma = pltpu.SemaphoreType.DMA
    full = pltpu.VMEM((2, rows, LANES), f32)
    blocks = pltpu.VMEM((2, 4, rows, LANES), f32)
    table = pltpu.VMEM((4, PART, LANES), f32)
    s_re, s_im, costs, pair = pl.pallas_call(
        gather_kernel,
        out_shape=(state, state, jax.ShapeDtypeStruct((4, 2, rows, LANES), f32), jax.ShapeDtypeStruct((2,), f32)),
        in_specs=[anyspace, sm, sm],
        out_specs=(anyspace, anyspace, anyspace, sm),
        scratch_shapes=[
            pltpu.VMEM((4, 2, rows, LANES), f32), blocks, blocks, full, full, full, full, full,
            pltpu.VMEM((256, 256), f32), pltpu.VMEM((256, 256), f32), table, table, table, table,
            pltpu.VMEM((8, LANES), f32), pltpu.VMEM((8, 8, LANES), f32),
            dma, dma((2, 4)), dma((4, 2, 4)), dma((4,)), dma((4,)), dma((4,)), dma((4, 4)), dma((4,)), dma((4,)),
            dma((4,)), dma((4, 4)), dma((4,)), dma((4,)), dma((8,)), dma((8,))],
        compiler_params=pltpu.CompilerParams(collective_id=0, has_side_effects=True,
                                             vmem_limit_bytes=60 << 20),
    )(cost_rows, gammas, betas)
    return pl.pallas_call(
        final_kernel,
        out_shape=(state, state, jax.ShapeDtypeStruct((1,), f32)),
        in_specs=[anyspace, anyspace, anyspace, sm, sm, sm],
        out_specs=(anyspace, anyspace, sm),
        scratch_shapes=[
            full, pltpu.VMEM((8, rows, LANES), f32), pltpu.VMEM((2, 8, rows, LANES), f32),
            pltpu.VMEM((256, 256), f32), table, table, dma((2, 4)), dma((2, 4)), dma((8,))],
        compiler_params=pltpu.CompilerParams(vmem_limit_bytes=60 << 20),
    )(s_re, s_im, costs, pair, gammas, betas)


def popcount(values, bits):
    return sum((values >> b) & 1 for b in range(bits))


def solution(mesh):
    state_spec = P(('inst', 'qx', 'qy'))

    def device_body(cost_local, gammas, betas):
        local_len = cost_local.shape[0]
        s_re, s_im, energy = simulate(cost_local.reshape(local_len // LANES, LANES), gammas, betas)
        return energy, s_re.reshape(local_len), s_im.reshape(local_len)

    return jax.shard_map(device_body, mesh=mesh, in_specs=(state_spec, P(), P()),
                         out_specs=(P('inst'), state_spec, state_spec), check_vma=False)
```

```python
import math
import jax
import jax.numpy as jnp
import numpy as np
from jax import lax
from jax.experimental import pallas as pl
from jax.experimental.pallas import tpu as pltpu
from jax.sharding import PartitionSpec as P

LANES = 128
MESH = pl.DeviceIdType.MESH
HIGHEST = lax.Precision.HIGHEST
ANGLE_MAX = 131072.0
INV_TURN = float(np.float32(1.0 / (2.0 * math.pi)))
TURN_HI = 6.28125
TURN_LO = float(np.float32(2.0 * math.pi - 6.28125))
CHUNKS = 4
DEVICES = 8
PART = 64

SIN_COEFS = [2 * v / 4.0 ** (2 * k + 1) for k, v in enumerate(
    [1.0, -1.6666654611e-1, 8.3321608736e-3, -1.9515295891e-4])]
COS_COEFS = [2 * v / 16.0 ** k for k, v in enumerate(
    [1.0, -0.5, 4.166664568298827e-2, -1.388731625493765e-3, 2.443315711809948e-5])]


def horner(coefs, z):
    acc = coefs[-1] * z + coefs[-2]
    for v in coefs[-3::-1]:
        acc = acc * z + v
    return acc


def double_phase(cost, gamma, scale, quarter=None, offset=None):
    angle = gamma * cost
    turns = angle * INV_TURN
    if quarter is not None:
        turns = turns - quarter
    n = lax.round(turns, lax.RoundingMethod.TO_NEAREST_EVEN)
    r = (n * TURN_HI - angle) + n * TURN_LO
    if offset is not None:
        r = r + offset
    z = r * r
    s = r * horner(SIN_COEFS, z)
    s2 = s * horner(COS_COEFS, z)
    t2 = scale * s2
    return (scale + scale) - t2 * s2, t2 * (2.0 - s * s)


def rotate_pair(x00, x01, x10, x11, cos_full, sin_full):
    u, v = x00 - x11, x00 + x11
    w, y = x01 + x10, x01 - x10
    u, w = cos_full * u - sin_full * w, sin_full * u + cos_full * w
    return v + u, w + y, w - y, v - u


def quot(a, b):
    return a // b if isinstance(a, int) else lax.div(a, jnp.int32(b))


def rest(a, b):
    return a % b if isinstance(a, int) else lax.rem(a, jnp.int32(b))


def popcount_small(k, bits):
    return sum(rest(quot(k, 1 << b), 2) for b in range(bits))


def rotation_power(cos_half, sin_half, bits, scale):
    n = 1 << bits
    row = lax.broadcasted_iota(jnp.int32, (n, n), 0)
    col = lax.broadcasted_iota(jnp.int32, (n, n), 1)
    acc = jnp.full((n, n), scale, jnp.float32)
    for b in range(bits):
        rb, cb = (row >> b) & 1, (col >> b) & 1
        acc = acc * jnp.where(rb == cb, cos_half, jnp.where(rb > cb, sin_half, -sin_half))
    return acc


def row_gates(arr, cos_half, signed, cos_full, sin_full):
    sub = lax.broadcasted_iota(jnp.int32, (8, LANES), 0)
    for b in range(3):
        k = 1 << b
        other = pltpu.roll(arr, k, 1)
        if 2 * k < 8:
            other = jnp.where((sub & k) == 0, pltpu.roll(arr, 8 - k, 1), other)
        arr = cos_half * arr + signed[b] * other
    v = [arr[k] for k in range(32)]
    for q in (1, 4):
        for k in range(32):
            if (k // q) % 4 == 0:
                quad = (k, k + q, k + 2 * q, k + 3 * q)
                for d, value in zip(quad, rotate_pair(*[v[d] for d in quad], cos_full, sin_full)):
                    v[d] = value
    for k in range(16):
        lo, hi = v[k], v[k + 16]
        v[k], v[k + 16] = cos_half * lo - signed[3] * hi, signed[3] * lo + cos_half * hi
    return v


def loop(start, stop, body, carry, steps=1):
    def turn(n, value):
        for k in range(steps):
            value = body(n * steps + k, value)
        return value
    return lax.fori_loop(start // steps, stop // steps, turn, carry)


def half_lanes(h):
    return pl.ds(pl.multiple_of(h * LANES, LANES), LANES)


def run_rows(ref, h, consts, value=None):
    rows = ref.shape[0]
    value = ref[:, half_lanes(h)] if value is None else value
    v = row_gates(value.reshape(rows // 8, 8, LANES), *consts)
    for k in range(rows // 8):
        ref[pl.ds(8 * k, 8), half_lanes(h)] = v[k]


def run_lanes(ref, w):
    if len(ref.shape) == 2:
        halves = [ref.at[pl.ds(k * LANES, LANES)] for k in range(2)]
    else:
        halves = [ref.at[k] for k in range(2)]
    values = [half[...].reshape(-1, ref.shape[-1]) for half in halves]
    values = [jnp.dot(v, w[...], precision=HIGHEST, preferred_element_type=jnp.float32) for v in values]
    for half, v in zip(halves, values):
        half[...] = v.reshape(half.shape)


def cos_sin(v):
    v = jnp.full((8, LANES), v)
    return jnp.cos(v), jnp.sin(v)


def signed_sines(sin_half):
    sub = lax.broadcasted_iota(jnp.int32, (8, LANES), 0)
    return [jnp.where((sub & (1 << b)) == 0, -sin_half, sin_half) for b in range(3)] + [sin_half]


def quarter_tables(tab_a, tab_b):
    low = (lax.broadcasted_iota(jnp.int32, (PART, LANES), 0) * LANES
           + lax.broadcasted_iota(jnp.int32, (PART, LANES), 1))
    pop = popcount(low, 13)
    for k in range(4):
        q = (pop + k) & 3
        tab_a[k] = jnp.where(q == 0, 1.0, jnp.where(q == 2, -1.0, 0.0))
        tab_b[k] = jnp.where(q == 1, 1.0, jnp.where(q == 3, -1.0, 0.0))
    return pop


def gather_kernel(c_hbm, angles, out_re, out_im, out_cost, out_sums,
                  cost, psi, trig, wave, mixed, part, final, w1, w2,
                  tab_q, tab_o, tab_a, tab_b, cmax, ebuf,
                  own_sem, out_sem, keep_sem, sx, sy, srx, sry, sc, rx, ry, rdx, rdy, rc, swave, rwave, se, re_sem, sums_sem):
    qx, qy = lax.axis_index("qx"), lax.axis_index("qy")
    x, core = quot(qx, 2), rest(qx, 2)
    rows = c_hbm.shape[0]
    chunk = rows // CHUNKS
    half = chunk // 2

    def dev(dx, dy, dc):
        return {"qx": lax.rem(x + dx, 2) * 2 + lax.rem(core + dc, 2), "qy": lax.rem(qy + dy, 2)}

    xn, yn, cn = dev(1, 0, 0), dev(0, 1, 0), dev(0, 0, 1)

    own_copy = pltpu.make_async_copy(c_hbm, cost.at[0, 0], own_sem)
    own_copy.start()
    barrier = pltpu.get_barrier_semaphore()
    for neighbour in (xn, yn, cn):
        pl.semaphore_signal(barrier, inc=1, device_id=neighbour, device_id_type=MESH)

    tile = (8, LANES)
    three = (PART // 8, 8, LANES)
    pl.semaphore_wait(barrier, 3)

    def remote(src, dst, ssem, rsem, device):
        return pltpu.make_async_remote_copy(src_ref=src, dst_ref=dst, send_sem=ssem, recv_sem=rsem,
                                            device_id=device, device_id_type=MESH)

    def rows_of(c):
        return pl.ds(c * chunk, chunk)

    def span(c, h):
        return pl.ds(c * chunk + h * half, half)

    def to_x(c):
        return remote(c_hbm.at[rows_of(c)], cost.at[1, 0, rows_of(c)], sx.at[c], rx.at[c], xn)

    def to_y(c):
        return remote(c_hbm.at[rows_of(c)], cost.at[2, 0, rows_of(c)], sy.at[c], ry.at[c], yn)

    def relay_y(c):
        return remote(cost.at[1, 0, span(c, 0)], cost.at[3, 0, span(c, 0)], sry.at[c], rdy.at[c], yn)

    def relay_x(c):
        return remote(cost.at[2, 0, span(c, 1)], cost.at[3, 0, span(c, 1)], srx.at[c], rdx.at[c], xn)

    def to_core(i, c, h):
        src = c_hbm.at[span(c, h)] if i == 0 else cost.at[i, 0, span(c, h)]
        return remote(src, cost.at[i, 1, span(c, h)], sc.at[i, c, h], rc.at[i, c, h], cn)

    def keep(i, k, c):
        return pltpu.make_async_copy(cost.at[i, k, rows_of(c)], out_cost.at[i, k, rows_of(c)], keep_sem.at[i, k, c])

    for c in range(CHUNKS):
        to_x(c).start()
        to_y(c).start()
    for c in range(CHUNKS):
        for h in range(2):
            to_core(0, c, h).start()

    g1, g2, beta1, beta2 = [angles[k] for k in range(4)]
    ch1, sh1 = cos_sin(0.5 * beta1)
    ch2, sh2 = cos_sin(0.5 * beta2)
    cf1, sf1 = cos_sin(beta1)
    cf2, sf2 = cos_sin(beta2)
    pop = quarter_tables(tab_a, tab_b)
    for k in range(4):
        q = ((pop + k) & 3).astype(jnp.float32)
        tab_q[k] = 0.25 * q
        tab_o[k] = q * float(np.float32(0.5 * math.pi))
    signed1, signed2 = signed_sines(sh1), signed_sines(sh2)

    w1[...] = rotation_power(ch1[0:1, 0:1], -sh1[0:1, 0:1], 8, 2.0 ** -6)
    w2[...] = rotation_power(ch2[0:1, 0:1], -sh2[0:1, 0:1], 8, 2.0 ** -3)
    cmax[...] = jnp.zeros(tile, jnp.float32)

    xf, yf, kf = x.astype(jnp.float32), qy.astype(jnp.float32), core.astype(jnp.float32)
    sign_x, sign_y, sign_k = 2.0 * xf - 1.0, 2.0 * yf - 1.0, 2.0 * kf - 1.0
    flip = sign_x * sign_y
    sx1 = -sign_x * sf1
    sx2, sy2 = sign_x * sh2, sign_y * sh2
    contract = [ch2 * ch2, sx2 * ch2, flip * (ch2 * sy2), flip * (sx2 * sy2)]
    spread = [1.0, 1.0, flip, flip]

    consts1 = (ch1, signed1, cf1, sf1)
    consts2 = (ch2, signed2, cf2, sf2)

    def phases(i, c, own=True, other=True):
        base = c % 2 + c // 2 + (x if i % 2 == 0 else 1 - x) + (qy if i < 2 else 1 - qy)
        ca, cb = spread[i] * ch1, spread[i] * sign_k * sh1
        def body(n, carry):
            r = pl.ds(pl.multiple_of(c * chunk + n * PART, PART), PART)
            spot = (pl.ds(pl.multiple_of(rest(n, 4) * PART, PART), PART), half_lanes(quot(n, 4)))
            terms = []
            for flag, side, coef in ((own, 0, ca), (other, 1, cb)):
                if flag:
                    q = lax.rem(base + popcount_small(n, 3) + (core if side == 0 else 1 - core), 4)
                    terms.append(double_phase(cost[i, side, r].reshape(three), g1, coef,
                                              tab_q[q].reshape(three), tab_o[q].reshape(three)))
            if not own:
                terms.append([psi[k, i, c, *spot].reshape(three) for k in range(2)])
            for k in range(2):
                u = terms[0][k] if len(terms) == 1 else terms[0][k] + terms[1][k]
                psi[k, i, c, *spot] = u.reshape(PART, LANES)
            if own:
                v = cost[i, 0, r].reshape(three)
                for k, u in enumerate(double_phase(v, g2, contract[i])):
                    trig[k, i, r] = u.reshape(PART, LANES)
                if i == 0:
                    cmax[...] = jnp.maximum(cmax[...], jnp.abs(v).max(axis=0))
            return carry

        lax.fori_loop(0, chunk // PART, body, 0)

    def rows_loop(i, c):
        def body(n, carry):
            run_rows(psi.at[quot(n, 2), i, c], rest(n, 2), consts1)
            return carry
        lax.fori_loop(0, 4, body, 0)

    def place(p):
        return pl.ds(pl.multiple_of(rest(p, half // 8) * 8, 8), 8), half_lanes(quot(p, half // 8))

    def chunk_bits(p, carry):
        for k in range(2):
            for i in range(3):
                v = rotate_pair(*[psi[k, i, c, *place(p)] for c in range(CHUNKS)], cf1, sf1)
                for c in range(CHUNKS):
                    psi[k, i, c, *place(p)] = v[c]
        return carry

    def arrived(i, c):
        if i == 1 or i == 2:
            (to_x if i == 1 else to_y)(c).wait_recv()
            (relay_y if i == 1 else relay_x)(c).start()
        if i == 3:
            relay_y(c).wait_recv()
            to_core(i, c, 0).start()
            relay_x(c).wait_recv()
            to_core(i, c, 1).start()
        elif i > 0:
            for h in range(2):
                to_core(i, c, h).start()
        keep(i, 0, c).start()

    def other_arrived(i, c):
        for h in range(2):
            to_core(i, c, h).wait_recv()
        keep(i, 1, c).start()

    def unit(i, c):
        other_arrived(i, c)
        phases(i, c)
        rows_loop(i, c)

    own_copy.wait()
    for c in range(CHUNKS):
        arrived(0, c)
        unit(0, c)
        if c % 2 == 1:
            run_lanes(psi.at[:, 0, pl.ds(c - 1, 2)], w1)
    for c in range(CHUNKS):
        for i in (1, 2):
            arrived(i, c)
        for i in (1, 2):
            unit(i, c)
        run_lanes(psi.at[:, pl.ds(1, 2), c], w1)
    arrived(3, 0)
    loop(0, chunk // 8, chunk_bits, 0, 4)
    arrived(3, 1)
    unit(3, 0)
    unit(3, 1)
    arrived(3, 2)
    run_lanes(psi.at[:, 3, pl.ds(0, 2)], w1)
    unit(3, 2)
    arrived(3, 3)
    run_lanes(psi.at[:, 3, 2], w1)
    phases(3, 3, other=False)
    other_arrived(3, 3)
    phases(3, 3, own=False)
    rows_loop(3, 3)
    run_lanes(psi.at[:, 3, 3], w1)

    def tail(p, carry):
        r = [pl.ds(pl.multiple_of(c * chunk + p * 8, 8), 8) for c in range(CHUNKS)]
        diag = [rotate_pair(*[psi[k, 3, c, *place(p)] for c in range(CHUNKS)], cf1, sf1) for k in range(2)]
        z = [[], []]
        for c in range(CHUNKS):
            v = [rotate_pair(*[psi[k, i, c, *place(p)] for i in (0, 2, 1)], diag[k][c], cf1, sx1) for k in range(2)]
            sums = None
            for n, i in enumerate((0, 2, 1, 3)):
                (re, im), (tr, ti) = (v[0][n], v[1][n]), (trig[0, i, r[c]], trig[1, i, r[c]])
                term = (re * tr - im * ti, re * ti + im * tr)
                sums = term if sums is None else (sums[0] + term[0], sums[1] + term[1])
            z[0].append(sums[0])
            z[1].append(sums[1])
        for k in range(2):
            for c, value in enumerate(rotate_pair(*z[k], cf2, sf2)):
                wave[quot(p, half // 8), k, c, place(p)[0]] = value
        return carry

    def swap(n):
        spot = (n // 2, slice(None), slice(None), pl.ds(n % 2 * LANES, LANES))
        return remote(wave.at[*spot], part.at[*spot], swave.at[n], rwave.at[n], cn)

    quarter = chunk // 8 // 4
    for n in range(4):
        loop(n * quarter, (n + 1) * quarter, tail, 0, 2)
        swap(n).start()

    sk2 = sign_k * sh2
    for h in range(2):
        for n in range(2):
            swap(2 * h + n).wait_recv()

        def turn(n, carry, h=h):
            k, c = quot(n, CHUNKS), rest(n, CHUNKS)
            shape = (half // 8, 8, LANES)
            run_rows(mixed.at[k, c], h, consts2, ch2 * wave[h, k, c].reshape(shape) + sk2 * part[h, k, c].reshape(shape))
            return carry

        lax.fori_loop(0, 2 * CHUNKS, turn, 0)

    energy = jnp.zeros(tile, jnp.float32)
    outs = []
    for c in range(CHUNKS):
        if c % 2 == 0:
            run_lanes(mixed.at[:, pl.ds(c, 2)], w2)

        def last(p, acc, c=c):
            r = pl.ds(pl.multiple_of(c * chunk + p * PART, PART), PART)
            spot = (pl.ds(pl.multiple_of(rest(p, 4) * PART, PART), PART), half_lanes(quot(p, 4)))
            vr, vi = [mixed[k, c, *spot] for k in range(2)]
            k = lax.rem(popcount_small(p, 3) + c % 2 + c // 2 + x + qy + core, 4)
            final[0, r] = tab_a[k] * vr + tab_b[k] * vi
            final[1, r] = tab_a[k] * vi - tab_b[k] * vr
            return acc + (cost[0, 0, r] * (vr * vr + vi * vi)).reshape(three).sum(axis=0)

        energy = loop(0, chunk // PART, last, energy, 4)
        for k, out in enumerate((out_re, out_im)):
            cp = pltpu.make_async_copy(final.at[k, rows_of(c)], out.at[rows_of(c)], out_sem.at[k, c])
            cp.start()
            outs.append(cp)

    me = qy * 4 + qx
    ebuf[me, 0], ebuf[me, 1] = energy, cmax[...] * jnp.maximum(jnp.abs(g1), jnp.abs(g2))
    sends = []
    for n in range(1, DEVICES):
        d = dev(n // 4, (n // 2) % 2, n % 2)
        sends.append(remote(ebuf.at[me], ebuf.at[me], se.at[n], re_sem.at[n], d))
    for cp in sends:
        cp.start()
    for c in range(CHUNKS):
        to_x(c).wait_send()
        to_y(c).wait_send()
        relay_x(c).wait_send()
        relay_y(c).wait_send()
        swap(c).wait_send()
        for i in range(4):
            for k in range(2):
                to_core(i, c, k).wait_send()
                keep(i, k, c).wait()
    for cp in outs:
        cp.wait()
    for cp in sends:
        cp.wait()
    for k in range(2):
        ebuf[DEVICES, k], ebuf[DEVICES + 1, k] = jnp.full(tile, (g1, g2)[k]), jnp.full(tile, (beta1, beta2)[k])
    sums = pltpu.make_async_copy(ebuf, out_sums, sums_sem)
    sums.start()
    sums.wait()


def final_kernel(in_re, in_im, in_cost, in_sums, out_re, out_im, out_energy,
                 state, cost, psi, w, tab_a, tab_b, sums, energy, out_sem, cost_sem, small_sem):
    rows = in_re.shape[0]
    chunk = rows // CHUNKS
    parts, spots = rows // PART, chunk // 8
    outs = (out_re, out_im)

    def put(k, c, src):
        r = pl.ds(c * chunk, chunk)
        return pltpu.make_async_copy(src.at[r], outs[k].at[r], out_sem.at[k, c])

    def put_all(srcs):
        return [put(k, c, srcs[k]) for c in range(CHUNKS) for k in range(2)]

    def put_energy(total):
        energy[0] = total * (1.0 / (DEVICES * rows * LANES))
        return pltpu.make_async_copy(energy, out_energy, small_sem.at[1])

    def run(copies):
        for cp in copies:
            cp.start()
        return copies

    def finish(copies):
        for cp in copies:
            cp.wait()

    moves = run(put_all((in_re, in_im)))
    finish(run([pltpu.make_async_copy(in_sums, sums, small_sem.at[0])]))
    total, largest = sums[0, 0], sums[0, 1]
    for n in range(1, DEVICES):
        total, largest = total + sums[n, 0], jnp.maximum(largest, sums[n, 1])
    moves += run([put_energy(jnp.sum(total))])
    small = jnp.max(largest) <= ANGLE_MAX
    finish(moves)

    @pl.when(jnp.logical_not(small))
    def _():
        qx, qy = lax.axis_index("qx"), lax.axis_index("qy")
        fetch = []
        for a in range(DEVICES):
            i = lax.rem(a // 4 + qx // 2, 2) + 2 * lax.rem(a % 2 + qy, 2)
            fetch.append(pltpu.make_async_copy(in_cost.at[i, lax.rem(a // 2 + qx, 2)], cost.at[a], cost_sem.at[a]))
        run(fetch)
        quarter_tables(tab_a, tab_b)
        finish(fetch)

        def part_of(n):
            a, p = quot(n, parts), rest(n, parts)
            c, q = quot(p, chunk // PART), rest(p, chunk // PART)
            spot = (a, c, pl.ds(pl.multiple_of(rest(q, 4) * PART, PART), PART), half_lanes(quot(q, 4)))
            k = lax.rem(popcount_small(p, 5) + popcount_small(a, 3), 4)
            return a, pl.ds(pl.multiple_of(p * PART, PART), PART), spot, k

        def tile_of(p):
            return pl.ds(pl.multiple_of(rest(p, spots // 2) * 8, 8), 8), half_lanes(quot(p, spots // 2))

        for layer in range(2):
            gamma, beta = [jnp.max(sums[DEVICES + k, layer]) for k in range(2)]
            ch, sh = cos_sin(0.5 * beta)
            cf, sf = cos_sin(beta)

            def phase(n, carry):
                a, r, spot, k = part_of(n)
                t = gamma * cost[a, r]
                vr, vi = jnp.cos(t), -jnp.sin(t)
                qr, qi = (tab_a[k], tab_b[k]) if layer == 0 else (psi[0, *spot], psi[1, *spot])
                psi[0, *spot] = vr * qr - vi * qi
                psi[1, *spot] = vr * qi + vi * qr
                return carry

            lax.fori_loop(0, DEVICES * parts, phase, 0)
            w[...] = rotation_power(ch[0:1, 0:1], -sh[0:1, 0:1], 8, 2.0 ** -4)
            consts = (ch, signed_sines(sh), cf, sf)

            def within(n, carry):
                ref = psi.at[rest(n, 2), quot(n, 2 * CHUNKS), rest(quot(n, 2), CHUNKS)]
                for h in range(2):
                    run_rows(ref, h, consts)
                run_lanes(ref, w)
                return carry

            lax.fori_loop(0, 16 * CHUNKS, within, 0)

            def chunk_bits(n, carry):
                a, p = quot(n, spots), rest(n, spots)
                for k in range(2):
                    v = [psi[k, a, c, *tile_of(p)] for c in range(CHUNKS)]
                    for c, value in enumerate(rotate_pair(*v, cf, sf)):
                        psi[k, a, c, *tile_of(p)] = value
                return carry

            lax.fori_loop(0, DEVICES * spots, chunk_bits, 0)

            def top_bits(n, carry):
                c, p = quot(n, spots), rest(n, spots)
                for k in range(2):
                    v = [psi[k, a, c, *tile_of(p)] for a in range(8)]
                    v = rotate_pair(*v[:4], cf, sf) + rotate_pair(*v[4:], cf, sf)
                    for a in range(4):
                        psi[k, a, c, *tile_of(p)] = ch * v[a] - sh * v[a + 4]
                        psi[k, a + 4, c, *tile_of(p)] = sh * v[a] + ch * v[a + 4]
                return carry

            lax.fori_loop(0, CHUNKS * spots, top_bits, 0)

        def add(n, acc):
            a, r, spot, _ = part_of(n)
            vr, vi = psi[0, *spot], psi[1, *spot]
            return acc + (cost[a, r] * (vr * vr + vi * vi)).reshape(PART // 8, 8, LANES).sum(axis=0)

        total = jnp.sum(lax.fori_loop(0, DEVICES * parts, add, jnp.zeros((8, LANES), jnp.float32)))
        def turn(p, carry):
            _, r, spot, k = part_of((qx * 2 + qy) * parts + p)
            vr, vi, ta, tb = psi[0, *spot], psi[1, *spot], tab_a[k], tab_b[k]
            state[0, r] = ta * vr + tb * vi
            state[1, r] = ta * vi - tb * vr
            return carry

        lax.fori_loop(0, parts, turn, 0)
        finish(run(put_all((state.at[0], state.at[1])) + [put_energy(total)]))


def simulate(cost_rows, gammas, betas):
    rows = cost_rows.shape[0]
    f32 = jnp.float32
    state = jax.ShapeDtypeStruct((rows, LANES), f32)
    near = pl.BlockSpec(memory_space=pl.ANY)
    dma = pltpu.SemaphoreType.DMA
    full = pltpu.VMEM((2, rows, LANES), f32)
    blocks = pltpu.VMEM((2, 4, rows, LANES), f32)
    table = pltpu.VMEM((4, PART, LANES), f32)
    four = dma((CHUNKS,))
    tiles = pltpu.VMEM((DEVICES + 2, 2, 8, LANES), f32)
    halves = pltpu.VMEM((2, 2, CHUNKS, 2 * LANES, LANES), f32)

    def square(*lead):
        return pltpu.VMEM(lead + (2 * LANES, 2 * LANES), f32)

    s_re, s_im, costs, sums = pl.pallas_call(
        gather_kernel,
        out_shape=(state, state, jax.ShapeDtypeStruct((4, 2, rows, LANES), f32),
                   jax.ShapeDtypeStruct((DEVICES + 2, 2, 8, LANES), f32)),
        in_specs=[near, pl.BlockSpec(memory_space=pltpu.SMEM)],
        out_specs=(near,) * 4,
        scratch_shapes=[
            pltpu.VMEM((4, 2, rows, LANES), f32), square(2, 4, CHUNKS), blocks,
            halves, square(2, CHUNKS), halves, full, square(), square(),
            table, table, table, table, pltpu.VMEM((8, LANES), f32), tiles,
            dma, dma((2, 4)), dma((4, 2, 4)), four, four, four, four, dma((4, 4, 2)),
            four, four, four, four, dma((4, 4, 2)), four, four, dma((DEVICES,)), dma((DEVICES,)), dma],
        compiler_params=pltpu.CompilerParams(collective_id=0, has_side_effects=True,
                                             vmem_limit_bytes=52736 << 10),
    )(cost_rows, jnp.concatenate([gammas, betas]))
    return pl.pallas_call(
        final_kernel,
        out_shape=(state, state, jax.ShapeDtypeStruct((1,), f32)),
        in_specs=[near] * 4,
        out_specs=(near,) * 3,
        scratch_shapes=[
            full, pltpu.VMEM((8, rows, LANES), f32), square(2, 8, CHUNKS), square(), table, table,
            tiles, pltpu.SMEM((1,), f32), dma((2, 4)), dma((DEVICES,)), dma((2,))],
        compiler_params=pltpu.CompilerParams(vmem_limit_bytes=52224 << 10),
    )(s_re, s_im, costs, sums)


def popcount(values, bits):
    return sum((values >> b) & 1 for b in range(bits))


def solution(mesh):
    state_spec = P(('inst', 'qx', 'qy'))

    def device_body(cost_local, gammas, betas):
        local_len = cost_local.shape[0]
        s_re, s_im, energy = simulate(cost_local.reshape(local_len // LANES, LANES), gammas, betas)
        return energy, s_re.reshape(local_len), s_im.reshape(local_len)

    return jax.shard_map(device_body, mesh=mesh, in_specs=(state_spec, P(), P()),
                         out_specs=(P('inst'), state_spec, state_spec), check_vma=False)
```

```python
import math
import jax
import jax.numpy as jnp
import numpy as np
from jax import lax
from jax.experimental import pallas as pl
from jax.experimental.pallas import tpu as pltpu
from jax.sharding import PartitionSpec as P

LANES = 128
MESH = pl.DeviceIdType.MESH
HIGHEST = lax.Precision.HIGHEST
ANGLE_MAX = 131072.0
INV_TURN = float(np.float32(1.0 / (2.0 * math.pi)))
TURN_HI = 6.28125
TURN_LO = float(np.float32(2.0 * math.pi - 6.28125))
CHUNKS = 4
BOTH = range(2)
DEVICES = 8
PART = 64

SIN_COEFS = [2 * v / 4.0 ** (2 * k + 1) for k, v in enumerate(
    [1.0, -1.6666654611e-1, 8.3321608736e-3, -1.9515295891e-4])]
COS_COEFS = [2 * v / 16.0 ** k for k, v in enumerate(
    [1.0, -0.5, 4.166664568298827e-2, -1.388731625493765e-3, 2.443315711809948e-5])]


def horner(coefs, z):
    acc = coefs[-1] * z + coefs[-2]
    for v in coefs[-3::-1]:
        acc = acc * z + v
    return acc


def double_phase(cost, gamma, scale, quarter=None, offset=None):
    angle = gamma * cost
    turns = angle * INV_TURN
    if quarter is not None:
        turns = turns - quarter
    n = lax.round(turns, lax.RoundingMethod.TO_NEAREST_EVEN)
    r = (n * TURN_HI - angle) + n * TURN_LO
    if offset is not None:
        r = r + offset
    z = r * r
    s = r * horner(SIN_COEFS, z)
    s2 = s * horner(COS_COEFS, z)
    t2 = scale * s2
    return (scale + scale) - t2 * s2, t2 * (2.0 - s * s)


def rotate_pair(x00, x01, x10, x11, cos_full, sin_full):
    u, v = x00 - x11, x00 + x11
    w, y = x01 + x10, x01 - x10
    u, w = cos_full * u - sin_full * w, sin_full * u + cos_full * w
    return v + u, w + y, w - y, v - u


def quot(a, b):
    return a // b if isinstance(a, int) else lax.div(a, jnp.int32(b))


def rest(a, b):
    return a % b if isinstance(a, int) else lax.rem(a, jnp.int32(b))


def popcount_small(k, bits):
    return sum(rest(quot(k, 1 << b), 2) for b in range(bits))


def rotation_power(cos_half, sin_half, bits, scale):
    n = 1 << bits
    row = lax.broadcasted_iota(jnp.int32, (n, n), 0)
    col = lax.broadcasted_iota(jnp.int32, (n, n), 1)
    acc = jnp.full((n, n), scale, jnp.float32)
    for b in range(bits):
        rb, cb = (row >> b) & 1, (col >> b) & 1
        acc = acc * jnp.where(rb == cb, cos_half, jnp.where(rb > cb, sin_half, -sin_half))
    return acc


def row_gates(arr, cos_half, signed, cos_full, sin_full):
    sub = lax.broadcasted_iota(jnp.int32, arr.shape, 1)
    for b in range(3):
        arr = cos_half * arr + signed[b] * jnp.take_along_axis(arr, sub ^ (1 << b), axis=1)
    v = [arr[k] for k in range(32)]
    for q in (1, 4):
        for k in range(32):
            if (k // q) % 4 == 0:
                quad = (k, k + q, k + 2 * q, k + 3 * q)
                for d, value in zip(quad, rotate_pair(*[v[d] for d in quad], cos_full, sin_full)):
                    v[d] = value
    for k in range(16):
        lo, hi = v[k], v[k + 16]
        v[k], v[k + 16] = cos_half * lo - signed[3] * hi, signed[3] * lo + cos_half * hi
    return v


def loop(start, stop, body, carry, steps=1):
    def turn(n, value):
        for k in range(steps):
            value = body(n * steps + k, value)
        return value
    return lax.fori_loop(start // steps, stop // steps, turn, carry)


def half_lanes(h):
    return pl.ds(pl.multiple_of(h * LANES, LANES), LANES)


def run_rows(ref, h, consts, value=None):
    rows = ref.shape[0]
    value = ref[:, half_lanes(h)] if value is None else value
    v = row_gates(value.reshape(rows // 8, 8, LANES), *consts)
    for k in range(rows // 8):
        ref[pl.ds(8 * k, 8), half_lanes(h)] = v[k]


def run_lanes(ref, w):
    if len(ref.shape) == 2:
        halves = [ref.at[pl.ds(k * LANES, LANES)] for k in BOTH]
    else:
        halves = [ref.at[k] for k in BOTH]
    values = [half[...].reshape(-1, ref.shape[-1]) for half in halves]
    values = [jnp.dot(v, w[...], precision=HIGHEST, preferred_element_type=jnp.float32) for v in values]
    for half, v in zip(halves, values):
        half[...] = v.reshape(half.shape)


def cos_sin(v):
    v = jnp.full((8, LANES), v)
    return jnp.cos(v), jnp.sin(v)


def signed_sines(sin_half):
    sub = lax.broadcasted_iota(jnp.int32, (8, LANES), 0)
    return [jnp.where((sub & (1 << b)) == 0, -sin_half, sin_half) for b in range(3)] + [sin_half]


def quarter_tables(tab_a, tab_b):
    low = (lax.broadcasted_iota(jnp.int32, (PART, LANES), 0) * LANES
           + lax.broadcasted_iota(jnp.int32, (PART, LANES), 1))
    pop = popcount(low, 13)
    for k in range(4):
        q = (pop + k) & 3
        tab_a[k] = jnp.where(q == 0, 1.0, jnp.where(q == 2, -1.0, 0.0))
        tab_b[k] = jnp.where(q == 1, 1.0, jnp.where(q == 3, -1.0, 0.0))
    return pop


def gather_kernel(c_hbm, angles, out_re, out_im, out_cost, out_sums,
                  cost, psi, trig, wave, mixed, part, final, w1, w2,
                  tab_q, tab_o, tab_a, tab_b, cmax, mine,
                  own_sem, out_sem, keep_sem, sx, sy, srx, sry, sc, rx, ry, rdx, rdy, rc, swave, rwave, se, re_sem, sums_sem):
    qx, qy = lax.axis_index("qx"), lax.axis_index("qy")
    x, core = quot(qx, 2), rest(qx, 2)
    rows = c_hbm.shape[0]
    chunk = rows // CHUNKS
    half = chunk // 2

    def dev(dx, dy, dc):
        return {"qx": lax.rem(x + dx, 2) * 2 + lax.rem(core + dc, 2), "qy": lax.rem(qy + dy, 2)}

    xn, yn, cn = dev(1, 0, 0), dev(0, 1, 0), dev(0, 0, 1)

    own_copies = [pltpu.make_async_copy(c_hbm.at[pl.ds(c * chunk, chunk)], cost.at[0, 0, pl.ds(c * chunk, chunk)],
                                        own_sem.at[c]) for c in range(CHUNKS)]
    for cp in own_copies:
        cp.start()
    barrier = pltpu.get_barrier_semaphore()
    for neighbour in (xn, yn, cn):
        pl.semaphore_signal(barrier, inc=1, device_id=neighbour, device_id_type=MESH)

    tile = (8, LANES)
    three = (PART // 8, 8, LANES)
    pl.semaphore_wait(barrier, 3)

    def remote(src, dst, ssem, rsem, device):
        return pltpu.make_async_remote_copy(src_ref=src, dst_ref=dst, send_sem=ssem, recv_sem=rsem,
                                            device_id=device, device_id_type=MESH)

    def rows_of(c):
        return pl.ds(c * chunk, chunk)

    def span(c, h):
        return pl.ds(c * chunk + h * half, half)

    def to_x(c):
        return remote(c_hbm.at[rows_of(c)], cost.at[1, 0, rows_of(c)], sx.at[c], rx.at[c], xn)

    def to_y(c):
        return remote(c_hbm.at[rows_of(c)], cost.at[2, 0, rows_of(c)], sy.at[c], ry.at[c], yn)

    def relay_y(c):
        return remote(cost.at[1, 0, span(c, 0)], cost.at[3, 0, span(c, 0)], sry.at[c], rdy.at[c], yn)

    def relay_x(c):
        return remote(cost.at[2, 0, span(c, 1)], cost.at[3, 0, span(c, 1)], srx.at[c], rdx.at[c], xn)

    def to_core(i, c, h):
        return remote(cost.at[i, 0, span(c, h)], cost.at[i, 1, span(c, h)], sc.at[i, c, h], rc.at[i, c, h], cn)

    def keep(i, k, c):
        return pltpu.make_async_copy(cost.at[i, k, rows_of(c)], out_cost.at[i, k, rows_of(c)], keep_sem.at[i, k, c])

    for c in range(CHUNKS):
        to_x(c).start()
        to_y(c).start()
    for c in range(CHUNKS):
        own_copies[c].wait()
        for h in BOTH:
            to_core(0, c, h).start()

    g1, g2, beta1, beta2 = [angles[k] for k in range(4)]
    for k, v in enumerate(((g1, g2), (beta1, beta2))):
        mine[k + 1] = jnp.concatenate([jnp.full((1, LANES), u) for u in v], axis=0)
    keep_angles = pltpu.make_async_copy(mine.at[pl.ds(1, 2)], out_sums.at[pl.ds(DEVICES, 2)], sums_sem.at[1])
    keep_angles.start()
    ch1, sh1 = cos_sin(0.5 * beta1)
    ch2, sh2 = cos_sin(0.5 * beta2)
    cf1, sf1 = cos_sin(beta1)
    cf2, sf2 = cos_sin(beta2)
    pop = quarter_tables(tab_a, tab_b)
    for k in range(4):
        q = ((pop + k) & 3).astype(jnp.float32)
        tab_q[k] = 0.25 * q
        tab_o[k] = q * float(np.float32(0.5 * math.pi))
    signed1, signed2 = signed_sines(sh1), signed_sines(sh2)

    w1[...] = rotation_power(ch1[0:1, 0:1], -sh1[0:1, 0:1], 8, 2.0 ** -6)
    w2[...] = rotation_power(ch2[0:1, 0:1], -sh2[0:1, 0:1], 8, 2.0 ** -3)
    cmax[...] = jnp.zeros(tile, jnp.float32)

    xf, yf, kf = x.astype(jnp.float32), qy.astype(jnp.float32), core.astype(jnp.float32)
    sign_x, sign_y, sign_k = 2.0 * xf - 1.0, 2.0 * yf - 1.0, 2.0 * kf - 1.0
    flip = sign_x * sign_y
    sx1 = -sign_x * sf1
    sx2, sy2 = sign_x * sh2, sign_y * sh2
    contract = [ch2 * ch2, sx2 * ch2, flip * (ch2 * sy2), flip * (sx2 * sy2)]
    spread = [1.0, 1.0, flip, flip]

    consts1 = (ch1, signed1, cf1, sf1)
    consts2 = (ch2, signed2, cf2, sf2)

    def phases(i, c, own=True, other=True):
        base = c % 2 + c // 2 + (x if i % 2 == 0 else 1 - x) + (qy if i < 2 else 1 - qy)
        ca, cb = spread[i] * ch1, spread[i] * sign_k * sh1
        def body(n, carry):
            r = pl.ds(pl.multiple_of(c * chunk + n * PART, PART), PART)
            spot = (pl.ds(pl.multiple_of(rest(n, 4) * PART, PART), PART), half_lanes(quot(n, 4)))
            terms = []
            for flag, side, coef in ((own, 0, ca), (other, 1, cb)):
                if flag:
                    q = lax.rem(base + popcount_small(n, 3) + (core if side == 0 else 1 - core), 4)
                    terms.append(double_phase(cost[i, side, r].reshape(three), g1, coef,
                                              tab_q[q].reshape(three), tab_o[q].reshape(three)))
            if not own:
                terms.append([psi[k, i, c, *spot].reshape(three) for k in BOTH])
            for k in BOTH:
                u = terms[0][k] if len(terms) == 1 else terms[0][k] + terms[1][k]
                psi[k, i, c, *spot] = u.reshape(PART, LANES)
            if own:
                v = cost[i, 0, r].reshape(three)
                for k, u in enumerate(double_phase(v, g2, contract[i])):
                    trig[k, i, r] = u.reshape(PART, LANES)
                if i == 0:
                    cmax[...] = jnp.maximum(cmax[...], jnp.abs(v).max(axis=0))
            return carry

        loop(0, chunk // PART, body, 0, 2)

    def rows_loop(i, c):
        def body(n, carry):
            run_rows(psi.at[quot(n, 2), i, c], rest(n, 2), consts1)
            return carry
        lax.fori_loop(0, 4, body, 0)

    def place(p):
        return pl.ds(pl.multiple_of(rest(p, half // 8) * 8, 8), 8), half_lanes(quot(p, half // 8))

    def chunk_bits(p, carry):
        for k in BOTH:
            for i in range(3):
                v = rotate_pair(*[psi[k, i, c, *place(p)] for c in range(CHUNKS)], cf1, sf1)
                for c in range(CHUNKS):
                    psi[k, i, c, *place(p)] = v[c]
        return carry

    def arrived(i, c):
        if i == 1 or i == 2:
            (to_x if i == 1 else to_y)(c).wait_recv()
            (relay_y if i == 1 else relay_x)(c).start()
        if i == 3:
            relay_y(c).wait_recv()
            to_core(i, c, 0).start()
            relay_x(c).wait_recv()
            to_core(i, c, 1).start()
        elif i > 0:
            for h in BOTH:
                to_core(i, c, h).start()
        keep(i, 0, c).start()

    def other_arrived(i, c):
        for h in BOTH:
            to_core(i, c, h).wait_recv()
        keep(i, 1, c).start()

    def unit(i, c):
        other_arrived(i, c)
        phases(i, c)
        rows_loop(i, c)

    for c in range(CHUNKS):
        arrived(0, c)
        unit(0, c)
        if c % 2 == 1:
            run_lanes(psi.at[:, 0, pl.ds(c - 1, 2)], w1)
    for c in range(CHUNKS):
        for i in (1, 2):
            arrived(i, c)
        for i in (1, 2):
            unit(i, c)
        run_lanes(psi.at[:, pl.ds(1, 2), c], w1)
    arrived(3, 0)
    loop(0, chunk // 8, chunk_bits, 0, 4)
    arrived(3, 1)
    unit(3, 0)
    unit(3, 1)
    arrived(3, 2)
    run_lanes(psi.at[:, 3, pl.ds(0, 2)], w1)
    unit(3, 2)
    arrived(3, 3)
    run_lanes(psi.at[:, 3, 2], w1)
    phases(3, 3, other=False)
    other_arrived(3, 3)
    phases(3, 3, own=False)
    rows_loop(3, 3)
    run_lanes(psi.at[:, 3, 3], w1)

    def tail(p, carry):
        r = [pl.ds(pl.multiple_of(c * chunk + p * 8, 8), 8) for c in range(CHUNKS)]
        diag = [rotate_pair(*[psi[k, 3, c, *place(p)] for c in range(CHUNKS)], cf1, sf1) for k in BOTH]
        z = [[], []]
        for c in range(CHUNKS):
            v = [rotate_pair(*[psi[k, i, c, *place(p)] for i in (0, 2, 1)], diag[k][c], cf1, sx1) for k in BOTH]
            sums = None
            for n, i in enumerate((0, 2, 1, 3)):
                (re, im), (tr, ti) = (v[0][n], v[1][n]), (trig[0, i, r[c]], trig[1, i, r[c]])
                term = (re * tr - im * ti, re * ti + im * tr)
                sums = term if sums is None else (sums[0] + term[0], sums[1] + term[1])
            z[0].append(sums[0])
            z[1].append(sums[1])
        for k in BOTH:
            for c, value in enumerate(rotate_pair(*z[k], cf2, sf2)):
                wave[quot(p, half // 8), k, c, place(p)[0]] = value
        return carry

    def swap(n):
        spot = (n // 4, slice(None), slice(None), pl.ds(n % 4 * PART, PART))
        return remote(wave.at[*spot], part.at[*spot], swave.at[n], rwave.at[n], cn)

    piece = PART // 8
    for n in range(DEVICES):
        loop(n * piece, (n + 1) * piece, tail, 0, 2)
        swap(n).start()

    sk2 = sign_k * sh2
    for h in BOTH:
        for n in range(4):
            swap(4 * h + n).wait_recv()

        def turn(n, carry, h=h):
            k, c = quot(n, CHUNKS), rest(n, CHUNKS)
            shape = (half // 8, 8, LANES)
            run_rows(mixed.at[k, c], h, consts2, ch2 * wave[h, k, c].reshape(shape) + sk2 * part[h, k, c].reshape(shape))
            return carry

        lax.fori_loop(0, 2 * CHUNKS, turn, 0)

    energy = jnp.zeros(tile, jnp.float32)
    outs = []
    for c in range(CHUNKS):
        if c % 2 == 0:
            run_lanes(mixed.at[:, pl.ds(c, 2)], w2)

        def last(p, acc, c=c):
            r = pl.ds(pl.multiple_of(c * chunk + p * PART, PART), PART)
            spot = (pl.ds(pl.multiple_of(rest(p, 4) * PART, PART), PART), half_lanes(quot(p, 4)))
            vr, vi = [mixed[k, c, *spot] for k in BOTH]
            k = lax.rem(popcount_small(p, 3) + c % 2 + c // 2 + x + qy + core, 4)
            final[0, r] = tab_a[k] * vr + tab_b[k] * vi
            final[1, r] = tab_a[k] * vi - tab_b[k] * vr
            return acc + (cost[0, 0, r] * (vr * vr + vi * vi)).reshape(three).sum(axis=0)

        energy = loop(0, chunk // PART, last, energy, 4)
        for k, out in enumerate((out_re, out_im)):
            cp = pltpu.make_async_copy(final.at[k, rows_of(c)], out.at[rows_of(c)], out_sem.at[k, c])
            cp.start()
            outs.append(cp)

    me = qy * 4 + qx
    largest = cmax[...].max(axis=0, keepdims=True) * jnp.maximum(jnp.abs(g1), jnp.abs(g2))
    mine[0] = jnp.concatenate([energy.sum(axis=0, keepdims=True), largest], axis=0)
    sends = [remote(mine.at[0], out_sums.at[me], se.at[n], re_sem.at[n], dev(n // 4, (n // 2) % 2, n % 2))
             for n in range(1, DEVICES)]
    for cp in sends:
        cp.start()
    keep_mine = pltpu.make_async_copy(mine.at[0], out_sums.at[me], sums_sem.at[0])
    keep_mine.start()
    outs += [keep_mine, keep_angles]
    for c in range(CHUNKS):
        to_x(c).wait_send()
        to_y(c).wait_send()
        relay_x(c).wait_send()
        relay_y(c).wait_send()
        swap(c).wait_send()
        swap(c + CHUNKS).wait_send()
        for i in range(4):
            for k in BOTH:
                to_core(i, c, k).wait_send()
                keep(i, k, c).wait()
    for cp in outs:
        cp.wait()
    for cp in sends:
        cp.wait()


def final_kernel(in_re, in_im, in_cost, in_sums, out_re, out_im, out_energy,
                 state, cost, psi, w, tab_a, tab_b, sums, energy, out_sem, cost_sem, small_sem):
    rows = in_re.shape[0]
    chunk = rows // CHUNKS
    parts, spots = rows // PART, chunk // 8
    outs = (out_re, out_im)

    def put(k, c, src):
        r = pl.ds(c * chunk, chunk)
        return pltpu.make_async_copy(src.at[r], outs[k].at[r], out_sem.at[k, c])

    def put_all(srcs):
        return [put(k, c, srcs[k]) for c in range(CHUNKS) for k in BOTH]

    def put_energy(total):
        energy[0] = total * (1.0 / (DEVICES * rows * LANES))
        return pltpu.make_async_copy(energy, out_energy, small_sem.at[1])

    def run(copies):
        for cp in copies:
            cp.start()
        return copies

    def finish(copies):
        for cp in copies:
            cp.wait()

    moves = run(put_all((in_re, in_im)))
    finish(run([pltpu.make_async_copy(in_sums, sums, small_sem.at[0])]))
    both = [sums[n] for n in range(DEVICES)]
    total = sum(v[:1] for v in both[1:]) + both[0][:1]
    moves += run([put_energy(jnp.sum(total))])
    small = jnp.max(jnp.stack(both)[:, 1:]) <= ANGLE_MAX
    finish(moves)

    @pl.when(jnp.logical_not(small))
    def _():
        qx, qy = lax.axis_index("qx"), lax.axis_index("qy")
        fetch = []
        for a in range(DEVICES):
            i = lax.rem(a // 4 + qx // 2, 2) + 2 * lax.rem(a % 2 + qy, 2)
            fetch.append(pltpu.make_async_copy(in_cost.at[i, lax.rem(a // 2 + qx, 2)], cost.at[a], cost_sem.at[a]))
        run(fetch)
        quarter_tables(tab_a, tab_b)
        finish(fetch)

        def part_of(n):
            a, p = quot(n, parts), rest(n, parts)
            c, q = quot(p, chunk // PART), rest(p, chunk // PART)
            spot = (a, c, pl.ds(pl.multiple_of(rest(q, 4) * PART, PART), PART), half_lanes(quot(q, 4)))
            k = lax.rem(popcount_small(p, 5) + popcount_small(a, 3), 4)
            return a, pl.ds(pl.multiple_of(p * PART, PART), PART), spot, k

        def tile_of(p):
            return pl.ds(pl.multiple_of(rest(p, spots // 2) * 8, 8), 8), half_lanes(quot(p, spots // 2))

        for layer in BOTH:
            gamma, beta = [jnp.max(sums[DEVICES + k][layer:layer + 1]) for k in BOTH]
            ch, sh = cos_sin(0.5 * beta)
            cf, sf = cos_sin(beta)

            def phase(n, carry):
                a, r, spot, k = part_of(n)
                t = gamma * cost[a, r]
                vr, vi = jnp.cos(t), -jnp.sin(t)
                qr, qi = (tab_a[k], tab_b[k]) if layer == 0 else (psi[0, *spot], psi[1, *spot])
                psi[0, *spot] = vr * qr - vi * qi
                psi[1, *spot] = vr * qi + vi * qr
                return carry

            lax.fori_loop(0, DEVICES * parts, phase, 0)
            w[...] = rotation_power(ch[0:1, 0:1], -sh[0:1, 0:1], 8, 2.0 ** -4)
            consts = (ch, signed_sines(sh), cf, sf)

            def within(n, carry):
                ref = psi.at[rest(n, 2), quot(n, 2 * CHUNKS), rest(quot(n, 2), CHUNKS)]
                for h in BOTH:
                    run_rows(ref, h, consts)
                run_lanes(ref, w)
                return carry

            lax.fori_loop(0, 16 * CHUNKS, within, 0)

            def chunk_bits(n, carry):
                a, p = quot(n, spots), rest(n, spots)
                for k in BOTH:
                    v = [psi[k, a, c, *tile_of(p)] for c in range(CHUNKS)]
                    for c, value in enumerate(rotate_pair(*v, cf, sf)):
                        psi[k, a, c, *tile_of(p)] = value
                return carry

            lax.fori_loop(0, DEVICES * spots, chunk_bits, 0)

            def top_bits(n, carry):
                c, p = quot(n, spots), rest(n, spots)
                for k in BOTH:
                    v = [psi[k, a, c, *tile_of(p)] for a in range(8)]
                    v = rotate_pair(*v[:4], cf, sf) + rotate_pair(*v[4:], cf, sf)
                    for a in range(4):
                        psi[k, a, c, *tile_of(p)] = ch * v[a] - sh * v[a + 4]
                        psi[k, a + 4, c, *tile_of(p)] = sh * v[a] + ch * v[a + 4]
                return carry

            lax.fori_loop(0, CHUNKS * spots, top_bits, 0)

        def add(n, acc):
            a, r, spot, _ = part_of(n)
            vr, vi = psi[0, *spot], psi[1, *spot]
            return acc + (cost[a, r] * (vr * vr + vi * vi)).reshape(PART // 8, 8, LANES).sum(axis=0)

        total = jnp.sum(lax.fori_loop(0, DEVICES * parts, add, jnp.zeros((8, LANES), jnp.float32)))
        def turn(p, carry):
            _, r, spot, k = part_of((qx * 2 + qy) * parts + p)
            vr, vi, ta, tb = psi[0, *spot], psi[1, *spot], tab_a[k], tab_b[k]
            state[0, r] = ta * vr + tb * vi
            state[1, r] = ta * vi - tb * vr
            return carry

        lax.fori_loop(0, parts, turn, 0)
        finish(run(put_all((state.at[0], state.at[1])) + [put_energy(total)]))


def simulate(cost_rows, gammas, betas):
    rows = cost_rows.shape[0]
    f32 = jnp.float32
    state = jax.ShapeDtypeStruct((rows, LANES), f32)
    near = pl.BlockSpec(memory_space=pl.ANY)
    dma = pltpu.SemaphoreType.DMA
    full = pltpu.VMEM((2, rows, LANES), f32)
    blocks = pltpu.VMEM((2, 4, rows, LANES), f32)
    table = pltpu.VMEM((4, PART, LANES), f32)
    four, eight = dma((CHUNKS,)), dma((DEVICES,))
    tiles = pltpu.VMEM((DEVICES + 2, 2, LANES), f32)
    halves = pltpu.VMEM((2, 2, CHUNKS, 2 * LANES, LANES), f32)

    def square(*lead):
        return pltpu.VMEM(lead + (2 * LANES, 2 * LANES), f32)

    s_re, s_im, costs, sums = pl.pallas_call(
        gather_kernel,
        out_shape=(state, state, jax.ShapeDtypeStruct((4, 2, rows, LANES), f32),
                   jax.ShapeDtypeStruct((DEVICES + 2, 2, LANES), f32)),
        in_specs=[near, pl.BlockSpec(memory_space=pltpu.SMEM)],
        out_specs=(near,) * 4,
        scratch_shapes=[
            pltpu.VMEM((4, 2, rows, LANES), f32), square(2, 4, CHUNKS), blocks,
            halves, square(2, CHUNKS), halves, full, square(), square(),
            table, table, table, table, pltpu.VMEM((8, LANES), f32), pltpu.VMEM((3, 2, LANES), f32),
            four, dma((2, 4)), dma((4, 2, 4)), four, four, four, four, dma((4, 4, 2)),
            four, four, four, four, dma((4, 4, 2)), eight, eight, eight, eight, dma((2,))],
        compiler_params=pltpu.CompilerParams(collective_id=0, has_side_effects=True,
                                             vmem_limit_bytes=52736 << 10),
    )(cost_rows, jnp.concatenate([gammas, betas]))
    return pl.pallas_call(
        final_kernel,
        out_shape=(state, state, jax.ShapeDtypeStruct((1,), f32)),
        in_specs=[near] * 4,
        out_specs=(near,) * 3,
        scratch_shapes=[
            full, pltpu.VMEM((8, rows, LANES), f32), square(2, 8, CHUNKS), square(), table, table,
            tiles, pltpu.SMEM((1,), f32), dma((2, 4)), dma((DEVICES,)), dma((2,))],
        compiler_params=pltpu.CompilerParams(vmem_limit_bytes=52224 << 10),
    )(s_re, s_im, costs, sums)


def popcount(values, bits):
    return sum((values >> b) & 1 for b in range(bits))


def solution(mesh):
    state_spec = P(('inst', 'qx', 'qy'))

    def device_body(cost_local, gammas, betas):
        local_len = cost_local.shape[0]
        s_re, s_im, energy = simulate(cost_local.reshape(local_len // LANES, LANES), gammas, betas)
        return energy, s_re.reshape(local_len), s_im.reshape(local_len)

    return jax.shard_map(device_body, mesh=mesh, in_specs=(state_spec, P(), P()),
                         out_specs=(P('inst'), state_spec, state_spec), check_vma=False)
```

```python
import math
import jax
import jax.numpy as jnp
import numpy as np
from jax import lax
from jax.experimental import pallas as pl
from jax.experimental.pallas import tpu as pltpu
from jax.sharding import PartitionSpec as P

LANES = 128
MESH = pl.DeviceIdType.MESH
HIGHEST = lax.Precision.HIGHEST
ANGLE_MAX = 131072.0
INV_TURN = float(np.float32(1.0 / (2.0 * math.pi)))
TURN_HI = 6.28125
TURN_LO = float(np.float32(2.0 * math.pi - 6.28125))
CHUNKS = 4
BOTH = range(2)
DEVICES = 8
PART = 64

SIN_COEFS = [2 * v / 4.0 ** (2 * k + 1) for k, v in enumerate(
    [1.0, -1.6666654611e-1, 8.3321608736e-3, -1.9515295891e-4])]
COS_COEFS = [2 * v / 16.0 ** k for k, v in enumerate(
    [1.0, -0.5, 4.166664568298827e-2, -1.388731625493765e-3, 2.443315711809948e-5])]


def horner(coefs, z):
    acc = coefs[-1] * z + coefs[-2]
    for v in coefs[-3::-1]:
        acc = acc * z + v
    return acc


def double_phase(cost, gamma, scale, quarter=None, offset=None):
    angle = gamma * cost
    turns = angle * INV_TURN
    if quarter is not None:
        turns = turns - quarter
    n = lax.round(turns, lax.RoundingMethod.TO_NEAREST_EVEN)
    r = (n * TURN_HI - angle) + n * TURN_LO
    if offset is not None:
        r = r + offset
    z = r * r
    s = r * horner(SIN_COEFS, z)
    s2 = s * horner(COS_COEFS, z)
    t2 = scale * s2
    return (scale + scale) - t2 * s2, t2 * (2.0 - s * s)


def rotate_pair(x00, x01, x10, x11, cos_full, sin_full):
    u, v = x00 - x11, x00 + x11
    w, y = x01 + x10, x01 - x10
    u, w = cos_full * u - sin_full * w, sin_full * u + cos_full * w
    return v + u, w + y, w - y, v - u


def quot(a, b):
    return a // b if isinstance(a, int) else lax.div(a, jnp.int32(b))


def rest(a, b):
    return a % b if isinstance(a, int) else lax.rem(a, jnp.int32(b))


def popcount_small(k, bits):
    return sum(rest(quot(k, 1 << b), 2) for b in range(bits))


def rotation_power(cos_half, sin_half, bits, scale):
    n = 1 << bits
    row = lax.broadcasted_iota(jnp.int32, (n, n), 0)
    col = lax.broadcasted_iota(jnp.int32, (n, n), 1)
    acc = jnp.full((n, n), scale, jnp.float32)
    for b in range(bits):
        rb, cb = (row >> b) & 1, (col >> b) & 1
        acc = acc * jnp.where(rb == cb, cos_half, jnp.where(rb > cb, sin_half, -sin_half))
    return acc


def row_gates(arr, cos_half, signed, cos_full, sin_full):
    sub = lax.broadcasted_iota(jnp.int32, arr.shape, 1)
    for b in range(3):
        arr = cos_half * arr + signed[b] * jnp.take_along_axis(arr, sub ^ (1 << b), axis=1)
    v = [arr[k] for k in range(32)]
    for q in (1, 4):
        for k in range(32):
            if (k // q) % 4 == 0:
                quad = (k, k + q, k + 2 * q, k + 3 * q)
                for d, value in zip(quad, rotate_pair(*[v[d] for d in quad], cos_full, sin_full)):
                    v[d] = value
    for k in range(16):
        lo, hi = v[k], v[k + 16]
        v[k], v[k + 16] = cos_half * lo - signed[3] * hi, signed[3] * lo + cos_half * hi
    return v


def loop(start, stop, body, carry, steps=1):
    def turn(n, value):
        for k in range(steps):
            value = body(n * steps + k, value)
        return value
    return lax.fori_loop(start // steps, stop // steps, turn, carry)


def half_lanes(h):
    return pl.ds(pl.multiple_of(h * LANES, LANES), LANES)


def run_rows(ref, h, consts, value=None):
    rows = ref.shape[0]
    value = ref[:, half_lanes(h)] if value is None else value
    v = row_gates(value.reshape(rows // 8, 8, LANES), *consts)
    for k in range(rows // 8):
        ref[pl.ds(8 * k, 8), half_lanes(h)] = v[k]


def run_lanes(ref, w):
    if len(ref.shape) == 2:
        halves = [ref.at[pl.ds(k * LANES, LANES)] for k in BOTH]
    else:
        halves = [ref.at[k] for k in BOTH]
    values = [half[...].reshape(-1, ref.shape[-1]) for half in halves]
    values = [jnp.dot(v, w[...], precision=HIGHEST, preferred_element_type=jnp.float32) for v in values]
    for half, v in zip(halves, values):
        half[...] = v.reshape(half.shape)


def cos_sin(v):
    v = jnp.full((8, LANES), v)
    return jnp.cos(v), jnp.sin(v)


def signed_sines(sin_half):
    sub = lax.broadcasted_iota(jnp.int32, (8, LANES), 0)
    return [jnp.where((sub & (1 << b)) == 0, -sin_half, sin_half) for b in range(3)] + [sin_half]


def quarter_tables(tab_a, tab_b):
    low = (lax.broadcasted_iota(jnp.int32, (PART, LANES), 0) * LANES
           + lax.broadcasted_iota(jnp.int32, (PART, LANES), 1))
    pop = popcount(low, 13)
    for k in range(4):
        q = (pop + k) & 3
        tab_a[k] = jnp.where(q == 0, 1.0, jnp.where(q == 2, -1.0, 0.0))
        tab_b[k] = jnp.where(q == 1, 1.0, jnp.where(q == 3, -1.0, 0.0))
    return pop


def gather_kernel(c_hbm, angles_any, out_re, out_im, out_cost, out_sums,
                  cost, psi, trig, wave, mixed, part, final, w1, w2,
                  tab_q, tab_o, tab_a, tab_b, cmax, mine, angles,
                  own_sem, out_sem, keep_sem, sx, sy, srx, sry, sc, rx, ry, rdx, rdy, rc, swave, rwave, se, re_sem, sums_sem, angle_sem):
    qx, qy = lax.axis_index("qx"), lax.axis_index("qy")
    x, core = quot(qx, 2), rest(qx, 2)
    rows = c_hbm.shape[0]
    chunk = rows // CHUNKS
    half = chunk // 2

    def dev(dx, dy, dc):
        return {"qx": lax.rem(x + dx, 2) * 2 + lax.rem(core + dc, 2), "qy": lax.rem(qy + dy, 2)}

    xn, yn, cn = dev(1, 0, 0), dev(0, 1, 0), dev(0, 0, 1)

    own_copy = pltpu.make_async_copy(c_hbm, cost.at[0, 0], own_sem)
    own_copy.start()
    angle_copy = pltpu.make_async_copy(angles_any, angles, angle_sem)
    angle_copy.start()
    barrier = pltpu.get_barrier_semaphore()
    for neighbour in (xn, yn, cn):
        pl.semaphore_signal(barrier, inc=1, device_id=neighbour, device_id_type=MESH)

    tile = (8, LANES)
    three = (PART // 8, 8, LANES)
    pl.semaphore_wait(barrier, 3)

    def remote(src, dst, ssem, rsem, device):
        return pltpu.make_async_remote_copy(src_ref=src, dst_ref=dst, send_sem=ssem, recv_sem=rsem,
                                            device_id=device, device_id_type=MESH)

    def rows_of(c):
        return pl.ds(c * chunk, chunk)

    def span(c, h):
        return pl.ds(c * chunk + h * half, half)

    def to_x(c):
        return remote(c_hbm.at[rows_of(c)], cost.at[1, 0, rows_of(c)], sx, rx.at[c], xn)

    def to_y(c):
        return remote(c_hbm.at[rows_of(c)], cost.at[2, 0, rows_of(c)], sy, ry.at[c], yn)

    def relay_y(c):
        return remote(cost.at[1, 0, span(c, 0)], cost.at[3, 0, span(c, 0)], sry, rdy.at[c], yn)

    def relay_x(c):
        return remote(cost.at[2, 0, span(c, 1)], cost.at[3, 0, span(c, 1)], srx, rdx.at[c], xn)

    def to_core(i, c):
        return remote(cost.at[i, 0, rows_of(c)], cost.at[i, 1, rows_of(c)], sc, rc.at[i, c], cn)

    def keep(i, k, c):
        return pltpu.make_async_copy(cost.at[i, k, rows_of(c)], out_cost.at[i, k, rows_of(c)], keep_sem)

    for c in range(CHUNKS):
        to_x(c).start()
        to_y(c).start()
    own_copy.wait()
    for c in range(CHUNKS):
        to_core(0, c).start()

    angle_copy.wait()
    g1, g2, beta1, beta2 = [angles[k] for k in range(4)]
    for k, v in enumerate(((g1, g2), (beta1, beta2))):
        mine[k + 1] = jnp.concatenate([jnp.full((1, LANES), u) for u in v], axis=0)
    keep_angles = pltpu.make_async_copy(mine.at[pl.ds(1, 2)], out_sums.at[pl.ds(DEVICES, 2)], sums_sem.at[1])
    keep_angles.start()
    ch1, sh1 = cos_sin(0.5 * beta1)
    ch2, sh2 = cos_sin(0.5 * beta2)
    cf1, sf1 = cos_sin(beta1)
    cf2, sf2 = cos_sin(beta2)
    pop = quarter_tables(tab_a, tab_b)
    for k in range(4):
        q = ((pop + k) & 3).astype(jnp.float32)
        tab_q[k] = 0.25 * q
        tab_o[k] = q * float(np.float32(0.5 * math.pi))
    signed1, signed2 = signed_sines(sh1), signed_sines(sh2)

    w1[...] = rotation_power(ch1[0:1, 0:1], -sh1[0:1, 0:1], 8, 2.0 ** -6)
    w2[...] = rotation_power(ch2[0:1, 0:1], -sh2[0:1, 0:1], 8, 2.0 ** -3)
    cmax[...] = jnp.zeros(tile, jnp.float32)

    xf, yf, kf = x.astype(jnp.float32), qy.astype(jnp.float32), core.astype(jnp.float32)
    sign_x, sign_y, sign_k = 2.0 * xf - 1.0, 2.0 * yf - 1.0, 2.0 * kf - 1.0
    flip = sign_x * sign_y
    sx1 = -sign_x * sf1
    sx2, sy2 = sign_x * sh2, sign_y * sh2
    contract = [ch2 * ch2, sx2 * ch2, flip * (ch2 * sy2), flip * (sx2 * sy2)]
    spread = [1.0, 1.0, flip, flip]

    consts1 = (ch1, signed1, cf1, sf1)
    consts2 = (ch2, signed2, cf2, sf2)

    def phases(i, c, own=True, other=True):
        base = c % 2 + c // 2 + (x if i % 2 == 0 else 1 - x) + (qy if i < 2 else 1 - qy)
        ca, cb = spread[i] * ch1, spread[i] * sign_k * sh1
        def body(n, carry):
            r = pl.ds(pl.multiple_of(c * chunk + n * PART, PART), PART)
            spot = (pl.ds(pl.multiple_of(rest(n, 4) * PART, PART), PART), half_lanes(quot(n, 4)))
            terms = []
            for flag, side, coef in ((own, 0, ca), (other, 1, cb)):
                if flag:
                    q = lax.rem(base + popcount_small(n, 3) + (core if side == 0 else 1 - core), 4)
                    terms.append(double_phase(cost[i, side, r].reshape(three), g1, coef,
                                              tab_q[q].reshape(three), tab_o[q].reshape(three)))
            if not own:
                terms.append([psi[k, i, c, *spot].reshape(three) for k in BOTH])
            for k in BOTH:
                u = terms[0][k] if len(terms) == 1 else terms[0][k] + terms[1][k]
                psi[k, i, c, *spot] = u.reshape(PART, LANES)
            if own:
                v = cost[i, 0, r].reshape(three)
                for k, u in enumerate(double_phase(v, g2, contract[i])):
                    trig[k, i, r] = u.reshape(PART, LANES)
                if i == 0:
                    cmax[...] = jnp.maximum(cmax[...], jnp.abs(v).max(axis=0))
            return carry

        loop(0, chunk // PART, body, 0, 2)

    def rows_loop(i, c):
        def body(n, carry):
            run_rows(psi.at[quot(n, 2), i, c], rest(n, 2), consts1)
            return carry
        lax.fori_loop(0, 4, body, 0)

    def place(p):
        return pl.ds(pl.multiple_of(rest(p, half // 8) * 8, 8), 8), half_lanes(quot(p, half // 8))

    def chunk_bits(p, carry):
        for k in BOTH:
            for i in range(3):
                v = rotate_pair(*[psi[k, i, c, *place(p)] for c in range(CHUNKS)], cf1, sf1)
                for c in range(CHUNKS):
                    psi[k, i, c, *place(p)] = v[c]
        return carry

    def arrived(i, c):
        if i == 1 or i == 2:
            (to_x if i == 1 else to_y)(c).wait_recv()
            (relay_y if i == 1 else relay_x)(c).start()
        if i == 3:
            relay_y(c).wait_recv()
            relay_x(c).wait_recv()
        if i > 0:
            to_core(i, c).start()
        keep(i, 0, c).start()

    def other_arrived(i, c):
        to_core(i, c).wait_recv()
        keep(i, 1, c).start()

    def unit(i, c):
        other_arrived(i, c)
        phases(i, c)
        rows_loop(i, c)

    for c in range(CHUNKS):
        arrived(0, c)
        unit(0, c)
        if c % 2 == 1:
            run_lanes(psi.at[:, 0, pl.ds(c - 1, 2)], w1)
    for c in range(CHUNKS):
        for i in (1, 2):
            arrived(i, c)
        for i in (1, 2):
            unit(i, c)
        run_lanes(psi.at[:, pl.ds(1, 2), c], w1)
    arrived(3, 0)
    loop(0, chunk // 8, chunk_bits, 0, 4)
    arrived(3, 1)
    unit(3, 0)
    unit(3, 1)
    arrived(3, 2)
    run_lanes(psi.at[:, 3, pl.ds(0, 2)], w1)
    unit(3, 2)
    arrived(3, 3)
    run_lanes(psi.at[:, 3, 2], w1)
    phases(3, 3, other=False)
    other_arrived(3, 3)
    phases(3, 3, own=False)
    rows_loop(3, 3)
    run_lanes(psi.at[:, 3, 3], w1)

    def tail(p, carry):
        r = [pl.ds(pl.multiple_of(c * chunk + p * 8, 8), 8) for c in range(CHUNKS)]
        diag = [rotate_pair(*[psi[k, 3, c, *place(p)] for c in range(CHUNKS)], cf1, sf1) for k in BOTH]
        z = [[], []]
        for c in range(CHUNKS):
            v = [rotate_pair(*[psi[k, i, c, *place(p)] for i in (0, 2, 1)], diag[k][c], cf1, sx1) for k in BOTH]
            sums = None
            for n, i in enumerate((0, 2, 1, 3)):
                (re, im), (tr, ti) = (v[0][n], v[1][n]), (trig[0, i, r[c]], trig[1, i, r[c]])
                term = (re * tr - im * ti, re * ti + im * tr)
                sums = term if sums is None else (sums[0] + term[0], sums[1] + term[1])
            z[0].append(sums[0])
            z[1].append(sums[1])
        for k in BOTH:
            for c, value in enumerate(rotate_pair(*z[k], cf2, sf2)):
                wave[quot(p, half // 8), k, c, place(p)[0]] = value
        return carry

    def swap(n):
        spot = (quot(n, 4), slice(None), slice(None), pl.ds(pl.multiple_of(rest(n, 4) * PART, PART), PART))
        return remote(wave.at[*spot], part.at[*spot], swave, rwave.at[quot(n, 4)], cn)

    def piece(n, carry):
        loop(0, PART // 8, lambda p, v: tail(n * (PART // 8) + p, v), 0, 4)
        swap(n).start()
        return carry

    lax.fori_loop(0, DEVICES, piece, 0)

    sk2 = sign_k * sh2
    for h in BOTH:
        remote(wave.at[h], part.at[h], swave, rwave.at[h], cn).wait_recv()

        def turn(n, carry, h=h):
            k, c = quot(n, CHUNKS), rest(n, CHUNKS)
            shape = (half // 8, 8, LANES)
            run_rows(mixed.at[k, c], h, consts2, ch2 * wave[h, k, c].reshape(shape) + sk2 * part[h, k, c].reshape(shape))
            return carry

        lax.fori_loop(0, 2 * CHUNKS, turn, 0)

    energy = jnp.zeros(tile, jnp.float32)
    for c in range(CHUNKS):
        if c == 0:
            run_lanes(mixed, w2)

        def last(p, acc, c=c):
            r = pl.ds(pl.multiple_of(c * chunk + p * PART, PART), PART)
            spot = (pl.ds(pl.multiple_of(rest(p, 4) * PART, PART), PART), half_lanes(quot(p, 4)))
            vr, vi = [mixed[k, c, *spot] for k in BOTH]
            k = lax.rem(popcount_small(p, 3) + c % 2 + c // 2 + x + qy + core, 4)
            final[0, r] = tab_a[k] * vr + tab_b[k] * vi
            final[1, r] = tab_a[k] * vi - tab_b[k] * vr
            return acc + (cost[0, 0, r] * (vr * vr + vi * vi)).reshape(three).sum(axis=0)

        energy = loop(0, chunk // PART, last, energy, 4)
        for k, out in enumerate((out_re, out_im)):
            pltpu.make_async_copy(final.at[k, rows_of(c)], out.at[rows_of(c)], out_sem.at[k]).start()

    me = qy * 4 + qx
    largest = cmax[...].max(axis=0, keepdims=True) * jnp.maximum(jnp.abs(g1), jnp.abs(g2))
    mine[0] = jnp.concatenate([energy.sum(axis=0, keepdims=True), largest], axis=0)
    sends = [remote(mine.at[0], out_sums.at[me], se, re_sem, dev(n // 4, (n // 2) % 2, n % 2))
             for n in range(1, DEVICES)]
    for cp in sends:
        cp.start()
    keep_mine = pltpu.make_async_copy(mine.at[0], out_sums.at[me], sums_sem.at[0])
    keep_mine.start()
    outs = [keep_mine, keep_angles, pltpu.make_async_copy(cost, out_cost, keep_sem)]
    outs += [pltpu.make_async_copy(final.at[k], out, out_sem.at[k]) for k, out in enumerate((out_re, out_im))]
    spot, others = pl.ds(0, rows // 2), out_sums.at[pl.ds(0, DEVICES - 1)]
    for src, dst, sem in ((c_hbm, cost.at[1, 0], sx), (c_hbm, cost.at[2, 0], sy),
                          (cost.at[1, 0, spot], cost.at[3, 0, spot], sry),
                          (cost.at[2, 0, spot], cost.at[3, 0, spot], srx),
                          (cost.at[:, 0], cost.at[:, 1], sc), (wave, part, swave)):
        remote(src, dst, sem, re_sem, cn).wait_send()
    for cp in outs:
        cp.wait()
    remote(others, others, se, re_sem, cn).wait()


def final_kernel(in_re, in_im, in_cost, in_sums, out_re, out_im, out_energy,
                 state, cost, psi, w, tab_a, tab_b, sums, energy, out_sem, cost_sem, small_sem):
    rows = in_re.shape[0]
    chunk = rows // CHUNKS
    parts, spots = rows // PART, chunk // 8
    outs = (out_re, out_im)

    def put_all(srcs):
        return [pltpu.make_async_copy(srcs[k], outs[k], out_sem.at[k]) for k in BOTH]

    def put_energy(total):
        energy[0] = total * (1.0 / (DEVICES * rows * LANES))
        return pltpu.make_async_copy(energy, out_energy, small_sem.at[1])

    def run(copies):
        for cp in copies:
            cp.start()
        return copies

    def finish(copies):
        for cp in copies:
            cp.wait()

    moves = run(put_all((in_re, in_im)))
    finish(run([pltpu.make_async_copy(in_sums, sums, small_sem.at[0])]))
    both = [sums[n] for n in range(DEVICES)]
    total = sum(v[:1] for v in both[1:]) + both[0][:1]
    moves += run([put_energy(jnp.sum(total))])
    small = jnp.max(jnp.stack(both)[:, 1:]) <= ANGLE_MAX
    finish(moves)

    @pl.when(jnp.logical_not(small))
    def _():
        qx, qy = lax.axis_index("qx"), lax.axis_index("qy")
        fetch = []
        for a in range(DEVICES):
            i = lax.rem(a // 4 + qx // 2, 2) + 2 * lax.rem(a % 2 + qy, 2)
            fetch.append(pltpu.make_async_copy(in_cost.at[i, lax.rem(a // 2 + qx, 2)], cost.at[a], cost_sem.at[a]))
        run(fetch)
        quarter_tables(tab_a, tab_b)
        finish(fetch)

        def part_of(n):
            a, p = quot(n, parts), rest(n, parts)
            c, q = quot(p, chunk // PART), rest(p, chunk // PART)
            spot = (a, c, pl.ds(pl.multiple_of(rest(q, 4) * PART, PART), PART), half_lanes(quot(q, 4)))
            k = lax.rem(popcount_small(p, 5) + popcount_small(a, 3), 4)
            return a, pl.ds(pl.multiple_of(p * PART, PART), PART), spot, k

        def tile_of(p):
            return pl.ds(pl.multiple_of(rest(p, spots // 2) * 8, 8), 8), half_lanes(quot(p, spots // 2))

        for layer in BOTH:
            gamma, beta = [jnp.max(sums[DEVICES + k][layer:layer + 1]) for k in BOTH]
            ch, sh = cos_sin(0.5 * beta)
            cf, sf = cos_sin(beta)

            def phase(n, carry):
                a, r, spot, k = part_of(n)
                t = gamma * cost[a, r]
                vr, vi = jnp.cos(t), -jnp.sin(t)
                qr, qi = (tab_a[k], tab_b[k]) if layer == 0 else (psi[0, *spot], psi[1, *spot])
                psi[0, *spot] = vr * qr - vi * qi
                psi[1, *spot] = vr * qi + vi * qr
                return carry

            lax.fori_loop(0, DEVICES * parts, phase, 0)
            w[...] = rotation_power(ch[0:1, 0:1], -sh[0:1, 0:1], 8, 2.0 ** -4)
            consts = (ch, signed_sines(sh), cf, sf)

            def within(n, carry):
                ref = psi.at[rest(n, 2), quot(n, 2 * CHUNKS), rest(quot(n, 2), CHUNKS)]
                for h in BOTH:
                    run_rows(ref, h, consts)
                run_lanes(ref, w)
                return carry

            lax.fori_loop(0, 16 * CHUNKS, within, 0)

            def chunk_bits(n, carry):
                a, p = quot(n, spots), rest(n, spots)
                for k in BOTH:
                    v = [psi[k, a, c, *tile_of(p)] for c in range(CHUNKS)]
                    for c, value in enumerate(rotate_pair(*v, cf, sf)):
                        psi[k, a, c, *tile_of(p)] = value
                return carry

            lax.fori_loop(0, DEVICES * spots, chunk_bits, 0)

            def top_bits(n, carry):
                c, p = quot(n, spots), rest(n, spots)
                for k in BOTH:
                    v = [psi[k, a, c, *tile_of(p)] for a in range(8)]
                    v = rotate_pair(*v[:4], cf, sf) + rotate_pair(*v[4:], cf, sf)
                    for a in range(4):
                        psi[k, a, c, *tile_of(p)] = ch * v[a] - sh * v[a + 4]
                        psi[k, a + 4, c, *tile_of(p)] = sh * v[a] + ch * v[a + 4]
                return carry

            lax.fori_loop(0, CHUNKS * spots, top_bits, 0)

        def add(n, acc):
            a, r, spot, _ = part_of(n)
            vr, vi = psi[0, *spot], psi[1, *spot]
            return acc + (cost[a, r] * (vr * vr + vi * vi)).reshape(PART // 8, 8, LANES).sum(axis=0)

        total = jnp.sum(lax.fori_loop(0, DEVICES * parts, add, jnp.zeros((8, LANES), jnp.float32)))
        def turn(p, carry):
            _, r, spot, k = part_of((qx * 2 + qy) * parts + p)
            vr, vi, ta, tb = psi[0, *spot], psi[1, *spot], tab_a[k], tab_b[k]
            state[0, r] = ta * vr + tb * vi
            state[1, r] = ta * vi - tb * vr
            return carry

        lax.fori_loop(0, parts, turn, 0)
        finish(run(put_all((state.at[0], state.at[1])) + [put_energy(total)]))


def simulate(cost_rows, gammas, betas):
    rows = cost_rows.shape[0]
    f32 = jnp.float32
    state = jax.ShapeDtypeStruct((rows, LANES), f32)
    near = pl.BlockSpec(memory_space=pl.ANY)
    dma = pltpu.SemaphoreType.DMA
    full = pltpu.VMEM((2, rows, LANES), f32)
    blocks = pltpu.VMEM((2, 4, rows, LANES), f32)
    table = pltpu.VMEM((4, PART, LANES), f32)
    two, four = dma((2,)), dma((CHUNKS,))
    tiles = pltpu.VMEM((DEVICES + 2, 2, LANES), f32)
    halves = pltpu.VMEM((2, 2, CHUNKS, 2 * LANES, LANES), f32)

    def square(*lead):
        return pltpu.VMEM(lead + (2 * LANES, 2 * LANES), f32)

    s_re, s_im, costs, sums = pl.pallas_call(
        gather_kernel,
        out_shape=(state, state, jax.ShapeDtypeStruct((4, 2, rows, LANES), f32),
                   jax.ShapeDtypeStruct((DEVICES + 2, 2, LANES), f32)),
        in_specs=[near] * 2,
        out_specs=(near,) * 4,
        scratch_shapes=[
            pltpu.VMEM((4, 2, rows, LANES), f32), square(2, 4, CHUNKS), blocks,
            halves, square(2, CHUNKS), halves, full, square(), square(),
            table, table, table, table, pltpu.VMEM((8, LANES), f32), pltpu.VMEM((3, 2, LANES), f32), pltpu.SMEM((4,), f32),
            dma, two, dma, dma, dma, dma, dma, dma, four, four, four, four, dma((4, CHUNKS)),
            dma, two, dma, dma, two, dma],
        compiler_params=pltpu.CompilerParams(collective_id=0, has_side_effects=True,
                                             vmem_limit_bytes=52736 << 10),
    )(cost_rows, jnp.concatenate([gammas, betas]))
    return pl.pallas_call(
        final_kernel,
        out_shape=(state, state, jax.ShapeDtypeStruct((1,), f32)),
        in_specs=[near] * 4,
        out_specs=(near,) * 3,
        scratch_shapes=[
            full, pltpu.VMEM((8, rows, LANES), f32), square(2, 8, CHUNKS), square(), table, table,
            tiles, pltpu.SMEM((1,), f32), two, dma((DEVICES,)), two],
        compiler_params=pltpu.CompilerParams(vmem_limit_bytes=52224 << 10),
    )(s_re, s_im, costs, sums)


def popcount(values, bits):
    return sum((values >> b) & 1 for b in range(bits))


def solution(mesh):
    state_spec = P(('inst', 'qx', 'qy'))

    def device_body(cost_local, gammas, betas):
        local_len = cost_local.shape[0]
        s_re, s_im, energy = simulate(cost_local.reshape(local_len // LANES, LANES), gammas, betas)
        return energy, s_re.reshape(local_len), s_im.reshape(local_len)

    return jax.shard_map(device_body, mesh=mesh, in_specs=(state_spec, P(), P()),
                         out_specs=(P('inst'), state_spec, state_spec), check_vma=False)
```

```python
import math
import jax
import jax.numpy as jnp
import numpy as np
from jax import lax
from jax.experimental import pallas as pl
from jax.experimental.pallas import tpu as pltpu
from jax.sharding import PartitionSpec as P

LANES = 128
MESH = pl.DeviceIdType.MESH
HIGHEST = lax.Precision.HIGHEST
ANGLE_MAX = 131072.0
INV_TURN = float(np.float32(1.0 / (2.0 * math.pi)))
TURN_HI = 6.28125
TURN_LO = float(np.float32(2.0 * math.pi - 6.28125))
CHUNKS = 4
BOTH = range(2)
DEVICES = 8
PART = 64

SIN_COEFS = [2 * v / 4.0 ** (2 * k + 1) for k, v in enumerate(
    [1.0, -1.6666654611e-1, 8.3321608736e-3, -1.9515295891e-4])]
COS_COEFS = [2 * v / 16.0 ** k for k, v in enumerate(
    [1.0, -0.5, 4.166664568298827e-2, -1.388731625493765e-3, 2.443315711809948e-5])]


def horner(coefs, z):
    acc = coefs[-1] * z + coefs[-2]
    for v in coefs[-3::-1]:
        acc = acc * z + v
    return acc


def double_phase(cost, gamma, scale, quarter=None, offset=None):
    angle = gamma * cost
    turns = angle * INV_TURN
    if quarter is not None:
        turns = turns - quarter
    n = lax.round(turns, lax.RoundingMethod.TO_NEAREST_EVEN)
    r = (n * TURN_HI - angle) + n * TURN_LO
    if offset is not None:
        r = r + offset
    z = r * r
    s = r * horner(SIN_COEFS, z)
    s2 = s * horner(COS_COEFS, z)
    t2 = scale * s2
    return (scale + scale) - t2 * s2, t2 * (2.0 - s * s)


def rotate_pair(x00, x01, x10, x11, cos_full, sin_full):
    u, v = x00 - x11, x00 + x11
    w, y = x01 + x10, x01 - x10
    u, w = cos_full * u - sin_full * w, sin_full * u + cos_full * w
    return v + u, w + y, w - y, v - u


def quot(a, b):
    return a // b if isinstance(a, int) else lax.div(a, jnp.int32(b))


def rest(a, b):
    return a % b if isinstance(a, int) else lax.rem(a, jnp.int32(b))


def popcount_small(k, bits):
    return sum(rest(quot(k, 1 << b), 2) for b in range(bits))


def rotation_power(cos_half, sin_half, bits, scale):
    n = 1 << bits
    row = lax.broadcasted_iota(jnp.int32, (n, n), 0)
    col = lax.broadcasted_iota(jnp.int32, (n, n), 1)
    acc = jnp.full((n, n), scale, jnp.float32)
    for b in range(bits):
        rb, cb = (row >> b) & 1, (col >> b) & 1
        acc = acc * jnp.where(rb == cb, cos_half, jnp.where(rb > cb, sin_half, -sin_half))
    return acc


def row_gates(arr, cos_half, signed, cos_full, sin_full):
    sub = lax.broadcasted_iota(jnp.int32, arr.shape, 1)
    for b in range(3):
        arr = cos_half * arr + signed[b] * jnp.take_along_axis(arr, sub ^ (1 << b), axis=1)
    v = [arr[k] for k in range(32)]
    for q in (1, 4):
        for k in range(32):
            if (k // q) % 4 == 0:
                quad = (k, k + q, k + 2 * q, k + 3 * q)
                for d, value in zip(quad, rotate_pair(*[v[d] for d in quad], cos_full, sin_full)):
                    v[d] = value
    for k in range(16):
        lo, hi = v[k], v[k + 16]
        v[k], v[k + 16] = cos_half * lo - signed[3] * hi, signed[3] * lo + cos_half * hi
    return v


def loop(start, stop, body, carry, steps=1):
    def turn(n, value):
        for k in range(steps):
            value = body(n * steps + k, value)
        return value
    return lax.fori_loop(start // steps, stop // steps, turn, carry)


def half_lanes(h):
    return pl.ds(pl.multiple_of(h * LANES, LANES), LANES)


def run_rows(ref, h, consts, value=None):
    rows = ref.shape[0]
    value = ref[:, half_lanes(h)] if value is None else value
    v = row_gates(value.reshape(rows // 8, 8, LANES), *consts)
    for k in range(rows // 8):
        ref[pl.ds(8 * k, 8), half_lanes(h)] = v[k]


def run_lanes(ref, w):
    if len(ref.shape) == 2:
        halves = [ref.at[pl.ds(k * LANES, LANES)] for k in BOTH]
    else:
        halves = [ref.at[k] for k in BOTH]
    values = [half[...].reshape(-1, ref.shape[-1]) for half in halves]
    values = [jnp.dot(v, w[...], precision=HIGHEST, preferred_element_type=jnp.float32) for v in values]
    for half, v in zip(halves, values):
        half[...] = v.reshape(half.shape)


def cos_sin(v):
    v = jnp.full((8, LANES), v)
    return jnp.cos(v), jnp.sin(v)


def signed_sines(sin_half):
    sub = lax.broadcasted_iota(jnp.int32, (8, LANES), 0)
    return [jnp.where((sub & (1 << b)) == 0, -sin_half, sin_half) for b in range(3)] + [sin_half]


def quarter_tables(tab_a, tab_b):
    low = (lax.broadcasted_iota(jnp.int32, (PART, LANES), 0) * LANES
           + lax.broadcasted_iota(jnp.int32, (PART, LANES), 1))
    pop = popcount(low, 13)
    for k in range(4):
        q = (pop + k) & 3
        tab_a[k] = jnp.where(q == 0, 1.0, jnp.where(q == 2, -1.0, 0.0))
        tab_b[k] = jnp.where(q == 1, 1.0, jnp.where(q == 3, -1.0, 0.0))
    return pop


def gather_kernel(c_hbm, angles_any, out_re, out_im, out_cost, out_sums,
                  cost, psi, trig, wave, mixed, part, final, w1, w2,
                  tab_q, tab_o, tab_a, tab_b, cmax, mine, angles,
                  own_sem, out_sem, keep_sem, sx, sy, srx, sry, sc, rx, ry, rdx, rdy, rc, swave, rwave, se, re_sem, sums_sem, angle_sem):
    qx, qy = lax.axis_index("qx"), lax.axis_index("qy")
    x, core = quot(qx, 2), rest(qx, 2)
    rows = c_hbm.shape[0]
    chunk = rows // CHUNKS
    half = chunk // 2

    def dev(dx, dy, dc):
        return {"qx": lax.rem(x + dx, 2) * 2 + lax.rem(core + dc, 2), "qy": lax.rem(qy + dy, 2)}

    xn, yn, cn = dev(1, 0, 0), dev(0, 1, 0), dev(0, 0, 1)

    own_copy = pltpu.make_async_copy(c_hbm, cost.at[0, 0], own_sem)
    own_copy.start()
    angle_copy = pltpu.make_async_copy(angles_any, angles, angle_sem)
    angle_copy.start()
    barrier = pltpu.get_barrier_semaphore()
    for neighbour in (xn, yn, cn):
        pl.semaphore_signal(barrier, inc=1, device_id=neighbour, device_id_type=MESH)

    tile = (8, LANES)
    three = (PART // 8, 8, LANES)
    pl.semaphore_wait(barrier, 3)

    def remote(src, dst, ssem, rsem, device):
        return pltpu.make_async_remote_copy(src_ref=src, dst_ref=dst, send_sem=ssem, recv_sem=rsem,
                                            device_id=device, device_id_type=MESH)

    def rows_of(c):
        return pl.ds(c * chunk, chunk)

    def span(c, h):
        return pl.ds(c * chunk + h * half, half)

    def to_x(c):
        return remote(c_hbm.at[rows_of(c)], cost.at[1, 0, rows_of(c)], sx, rx.at[c], xn)

    def to_y(c):
        return remote(c_hbm.at[rows_of(c)], cost.at[2, 0, rows_of(c)], sy, ry.at[c], yn)

    def relay_y(c):
        return remote(cost.at[1, 0, span(c, 0)], cost.at[3, 0, span(c, 0)], sry, rdy.at[c], yn)

    def relay_x(c):
        return remote(cost.at[2, 0, span(c, 1)], cost.at[3, 0, span(c, 1)], srx, rdx.at[c], xn)

    def to_core(i, c):
        return remote(cost.at[i, 0, rows_of(c)], cost.at[i, 1, rows_of(c)], sc, rc.at[i, c], cn)

    def keep(i, k, c):
        return pltpu.make_async_copy(cost.at[i, k, rows_of(c)], out_cost.at[i, k, rows_of(c)], keep_sem)

    for c in range(CHUNKS):
        to_x(c).start()
        to_y(c).start()
    own_copy.wait()
    for c in range(CHUNKS):
        to_core(0, c).start()

    angle_copy.wait()
    g1, g2, beta1, beta2 = [angles[k] for k in range(4)]
    for k, v in enumerate(((g1, g2), (beta1, beta2))):
        mine[k + 1] = jnp.concatenate([jnp.full((1, LANES), u) for u in v], axis=0)
    keep_angles = pltpu.make_async_copy(mine.at[pl.ds(1, 2)], out_sums.at[pl.ds(DEVICES, 2)], sums_sem.at[1])
    keep_angles.start()
    ch1, sh1 = cos_sin(0.5 * beta1)
    ch2, sh2 = cos_sin(0.5 * beta2)
    cf1, sf1 = cos_sin(beta1)
    cf2, sf2 = cos_sin(beta2)
    pop = quarter_tables(tab_a, tab_b)
    for k in range(4):
        q = ((pop + k) & 3).astype(jnp.float32)
        tab_q[k] = 0.25 * q
        tab_o[k] = q * float(np.float32(0.5 * math.pi))
    signed1, signed2 = signed_sines(sh1), signed_sines(sh2)

    w1[...] = rotation_power(ch1[0:1, 0:1], -sh1[0:1, 0:1], 8, 2.0 ** -6)
    w2[...] = rotation_power(ch2[0:1, 0:1], -sh2[0:1, 0:1], 8, 2.0 ** -3)
    cmax[...] = jnp.zeros(tile, jnp.float32)

    xf, yf, kf = x.astype(jnp.float32), qy.astype(jnp.float32), core.astype(jnp.float32)
    sign_x, sign_y, sign_k = 2.0 * xf - 1.0, 2.0 * yf - 1.0, 2.0 * kf - 1.0
    flip = sign_x * sign_y
    sx1 = -sign_x * sf1
    sx2, sy2 = sign_x * sh2, sign_y * sh2
    contract = [ch2 * ch2, sx2 * ch2, flip * (ch2 * sy2), flip * (sx2 * sy2)]
    spread = [1.0, 1.0, flip, flip]

    consts1 = (ch1, signed1, cf1, sf1)
    consts2 = (ch2, signed2, cf2, sf2)

    def phases(i, c, own=True, other=True):
        base = c % 2 + c // 2 + (x if i % 2 == 0 else 1 - x) + (qy if i < 2 else 1 - qy)
        ca, cb = spread[i] * ch1, spread[i] * sign_k * sh1
        def body(n, carry):
            r = pl.ds(pl.multiple_of(c * chunk + n * PART, PART), PART)
            spot = (pl.ds(pl.multiple_of(rest(n, 4) * PART, PART), PART), half_lanes(quot(n, 4)))
            terms = []
            for flag, side, coef in ((own, 0, ca), (other, 1, cb)):
                if flag:
                    q = lax.rem(base + popcount_small(n, 3) + (core if side == 0 else 1 - core), 4)
                    terms.append(double_phase(cost[i, side, r].reshape(three), g1, coef,
                                              tab_q[q].reshape(three), tab_o[q].reshape(three)))
            if not own:
                terms.append([psi[k, i, c, *spot].reshape(three) for k in BOTH])
            for k in BOTH:
                u = terms[0][k] if len(terms) == 1 else terms[0][k] + terms[1][k]
                psi[k, i, c, *spot] = u.reshape(PART, LANES)
            if own:
                v = cost[i, 0, r].reshape(three)
                for k, u in enumerate(double_phase(v, g2, contract[i])):
                    trig[k, i, r] = u.reshape(PART, LANES)
                if i == 0:
                    cmax[...] = jnp.maximum(cmax[...], jnp.abs(v).max(axis=0))
            return carry

        loop(0, chunk // PART, body, 0, 2)

    def rows_loop(i, c):
        def body(n, carry):
            run_rows(psi.at[quot(n, 2), i, c], rest(n, 2), consts1)
            return carry
        lax.fori_loop(0, 4, body, 0)

    def place(p):
        return pl.ds(pl.multiple_of(rest(p, half // 8) * 8, 8), 8), half_lanes(quot(p, half // 8))

    def chunk_bits(p, carry, blocks=(1, 2)):
        for k in BOTH:
            for i in blocks:
                v = rotate_pair(*[psi[k, i, c, *place(p)] for c in range(CHUNKS)], cf1, sf1)
                for c in range(CHUNKS):
                    psi[k, i, c, *place(p)] = v[c]
        return carry

    def arrived(i, c):
        if i == 1 or i == 2:
            (to_x if i == 1 else to_y)(c).wait_recv()
            (relay_y if i == 1 else relay_x)(c).start()
        if i == 3:
            relay_y(c).wait_recv()
            relay_x(c).wait_recv()
        if i > 0:
            to_core(i, c).start()
        keep(i, 0, c).start()

    def other_arrived(i, c):
        to_core(i, c).wait_recv()
        keep(i, 1, c).start()

    def unit(i, c):
        other_arrived(i, c)
        phases(i, c)
        rows_loop(i, c)

    for c in range(CHUNKS):
        arrived(0, c)
        unit(0, c)
        if c % 2 == 1:
            run_lanes(psi.at[:, 0, pl.ds(c - 1, 2)], w1)
    for c in range(CHUNKS):
        for i in (1, 2):
            arrived(i, c)
        for i in (1, 2):
            unit(i, c)
        if c == CHUNKS - 1:
            arrived(3, 0)
        run_lanes(psi.at[:, pl.ds(1, 2), c], w1)
        if c == 0:
            loop(0, chunk // 8, lambda p, v: chunk_bits(p, v, (0,)), 0, 4)
    loop(0, chunk // 8, chunk_bits, 0, 4)
    arrived(3, 1)
    unit(3, 0)
    unit(3, 1)
    arrived(3, 2)
    run_lanes(psi.at[:, 3, pl.ds(0, 2)], w1)
    unit(3, 2)
    arrived(3, 3)
    run_lanes(psi.at[:, 3, 2], w1)
    phases(3, 3, other=False)
    other_arrived(3, 3)
    phases(3, 3, own=False)
    for k in BOTH:
        for h in BOTH:
            run_rows(psi.at[k, 3, 3], h, consts1)
    run_lanes(psi.at[:, 3, 3], w1)

    def tail(p, carry):
        r = [pl.ds(pl.multiple_of(c * chunk + p * 8, 8), 8) for c in range(CHUNKS)]
        diag = [rotate_pair(*[psi[k, 3, c, *place(p)] for c in range(CHUNKS)], cf1, sf1) for k in BOTH]
        z = [[], []]
        for c in range(CHUNKS):
            v = [rotate_pair(*[psi[k, i, c, *place(p)] for i in (0, 2, 1)], diag[k][c], cf1, sx1) for k in BOTH]
            sums = None
            for n, i in enumerate((0, 2, 1, 3)):
                (re, im), (tr, ti) = (v[0][n], v[1][n]), (trig[0, i, r[c]], trig[1, i, r[c]])
                term = (re * tr - im * ti, re * ti + im * tr)
                sums = term if sums is None else (sums[0] + term[0], sums[1] + term[1])
            z[0].append(sums[0])
            z[1].append(sums[1])
        for k in BOTH:
            for c, value in enumerate(rotate_pair(*z[k], cf2, sf2)):
                wave[quot(p, half // 8), k, c, place(p)[0]] = value
        return carry

    def swap(n):
        spot = (quot(n, 4), slice(None), slice(None), pl.ds(pl.multiple_of(rest(n, 4) * PART, PART), PART))
        return remote(wave.at[*spot], part.at[*spot], swave, rwave.at[quot(n, 4)], cn)

    def piece(n, carry):
        loop(0, PART // 8, lambda p, v: tail(n * (PART // 8) + p, v), 0, 4)
        swap(n).start()
        return carry

    lax.fori_loop(0, DEVICES, piece, 0)

    sk2 = sign_k * sh2
    for h in BOTH:
        remote(wave.at[h], part.at[h], swave, rwave.at[h], cn).wait_recv()

        def turn(n, carry, h=h):
            k, c = quot(n, CHUNKS), rest(n, CHUNKS)
            shape = (half // 8, 8, LANES)
            run_rows(mixed.at[k, c], h, consts2, ch2 * wave[h, k, c].reshape(shape) + sk2 * part[h, k, c].reshape(shape))
            return carry

        lax.fori_loop(0, 2 * CHUNKS, turn, 0)

    energy = jnp.zeros(tile, jnp.float32)
    for c in range(CHUNKS):
        if c == 0:
            run_lanes(mixed, w2)

        def last(p, acc, c=c):
            r = pl.ds(pl.multiple_of(c * chunk + p * PART, PART), PART)
            spot = (pl.ds(pl.multiple_of(rest(p, 4) * PART, PART), PART), half_lanes(quot(p, 4)))
            vr, vi = [mixed[k, c, *spot] for k in BOTH]
            k = lax.rem(popcount_small(p, 3) + c % 2 + c // 2 + x + qy + core, 4)
            final[0, r] = tab_a[k] * vr + tab_b[k] * vi
            final[1, r] = tab_a[k] * vi - tab_b[k] * vr
            return acc + (cost[0, 0, r] * (vr * vr + vi * vi)).reshape(three).sum(axis=0)

        energy = loop(0, chunk // PART, last, energy, 4)
        for k, out in enumerate((out_re, out_im)):
            pltpu.make_async_copy(final.at[k, rows_of(c)], out.at[rows_of(c)], out_sem.at[k]).start()

    me = qy * 4 + qx
    largest = cmax[...].max(axis=0, keepdims=True) * jnp.maximum(jnp.abs(g1), jnp.abs(g2))
    mine[0] = jnp.concatenate([energy.sum(axis=0, keepdims=True), largest], axis=0)
    sends = [remote(mine.at[0], out_sums.at[me], se, re_sem, dev(n // 4, (n // 2) % 2, n % 2))
             for n in range(1, DEVICES)]
    for cp in sends:
        cp.start()
    keep_mine = pltpu.make_async_copy(mine.at[0], out_sums.at[me], sums_sem.at[0])
    keep_mine.start()
    outs = [keep_mine, keep_angles, pltpu.make_async_copy(cost, out_cost, keep_sem)]
    outs += [pltpu.make_async_copy(final.at[k], out, out_sem.at[k]) for k, out in enumerate((out_re, out_im))]
    spot, others = pl.ds(0, rows // 2), out_sums.at[pl.ds(0, DEVICES - 1)]
    for src, dst, sem in ((c_hbm, cost.at[1, 0], sx), (c_hbm, cost.at[2, 0], sy),
                          (cost.at[1, 0, spot], cost.at[3, 0, spot], sry),
                          (cost.at[2, 0, spot], cost.at[3, 0, spot], srx),
                          (cost.at[:, 0], cost.at[:, 1], sc), (wave, part, swave)):
        remote(src, dst, sem, re_sem, cn).wait_send()
    for cp in outs:
        cp.wait()
    remote(others, others, se, re_sem, cn).wait()


def final_kernel(in_re, in_im, in_cost, in_sums, out_re, out_im, out_energy,
                 state, cost, psi, w, tab_a, tab_b, sums, energy, out_sem, cost_sem, small_sem):
    rows = in_re.shape[0]
    chunk = rows // CHUNKS
    parts, spots = rows // PART, chunk // 8
    outs = (out_re, out_im)

    def put_all(srcs):
        return [pltpu.make_async_copy(srcs[k], outs[k], out_sem.at[k]) for k in BOTH]

    def put_energy(total):
        energy[0] = total * (1.0 / (DEVICES * rows * LANES))
        return pltpu.make_async_copy(energy, out_energy, small_sem.at[1])

    def run(copies):
        for cp in copies:
            cp.start()
        return copies

    def finish(copies):
        for cp in copies:
            cp.wait()

    moves = run(put_all((in_re, in_im)))
    finish(run([pltpu.make_async_copy(in_sums, sums, small_sem.at[0])]))
    both = [sums[n] for n in range(DEVICES)]
    total = sum(v[:1] for v in both[1:]) + both[0][:1]
    moves += run([put_energy(jnp.sum(total))])
    small = jnp.max(jnp.stack(both)[:, 1:]) <= ANGLE_MAX
    finish(moves)

    @pl.when(jnp.logical_not(small))
    def _():
        qx, qy = lax.axis_index("qx"), lax.axis_index("qy")
        fetch = []
        for a in range(DEVICES):
            i = lax.rem(a // 4 + qx // 2, 2) + 2 * lax.rem(a % 2 + qy, 2)
            fetch.append(pltpu.make_async_copy(in_cost.at[i, lax.rem(a // 2 + qx, 2)], cost.at[a], cost_sem.at[a]))
        run(fetch)
        quarter_tables(tab_a, tab_b)
        finish(fetch)

        def part_of(n):
            a, p = quot(n, parts), rest(n, parts)
            c, q = quot(p, chunk // PART), rest(p, chunk // PART)
            spot = (a, c, pl.ds(pl.multiple_of(rest(q, 4) * PART, PART), PART), half_lanes(quot(q, 4)))
            k = lax.rem(popcount_small(p, 5) + popcount_small(a, 3), 4)
            return a, pl.ds(pl.multiple_of(p * PART, PART), PART), spot, k

        def tile_of(p):
            return pl.ds(pl.multiple_of(rest(p, spots // 2) * 8, 8), 8), half_lanes(quot(p, spots // 2))

        for layer in BOTH:
            gamma, beta = [jnp.max(sums[DEVICES + k][layer:layer + 1]) for k in BOTH]
            ch, sh = cos_sin(0.5 * beta)
            cf, sf = cos_sin(beta)

            def phase(n, carry):
                a, r, spot, k = part_of(n)
                t = gamma * cost[a, r]
                vr, vi = jnp.cos(t), -jnp.sin(t)
                qr, qi = (tab_a[k], tab_b[k]) if layer == 0 else (psi[0, *spot], psi[1, *spot])
                psi[0, *spot] = vr * qr - vi * qi
                psi[1, *spot] = vr * qi + vi * qr
                return carry

            lax.fori_loop(0, DEVICES * parts, phase, 0)
            w[...] = rotation_power(ch[0:1, 0:1], -sh[0:1, 0:1], 8, 2.0 ** -4)
            consts = (ch, signed_sines(sh), cf, sf)

            def within(n, carry):
                ref = psi.at[rest(n, 2), quot(n, 2 * CHUNKS), rest(quot(n, 2), CHUNKS)]
                for h in BOTH:
                    run_rows(ref, h, consts)
                run_lanes(ref, w)
                return carry

            lax.fori_loop(0, 16 * CHUNKS, within, 0)

            def chunk_bits(n, carry):
                a, p = quot(n, spots), rest(n, spots)
                for k in BOTH:
                    v = [psi[k, a, c, *tile_of(p)] for c in range(CHUNKS)]
                    for c, value in enumerate(rotate_pair(*v, cf, sf)):
                        psi[k, a, c, *tile_of(p)] = value
                return carry

            lax.fori_loop(0, DEVICES * spots, chunk_bits, 0)

            def top_bits(n, carry):
                c, p = quot(n, spots), rest(n, spots)
                for k in BOTH:
                    v = [psi[k, a, c, *tile_of(p)] for a in range(8)]
                    v = rotate_pair(*v[:4], cf, sf) + rotate_pair(*v[4:], cf, sf)
                    for a in range(4):
                        psi[k, a, c, *tile_of(p)] = ch * v[a] - sh * v[a + 4]
                        psi[k, a + 4, c, *tile_of(p)] = sh * v[a] + ch * v[a + 4]
                return carry

            lax.fori_loop(0, CHUNKS * spots, top_bits, 0)

        def add(n, acc):
            a, r, spot, _ = part_of(n)
            vr, vi = psi[0, *spot], psi[1, *spot]
            return acc + (cost[a, r] * (vr * vr + vi * vi)).reshape(PART // 8, 8, LANES).sum(axis=0)

        total = jnp.sum(lax.fori_loop(0, DEVICES * parts, add, jnp.zeros((8, LANES), jnp.float32)))
        def turn(p, carry):
            _, r, spot, k = part_of((qx * 2 + qy) * parts + p)
            vr, vi, ta, tb = psi[0, *spot], psi[1, *spot], tab_a[k], tab_b[k]
            state[0, r] = ta * vr + tb * vi
            state[1, r] = ta * vi - tb * vr
            return carry

        lax.fori_loop(0, parts, turn, 0)
        finish(run(put_all((state.at[0], state.at[1])) + [put_energy(total)]))


def simulate(cost_rows, gammas, betas):
    rows = cost_rows.shape[0]
    f32 = jnp.float32
    state = jax.ShapeDtypeStruct((rows, LANES), f32)
    near = pl.BlockSpec(memory_space=pl.ANY)
    dma = pltpu.SemaphoreType.DMA
    full = pltpu.VMEM((2, rows, LANES), f32)
    blocks = pltpu.VMEM((2, 4, rows, LANES), f32)
    table = pltpu.VMEM((4, PART, LANES), f32)
    two, four = dma((2,)), dma((CHUNKS,))
    tiles = pltpu.VMEM((DEVICES + 2, 2, LANES), f32)
    halves = pltpu.VMEM((2, 2, CHUNKS, 2 * LANES, LANES), f32)

    def square(*lead):
        return pltpu.VMEM(lead + (2 * LANES, 2 * LANES), f32)

    s_re, s_im, costs, sums = pl.pallas_call(
        gather_kernel,
        out_shape=(state, state, jax.ShapeDtypeStruct((4, 2, rows, LANES), f32),
                   jax.ShapeDtypeStruct((DEVICES + 2, 2, LANES), f32)),
        in_specs=[near] * 2,
        out_specs=(near,) * 4,
        scratch_shapes=[
            pltpu.VMEM((4, 2, rows, LANES), f32), square(2, 4, CHUNKS), blocks,
            halves, square(2, CHUNKS), halves, full, square(), square(),
            table, table, table, table, pltpu.VMEM((8, LANES), f32), pltpu.VMEM((3, 2, LANES), f32), pltpu.SMEM((4,), f32),
            dma, two, dma, dma, dma, dma, dma, dma, four, four, four, four, dma((4, CHUNKS)),
            dma, two, dma, dma, two, dma],
        compiler_params=pltpu.CompilerParams(collective_id=0, has_side_effects=True,
                                             vmem_limit_bytes=52736 << 10),
    )(cost_rows, jnp.concatenate([gammas, betas]))
    return pl.pallas_call(
        final_kernel,
        out_shape=(state, state, jax.ShapeDtypeStruct((1,), f32)),
        in_specs=[near] * 4,
        out_specs=(near,) * 3,
        scratch_shapes=[
            full, pltpu.VMEM((8, rows, LANES), f32), square(2, 8, CHUNKS), square(), table, table,
            tiles, pltpu.SMEM((1,), f32), two, dma((DEVICES,)), two],
        compiler_params=pltpu.CompilerParams(vmem_limit_bytes=52224 << 10),
    )(s_re, s_im, costs, sums)


def popcount(values, bits):
    return sum((values >> b) & 1 for b in range(bits))


def solution(mesh):
    state_spec = P(('inst', 'qx', 'qy'))

    def device_body(cost_local, gammas, betas):
        local_len = cost_local.shape[0]
        s_re, s_im, energy = simulate(cost_local.reshape(local_len // LANES, LANES), gammas, betas)
        return energy, s_re.reshape(local_len), s_im.reshape(local_len)

    return jax.shard_map(device_body, mesh=mesh, in_specs=(state_spec, P(), P()),
                         out_specs=(P('inst'), state_spec, state_spec), check_vma=False)
```

```python
import math
import jax
import jax.numpy as jnp
import numpy as np
from jax import lax
from jax.experimental import pallas as pl
from jax.experimental.pallas import tpu as pltpu
from jax.sharding import PartitionSpec as P

LANES = 128
MESH = pl.DeviceIdType.MESH
HIGHEST = lax.Precision.HIGHEST
ANGLE_MAX = 131072.0
INV_TURN = float(np.float32(1.0 / (2.0 * math.pi)))
TURN_HI = 6.28125
TURN_LO = float(np.float32(2.0 * math.pi - 6.28125))
CHUNKS = 4
BOTH = range(2)
DEVICES = 8
PART = 64

SIN_COEFS = [2 * v / 4.0 ** (2 * k + 1) for k, v in enumerate(
    [1.0, -1.6666654611e-1, 8.3321608736e-3, -1.9515295891e-4])]
COS_COEFS = [2 * v / 16.0 ** k for k, v in enumerate(
    [1.0, -0.5, 4.166664568298827e-2, -1.388731625493765e-3, 2.443315711809948e-5])]


def horner(coefs, z):
    acc = coefs[-1] * z + coefs[-2]
    for v in coefs[-3::-1]:
        acc = acc * z + v
    return acc


def double_phase(cost, gamma, scale, quarter=None, offset=None):
    angle = gamma * cost
    turns = angle * INV_TURN
    if quarter is not None:
        turns = turns - quarter
    n = lax.round(turns, lax.RoundingMethod.TO_NEAREST_EVEN)
    r = (n * TURN_HI - angle) + n * TURN_LO
    if offset is not None:
        r = r + offset
    z = r * r
    s = r * horner(SIN_COEFS, z)
    s2 = s * horner(COS_COEFS, z)
    t2 = scale * s2
    return (scale + scale) - t2 * s2, t2 * (2.0 - s * s)


def rotate_pair(x00, x01, x10, x11, cos_full, sin_full):
    u, v = x00 - x11, x00 + x11
    w, y = x01 + x10, x01 - x10
    u, w = cos_full * u - sin_full * w, sin_full * u + cos_full * w
    return v + u, w + y, w - y, v - u


def quot(a, b):
    return a // b if isinstance(a, int) else lax.div(a, jnp.int32(b))


def rest(a, b):
    return a % b if isinstance(a, int) else lax.rem(a, jnp.int32(b))


def popcount_small(k, bits):
    return sum(rest(quot(k, 1 << b), 2) for b in range(bits))


def rotation_power(cos_half, sin_half, bits, scale):
    n = 1 << bits
    row = lax.broadcasted_iota(jnp.int32, (n, n), 0)
    col = lax.broadcasted_iota(jnp.int32, (n, n), 1)
    acc = jnp.full((n, n), scale, jnp.float32)
    for b in range(bits):
        rb, cb = (row >> b) & 1, (col >> b) & 1
        acc = acc * jnp.where(rb == cb, cos_half, jnp.where(rb > cb, sin_half, -sin_half))
    return acc


def row_gates(arr, cos_half, signed, cos_full, sin_full):
    sub = lax.broadcasted_iota(jnp.int32, arr.shape, 1)
    for b in range(3):
        arr = cos_half * arr + signed[b] * jnp.take_along_axis(arr, sub ^ (1 << b), axis=1)
    v = [arr[k] for k in range(32)]
    for q in (1, 4):
        for k in range(32):
            if (k // q) % 4 == 0:
                quad = (k, k + q, k + 2 * q, k + 3 * q)
                for d, value in zip(quad, rotate_pair(*[v[d] for d in quad], cos_full, sin_full)):
                    v[d] = value
    for k in range(16):
        lo, hi = v[k], v[k + 16]
        v[k], v[k + 16] = cos_half * lo - signed[3] * hi, signed[3] * lo + cos_half * hi
    return v


def loop(start, stop, body, carry, steps=1):
    def turn(n, value):
        for k in range(steps):
            value = body(n * steps + k, value)
        return value
    return lax.fori_loop(start // steps, stop // steps, turn, carry)


def half_lanes(h):
    return pl.ds(pl.multiple_of(h * LANES, LANES), LANES)


def run_rows(ref, h, consts, value=None):
    rows = ref.shape[0]
    value = ref[:, half_lanes(h)] if value is None else value
    v = row_gates(value.reshape(rows // 8, 8, LANES), *consts)
    for k in range(rows // 8):
        ref[pl.ds(8 * k, 8), half_lanes(h)] = v[k]


def run_lanes(ref, w):
    if len(ref.shape) == 2:
        halves = [ref.at[pl.ds(k * LANES, LANES)] for k in BOTH]
    else:
        halves = [ref.at[k] for k in BOTH]
    values = [half[...].reshape(-1, ref.shape[-1]) for half in halves]
    values = [jnp.dot(v, w[...], precision=HIGHEST, preferred_element_type=jnp.float32) for v in values]
    for half, v in zip(halves, values):
        half[...] = v.reshape(half.shape)


def cos_sin(v):
    v = jnp.full((8, LANES), v)
    return jnp.cos(v), jnp.sin(v)


def signed_sines(sin_half):
    sub = lax.broadcasted_iota(jnp.int32, (8, LANES), 0)
    return [jnp.where((sub & (1 << b)) == 0, -sin_half, sin_half) for b in range(3)] + [sin_half]


def quarter_tables(tab_a, tab_b):
    low = (lax.broadcasted_iota(jnp.int32, (PART, LANES), 0) * LANES
           + lax.broadcasted_iota(jnp.int32, (PART, LANES), 1))
    pop = popcount(low, 13)
    for k in range(4):
        q = (pop + k) & 3
        tab_a[k] = jnp.where(q == 0, 1.0, jnp.where(q == 2, -1.0, 0.0))
        tab_b[k] = jnp.where(q == 1, 1.0, jnp.where(q == 3, -1.0, 0.0))
    return pop


def gather_kernel(c_hbm, angles_any, out_re, out_im, out_cost, out_sums,
                  cost, psi, trig, wave, mixed, part, final, w1, w2,
                  tab_q, tab_o, tab_a, tab_b, cmax, mine, angles,
                  own_sem, out_sem, keep_sem, sx, sy, srx, sry, sc, rx, ry, rdx, rdy, rc, swave, rwave, se, re_sem, sums_sem, angle_sem):
    qx, qy = lax.axis_index("qx"), lax.axis_index("qy")
    x, core = quot(qx, 2), rest(qx, 2)
    rows = c_hbm.shape[0]
    chunk = rows // CHUNKS
    half = chunk // 2

    def dev(dx, dy, dc):
        return {"qx": lax.rem(x + dx, 2) * 2 + lax.rem(core + dc, 2), "qy": lax.rem(qy + dy, 2)}

    xn, yn, cn = dev(1, 0, 0), dev(0, 1, 0), dev(0, 0, 1)

    own_copy = pltpu.make_async_copy(c_hbm, cost.at[0, 0], own_sem)
    own_copy.start()
    angle_copy = pltpu.make_async_copy(angles_any, angles, angle_sem)
    angle_copy.start()
    barrier = pltpu.get_barrier_semaphore()
    for neighbour in (xn, yn, cn):
        pl.semaphore_signal(barrier, inc=1, device_id=neighbour, device_id_type=MESH)

    tile = (8, LANES)
    three = (PART // 8, 8, LANES)
    pl.semaphore_wait(barrier, 3)

    def remote(src, dst, ssem, rsem, device):
        return pltpu.make_async_remote_copy(src_ref=src, dst_ref=dst, send_sem=ssem, recv_sem=rsem,
                                            device_id=device, device_id_type=MESH)

    def rows_of(c):
        return pl.ds(c * chunk, chunk)

    def span(c, h):
        return pl.ds(c * chunk + h * half, half)

    def to_x(c):
        return remote(c_hbm.at[rows_of(c)], cost.at[1, 0, rows_of(c)], sx, rx.at[c], xn)

    def to_y(c):
        return remote(c_hbm.at[rows_of(c)], cost.at[2, 0, rows_of(c)], sy, ry.at[c], yn)

    def relay_y(c):
        return remote(cost.at[1, 0, span(c, 0)], cost.at[3, 0, span(c, 0)], sry, rdy.at[c], yn)

    def relay_x(c):
        return remote(cost.at[2, 0, span(c, 1)], cost.at[3, 0, span(c, 1)], srx, rdx.at[c], xn)

    def to_core(i, c):
        return remote(cost.at[i, 0, rows_of(c)], cost.at[i, 1, rows_of(c)], sc, rc.at[i, c], cn)

    def keep(i, k, c):
        return pltpu.make_async_copy(cost.at[i, k, rows_of(c)], out_cost.at[i, k, rows_of(c)], keep_sem)

    for c in range(CHUNKS):
        to_x(c).start()
        to_y(c).start()
    own_copy.wait()
    for c in range(CHUNKS):
        to_core(0, c).start()

    angle_copy.wait()
    g1, g2, beta1, beta2 = [angles[k] for k in range(4)]
    for k, v in enumerate(((g1, g2), (beta1, beta2))):
        mine[k + 1] = jnp.concatenate([jnp.full((1, LANES), u) for u in v], axis=0)
    keep_angles = pltpu.make_async_copy(mine.at[pl.ds(1, 2)], out_sums.at[pl.ds(DEVICES, 2)], sums_sem.at[1])
    keep_angles.start()
    ch1, sh1 = cos_sin(0.5 * beta1)
    ch2, sh2 = cos_sin(0.5 * beta2)
    cf1, sf1 = cos_sin(beta1)
    cf2, sf2 = cos_sin(beta2)
    pop = quarter_tables(tab_a, tab_b)
    for k in range(4):
        q = ((pop + k) & 3).astype(jnp.float32)
        tab_q[k] = 0.25 * q
        tab_o[k] = q * float(np.float32(0.5 * math.pi))
    signed1, signed2 = signed_sines(sh1), signed_sines(sh2)

    w1[...] = rotation_power(ch1[0:1, 0:1], -sh1[0:1, 0:1], 8, 2.0 ** -6)
    w2[...] = rotation_power(ch2[0:1, 0:1], -sh2[0:1, 0:1], 8, 2.0 ** -3)
    cmax[...] = jnp.zeros(tile, jnp.float32)

    xf, yf, kf = x.astype(jnp.float32), qy.astype(jnp.float32), core.astype(jnp.float32)
    sign_x, sign_y, sign_k = 2.0 * xf - 1.0, 2.0 * yf - 1.0, 2.0 * kf - 1.0
    flip = sign_x * sign_y
    sx1 = -sign_x * sf1
    sx2, sy2 = sign_x * sh2, sign_y * sh2
    contract = [ch2 * ch2, sx2 * ch2, flip * (ch2 * sy2), flip * (sx2 * sy2)]
    spread = [1.0, 1.0, flip, flip]

    consts1 = (ch1, signed1, cf1, sf1)
    consts2 = (ch2, signed2, cf2, sf2)

    def phases(i, c, own=True, other=True):
        base = c % 2 + c // 2 + (x if i % 2 == 0 else 1 - x) + (qy if i < 2 else 1 - qy)
        ca, cb = spread[i] * ch1, spread[i] * sign_k * sh1
        def body(n, carry):
            r = pl.ds(pl.multiple_of(c * chunk + n * PART, PART), PART)
            spot = (pl.ds(pl.multiple_of(rest(n, 4) * PART, PART), PART), half_lanes(quot(n, 4)))
            terms = []
            for flag, side, coef in ((own, 0, ca), (other, 1, cb)):
                if flag:
                    q = lax.rem(base + popcount_small(n, 3) + (core if side == 0 else 1 - core), 4)
                    terms.append(double_phase(cost[i, side, r].reshape(three), g1, coef,
                                              tab_q[q].reshape(three), tab_o[q].reshape(three)))
            if not own:
                terms.append([psi[k, i, c, *spot].reshape(three) for k in BOTH])
            for k in BOTH:
                u = terms[0][k] if len(terms) == 1 else terms[0][k] + terms[1][k]
                psi[k, i, c, *spot] = u.reshape(PART, LANES)
            if own:
                v = cost[i, 0, r].reshape(three)
                for k, u in enumerate(double_phase(v, g2, contract[i])):
                    trig[k, i, r] = u.reshape(PART, LANES)
                if i == 0:
                    cmax[...] = jnp.maximum(cmax[...], jnp.abs(v).max(axis=0))
            return carry

        loop(0, chunk // PART, body, 0, 2)

    def rows_loop(i, c):
        def body(n, carry):
            run_rows(psi.at[quot(n, 2), i, c], rest(n, 2), consts1)
            return carry
        lax.fori_loop(0, 4, body, 0)

    def place(p):
        return pl.ds(pl.multiple_of(rest(p, half // 8) * 8, 8), 8), half_lanes(quot(p, half // 8))

    def chunk_bits(p, carry, blocks=(1, 2)):
        for k in BOTH:
            for i in blocks:
                v = rotate_pair(*[psi[k, i, c, *place(p)] for c in range(CHUNKS)], cf1, sf1)
                for c in range(CHUNKS):
                    psi[k, i, c, *place(p)] = v[c]
        return carry

    def arrived(i, c):
        if i == 1 or i == 2:
            (to_x if i == 1 else to_y)(c).wait_recv()
            (relay_y if i == 1 else relay_x)(c).start()
        if i == 3:
            relay_y(c).wait_recv()
            relay_x(c).wait_recv()
        if i > 0:
            to_core(i, c).start()
        keep(i, 0, c).start()

    def other_arrived(i, c):
        to_core(i, c).wait_recv()
        keep(i, 1, c).start()

    def unit(i, c):
        other_arrived(i, c)
        phases(i, c)
        rows_loop(i, c)

    for c in range(CHUNKS):
        arrived(0, c)
        unit(0, c)
        if c % 2 == 1:
            run_lanes(psi.at[:, 0, pl.ds(c - 1, 2)], w1)
    for c in range(CHUNKS):
        for i in (1, 2):
            arrived(i, c)
        for i in (1, 2):
            unit(i, c)
        if c == CHUNKS - 1:
            arrived(3, 0)
        run_lanes(psi.at[:, pl.ds(1, 2), c], w1)
        if c == 0:
            loop(0, chunk // 8, lambda p, v: chunk_bits(p, v, (0,)), 0, 4)
    loop(0, chunk // 8, chunk_bits, 0, 4)
    arrived(3, 1)
    unit(3, 0)
    unit(3, 1)
    arrived(3, 2)
    run_lanes(psi.at[:, 3, pl.ds(0, 2)], w1)
    unit(3, 2)
    arrived(3, 3)
    run_lanes(psi.at[:, 3, 2], w1)
    phases(3, 3, other=False)
    other_arrived(3, 3)
    phases(3, 3, own=False)
    for k in BOTH:
        for h in BOTH:
            run_rows(psi.at[k, 3, 3], h, consts1)
    run_lanes(psi.at[:, 3, 3], w1)

    def tail(p, carry):
        r = [pl.ds(pl.multiple_of(c * chunk + p * 8, 8), 8) for c in range(CHUNKS)]
        diag = [rotate_pair(*[psi[k, 3, c, *place(p)] for c in range(CHUNKS)], cf1, sf1) for k in BOTH]
        z = [[], []]
        for c in range(CHUNKS):
            v = [rotate_pair(*[psi[k, i, c, *place(p)] for i in (0, 2, 1)], diag[k][c], cf1, sx1) for k in BOTH]
            sums = None
            for n, i in enumerate((0, 2, 1, 3)):
                (re, im), (tr, ti) = (v[0][n], v[1][n]), (trig[0, i, r[c]], trig[1, i, r[c]])
                term = (re * tr - im * ti, re * ti + im * tr)
                sums = term if sums is None else (sums[0] + term[0], sums[1] + term[1])
            z[0].append(sums[0])
            z[1].append(sums[1])
        for k in BOTH:
            for c, value in enumerate(rotate_pair(*z[k], cf2, sf2)):
                wave[quot(p, half // 8), k, c, place(p)[0]] = value
        return carry

    def swap(n):
        spot = (quot(n, 8), slice(None), slice(None), pl.ds(pl.multiple_of(rest(n, 8) * 32, 32), 32))
        return remote(wave.at[*spot], part.at[*spot], swave, rwave.at[quot(n, 8)], cn)

    def piece(n, carry):
        for k in range(4):
            tail(4 * n + k, carry)
        swap(n).start()
        return carry

    lax.fori_loop(0, 2 * DEVICES, piece, 0)

    sk2 = sign_k * sh2
    for h in BOTH:
        remote(wave.at[h], part.at[h], swave, rwave.at[h], cn).wait_recv()

        def turn(n, carry, h=h):
            k, c = quot(n, CHUNKS), rest(n, CHUNKS)
            shape = (half // 8, 8, LANES)
            run_rows(mixed.at[k, c], h, consts2, ch2 * wave[h, k, c].reshape(shape) + sk2 * part[h, k, c].reshape(shape))
            return carry

        loop(0, 2 * CHUNKS, turn, 0, 2)

    energy = jnp.zeros(tile, jnp.float32)
    for c in range(CHUNKS):
        if c == 0:
            run_lanes(mixed, w2)

        def last(p, acc, c=c):
            r = pl.ds(pl.multiple_of(c * chunk + p * PART, PART), PART)
            spot = (pl.ds(pl.multiple_of(rest(p, 4) * PART, PART), PART), half_lanes(quot(p, 4)))
            vr, vi = [mixed[k, c, *spot] for k in BOTH]
            k = lax.rem(popcount_small(p, 3) + c % 2 + c // 2 + x + qy + core, 4)
            final[0, r] = tab_a[k] * vr + tab_b[k] * vi
            final[1, r] = tab_a[k] * vi - tab_b[k] * vr
            return acc + (cost[0, 0, r] * (vr * vr + vi * vi)).reshape(three).sum(axis=0)

        energy = loop(0, chunk // PART, last, energy, 4)
        for k, out in enumerate((out_re, out_im)):
            pltpu.make_async_copy(final.at[k, rows_of(c)], out.at[rows_of(c)], out_sem.at[k]).start()

    me = qy * 4 + qx
    largest = cmax[...].max(axis=0, keepdims=True) * jnp.maximum(jnp.abs(g1), jnp.abs(g2))
    mine[0] = jnp.concatenate([energy.sum(axis=0, keepdims=True), largest], axis=0)
    sends = [remote(mine.at[0], out_sums.at[me], se, re_sem, dev(n // 4, (n // 2) % 2, n % 2))
             for n in range(1, DEVICES)]
    for cp in sends:
        cp.start()
    keep_mine = pltpu.make_async_copy(mine.at[0], out_sums.at[me], sums_sem.at[0])
    keep_mine.start()
    outs = [keep_mine, keep_angles, pltpu.make_async_copy(cost, out_cost, keep_sem)]
    outs += [pltpu.make_async_copy(final.at[k], out, out_sem.at[k]) for k, out in enumerate((out_re, out_im))]
    spot, others = pl.ds(0, rows // 2), out_sums.at[pl.ds(0, DEVICES - 1)]
    for src, dst, sem in ((c_hbm, cost.at[1, 0], sx), (c_hbm, cost.at[2, 0], sy),
                          (cost.at[1, 0, spot], cost.at[3, 0, spot], sry),
                          (cost.at[2, 0, spot], cost.at[3, 0, spot], srx),
                          (cost.at[:, 0], cost.at[:, 1], sc), (wave, part, swave)):
        remote(src, dst, sem, re_sem, cn).wait_send()
    for cp in outs:
        cp.wait()
    remote(others, others, se, re_sem, cn).wait()


def final_kernel(in_re, in_im, in_cost, in_sums, out_re, out_im, out_energy,
                 state, cost, psi, w, tab_a, tab_b, sums, energy, out_sem, cost_sem, small_sem):
    rows = in_re.shape[0]
    chunk = rows // CHUNKS
    parts, spots = rows // PART, chunk // 8
    outs = (out_re, out_im)

    def put_all(srcs):
        return [pltpu.make_async_copy(srcs[k], outs[k], out_sem.at[k]) for k in BOTH]

    def put_energy(total):
        energy[0] = total * (1.0 / (DEVICES * rows * LANES))
        return pltpu.make_async_copy(energy, out_energy, small_sem.at[1])

    def run(copies):
        for cp in copies:
            cp.start()
        return copies

    def finish(copies):
        for cp in copies:
            cp.wait()

    moves = run(put_all((in_re, in_im)))
    finish(run([pltpu.make_async_copy(in_sums, sums, small_sem.at[0])]))
    both = [sums[n] for n in range(DEVICES)]
    total = sum(v[:1] for v in both[1:]) + both[0][:1]
    moves += run([put_energy(jnp.sum(total))])
    small = jnp.max(jnp.stack(both)[:, 1:]) <= ANGLE_MAX
    finish(moves)

    @pl.when(jnp.logical_not(small))
    def _():
        qx, qy = lax.axis_index("qx"), lax.axis_index("qy")
        fetch = []
        for a in range(DEVICES):
            i = lax.rem(a // 4 + qx // 2, 2) + 2 * lax.rem(a % 2 + qy, 2)
            fetch.append(pltpu.make_async_copy(in_cost.at[i, lax.rem(a // 2 + qx, 2)], cost.at[a], cost_sem.at[a]))
        run(fetch)
        quarter_tables(tab_a, tab_b)
        finish(fetch)

        def part_of(n):
            a, p = quot(n, parts), rest(n, parts)
            c, q = quot(p, chunk // PART), rest(p, chunk // PART)
            spot = (a, c, pl.ds(pl.multiple_of(rest(q, 4) * PART, PART), PART), half_lanes(quot(q, 4)))
            k = lax.rem(popcount_small(p, 5) + popcount_small(a, 3), 4)
            return a, pl.ds(pl.multiple_of(p * PART, PART), PART), spot, k

        def tile_of(p):
            return pl.ds(pl.multiple_of(rest(p, spots // 2) * 8, 8), 8), half_lanes(quot(p, spots // 2))

        for layer in BOTH:
            gamma, beta = [jnp.max(sums[DEVICES + k][layer:layer + 1]) for k in BOTH]
            ch, sh = cos_sin(0.5 * beta)
            cf, sf = cos_sin(beta)

            def phase(n, carry):
                a, r, spot, k = part_of(n)
                t = gamma * cost[a, r]
                vr, vi = jnp.cos(t), -jnp.sin(t)
                qr, qi = (tab_a[k], tab_b[k]) if layer == 0 else (psi[0, *spot], psi[1, *spot])
                psi[0, *spot] = vr * qr - vi * qi
                psi[1, *spot] = vr * qi + vi * qr
                return carry

            lax.fori_loop(0, DEVICES * parts, phase, 0)
            w[...] = rotation_power(ch[0:1, 0:1], -sh[0:1, 0:1], 8, 2.0 ** -4)
            consts = (ch, signed_sines(sh), cf, sf)

            def within(n, carry):
                ref = psi.at[rest(n, 2), quot(n, 2 * CHUNKS), rest(quot(n, 2), CHUNKS)]
                for h in BOTH:
                    run_rows(ref, h, consts)
                run_lanes(ref, w)
                return carry

            lax.fori_loop(0, 16 * CHUNKS, within, 0)

            def chunk_bits(n, carry):
                a, p = quot(n, spots), rest(n, spots)
                for k in BOTH:
                    v = [psi[k, a, c, *tile_of(p)] for c in range(CHUNKS)]
                    for c, value in enumerate(rotate_pair(*v, cf, sf)):
                        psi[k, a, c, *tile_of(p)] = value
                return carry

            lax.fori_loop(0, DEVICES * spots, chunk_bits, 0)

            def top_bits(n, carry):
                c, p = quot(n, spots), rest(n, spots)
                for k in BOTH:
                    v = [psi[k, a, c, *tile_of(p)] for a in range(8)]
                    v = rotate_pair(*v[:4], cf, sf) + rotate_pair(*v[4:], cf, sf)
                    for a in range(4):
                        psi[k, a, c, *tile_of(p)] = ch * v[a] - sh * v[a + 4]
                        psi[k, a + 4, c, *tile_of(p)] = sh * v[a] + ch * v[a + 4]
                return carry

            lax.fori_loop(0, CHUNKS * spots, top_bits, 0)

        def add(n, acc):
            a, r, spot, _ = part_of(n)
            vr, vi = psi[0, *spot], psi[1, *spot]
            return acc + (cost[a, r] * (vr * vr + vi * vi)).reshape(PART // 8, 8, LANES).sum(axis=0)

        total = jnp.sum(lax.fori_loop(0, DEVICES * parts, add, jnp.zeros((8, LANES), jnp.float32)))
        def turn(p, carry):
            _, r, spot, k = part_of((qx * 2 + qy) * parts + p)
            vr, vi, ta, tb = psi[0, *spot], psi[1, *spot], tab_a[k], tab_b[k]
            state[0, r] = ta * vr + tb * vi
            state[1, r] = ta * vi - tb * vr
            return carry

        lax.fori_loop(0, parts, turn, 0)
        finish(run(put_all((state.at[0], state.at[1])) + [put_energy(total)]))


def simulate(cost_rows, gammas, betas):
    rows = cost_rows.shape[0]
    f32 = jnp.float32
    state = jax.ShapeDtypeStruct((rows, LANES), f32)
    near = pl.BlockSpec(memory_space=pl.ANY)
    dma = pltpu.SemaphoreType.DMA
    full = pltpu.VMEM((2, rows, LANES), f32)
    blocks = pltpu.VMEM((2, 4, rows, LANES), f32)
    table = pltpu.VMEM((4, PART, LANES), f32)
    two, four = dma((2,)), dma((CHUNKS,))
    tiles = pltpu.VMEM((DEVICES + 2, 2, LANES), f32)
    halves = pltpu.VMEM((2, 2, CHUNKS, 2 * LANES, LANES), f32)

    def square(*lead):
        return pltpu.VMEM(lead + (2 * LANES, 2 * LANES), f32)

    s_re, s_im, costs, sums = pl.pallas_call(
        gather_kernel,
        out_shape=(state, state, jax.ShapeDtypeStruct((4, 2, rows, LANES), f32),
                   jax.ShapeDtypeStruct((DEVICES + 2, 2, LANES), f32)),
        in_specs=[near] * 2,
        out_specs=(near,) * 4,
        scratch_shapes=[
            pltpu.VMEM((4, 2, rows, LANES), f32), square(2, 4, CHUNKS), blocks,
            halves, square(2, CHUNKS), halves, full, square(), square(),
            table, table, table, table, pltpu.VMEM((8, LANES), f32), pltpu.VMEM((3, 2, LANES), f32), pltpu.SMEM((4,), f32),
            dma, two, dma, dma, dma, dma, dma, dma, four, four, four, four, dma((4, CHUNKS)),
            dma, two, dma, dma, two, dma],
        compiler_params=pltpu.CompilerParams(collective_id=0, has_side_effects=True,
                                             vmem_limit_bytes=52736 << 10),
    )(cost_rows, jnp.concatenate([gammas, betas]))
    return pl.pallas_call(
        final_kernel,
        out_shape=(state, state, jax.ShapeDtypeStruct((1,), f32)),
        in_specs=[near] * 4,
        out_specs=(near,) * 3,
        scratch_shapes=[
            full, pltpu.VMEM((8, rows, LANES), f32), square(2, 8, CHUNKS), square(), table, table,
            tiles, pltpu.SMEM((1,), f32), two, dma((DEVICES,)), two],
        compiler_params=pltpu.CompilerParams(vmem_limit_bytes=52224 << 10),
    )(s_re, s_im, costs, sums)


def popcount(values, bits):
    return sum((values >> b) & 1 for b in range(bits))


def solution(mesh):
    state_spec = P(('inst', 'qx', 'qy'))

    def device_body(cost_local, gammas, betas):
        local_len = cost_local.shape[0]
        s_re, s_im, energy = simulate(cost_local.reshape(local_len // LANES, LANES), gammas, betas)
        return energy, s_re.reshape(local_len), s_im.reshape(local_len)

    return jax.shard_map(device_body, mesh=mesh, in_specs=(state_spec, P(), P()),
                         out_specs=(P('inst'), state_spec, state_spec), check_vma=False)
```

```python
import math
import jax
import jax.numpy as jnp
import numpy as np
from jax import lax
from jax.experimental import pallas as pl
from jax.experimental.pallas import tpu as pltpu
from jax.sharding import PartitionSpec as P

LANES = 128
MESH = pl.DeviceIdType.MESH
HIGHEST = lax.Precision.HIGHEST
ANGLE_MAX = 131072.0
INV_TURN = float(np.float32(1.0 / (2.0 * math.pi)))
TURN_HI = 6.28125
TURN_LO = float(np.float32(2.0 * math.pi - 6.28125))
CHUNKS = 4
BOTH = range(2)
DEVICES = 8
PART = 64

SIN_COEFS = [2 * v / 4.0 ** (2 * k + 1) for k, v in enumerate(
    [1.0, -1.6666654611e-1, 8.3321608736e-3, -1.9515295891e-4])]
COS_COEFS = [2 * v / 16.0 ** k for k, v in enumerate(
    [1.0, -0.5, 4.166664568298827e-2, -1.388731625493765e-3, 2.443315711809948e-5])]


def horner(coefs, z):
    acc = coefs[-1] * z + coefs[-2]
    for v in coefs[-3::-1]:
        acc = acc * z + v
    return acc


def double_phase(cost, gamma, scale, quarter=None, offset=None):
    angle = gamma * cost
    turns = angle * INV_TURN
    if quarter is not None:
        turns = turns - quarter
    n = lax.round(turns, lax.RoundingMethod.TO_NEAREST_EVEN)
    r = (n * TURN_HI - angle) + n * TURN_LO
    if offset is not None:
        r = r + offset
    z = r * r
    s = r * horner(SIN_COEFS, z)
    s2 = s * horner(COS_COEFS, z)
    t2 = scale * s2
    return (scale + scale) - t2 * s2, t2 * (2.0 - s * s)


def rotate_pair(x00, x01, x10, x11, cos_full, sin_full):
    u, v = x00 - x11, x00 + x11
    w, y = x01 + x10, x01 - x10
    u, w = cos_full * u - sin_full * w, sin_full * u + cos_full * w
    return v + u, w + y, w - y, v - u


def quot(a, b):
    return a // b if isinstance(a, int) else lax.div(a, jnp.int32(b))


def rest(a, b):
    return a % b if isinstance(a, int) else lax.rem(a, jnp.int32(b))


def popcount_small(k, bits):
    return sum(rest(quot(k, 1 << b), 2) for b in range(bits))


def rotation_power(cos_half, sin_half, bits, scale):
    n = 1 << bits
    row = lax.broadcasted_iota(jnp.int32, (n, n), 0)
    col = lax.broadcasted_iota(jnp.int32, (n, n), 1)
    acc = jnp.full((n, n), scale, jnp.float32)
    for b in range(bits):
        rb, cb = (row >> b) & 1, (col >> b) & 1
        acc = acc * jnp.where(rb == cb, cos_half, jnp.where(rb > cb, sin_half, -sin_half))
    return acc


def row_gates(arr, cos_half, signed, cos_full, sin_full):
    sub = lax.broadcasted_iota(jnp.int32, arr.shape, 1)
    for b in range(3):
        arr = cos_half * arr + signed[b] * jnp.take_along_axis(arr, sub ^ (1 << b), axis=1)
    v = [arr[k] for k in range(32)]
    for q in (1, 4):
        for k in range(32):
            if (k // q) % 4 == 0:
                quad = (k, k + q, k + 2 * q, k + 3 * q)
                for d, value in zip(quad, rotate_pair(*[v[d] for d in quad], cos_full, sin_full)):
                    v[d] = value
    for k in range(16):
        lo, hi = v[k], v[k + 16]
        v[k], v[k + 16] = cos_half * lo - signed[3] * hi, signed[3] * lo + cos_half * hi
    return v


def loop(start, stop, body, carry, steps=1):
    def turn(n, value):
        for k in range(steps):
            value = body(n * steps + k, value)
        return value
    return lax.fori_loop(start // steps, stop // steps, turn, carry)


def half_lanes(h):
    return pl.ds(pl.multiple_of(h * LANES, LANES), LANES)


def run_rows(ref, h, consts, value=None):
    rows = ref.shape[0]
    value = ref[:, half_lanes(h)] if value is None else value
    v = row_gates(value.reshape(rows // 8, 8, LANES), *consts)
    for k in range(rows // 8):
        ref[pl.ds(8 * k, 8), half_lanes(h)] = v[k]


def run_lanes(ref, w):
    if len(ref.shape) == 2:
        halves = [ref.at[pl.ds(k * LANES, LANES)] for k in BOTH]
    else:
        halves = [ref.at[k] for k in BOTH]
    values = [half[...].reshape(-1, ref.shape[-1]) for half in halves]
    values = [jnp.dot(v, w[...], precision=HIGHEST, preferred_element_type=jnp.float32) for v in values]
    for half, v in zip(halves, values):
        half[...] = v.reshape(half.shape)


def cos_sin(v):
    v = jnp.full((8, LANES), v)
    return jnp.cos(v), jnp.sin(v)


def signed_sines(sin_half):
    sub = lax.broadcasted_iota(jnp.int32, (8, LANES), 0)
    return [jnp.where((sub & (1 << b)) == 0, -sin_half, sin_half) for b in range(3)] + [sin_half]


def quarter_tables(tab_a, tab_b):
    low = (lax.broadcasted_iota(jnp.int32, (PART, LANES), 0) * LANES
           + lax.broadcasted_iota(jnp.int32, (PART, LANES), 1))
    pop = popcount(low, 13)
    for k in range(4):
        q = (pop + k) & 3
        tab_a[k] = jnp.where(q == 0, 1.0, jnp.where(q == 2, -1.0, 0.0))
        tab_b[k] = jnp.where(q == 1, 1.0, jnp.where(q == 3, -1.0, 0.0))
    return pop


def gather_kernel(c_hbm, angles_any, out_re, out_im, out_cost, out_sums,
                  cost, psi, trig, wave, mixed, part, final, w1, w2,
                  tab_q, tab_o, tab_a, tab_b, cmax, mine, angles,
                  own_sem, out_sem, keep_sem, sx, sy, srx, sry, sc, rx, ry, rdx, rdy, rc, swave, rwave, se, re_sem, sums_sem, angle_sem):
    qx, qy = lax.axis_index("qx"), lax.axis_index("qy")
    x, core = quot(qx, 2), rest(qx, 2)
    rows = c_hbm.shape[0]
    chunk = rows // CHUNKS
    half = chunk // 2

    def dev(dx, dy, dc):
        return {"qx": lax.rem(x + dx, 2) * 2 + lax.rem(core + dc, 2), "qy": lax.rem(qy + dy, 2)}

    xn, yn, cn = dev(1, 0, 0), dev(0, 1, 0), dev(0, 0, 1)

    own_copy = pltpu.make_async_copy(c_hbm, cost.at[0, 0], own_sem)
    own_copy.start()
    angle_copy = pltpu.make_async_copy(angles_any, angles, angle_sem)
    angle_copy.start()
    barrier = pltpu.get_barrier_semaphore()
    for neighbour in (xn, yn, cn):
        pl.semaphore_signal(barrier, inc=1, device_id=neighbour, device_id_type=MESH)

    tile = (8, LANES)
    three = (PART // 8, 8, LANES)
    pl.semaphore_wait(barrier, 3)

    def remote(src, dst, ssem, rsem, device):
        return pltpu.make_async_remote_copy(src_ref=src, dst_ref=dst, send_sem=ssem, recv_sem=rsem,
                                            device_id=device, device_id_type=MESH)

    def rows_of(c):
        return pl.ds(c * chunk, chunk)

    def span(c, h):
        return pl.ds(c * chunk + h * half, half)

    def to_x(c):
        return remote(c_hbm.at[rows_of(c)], cost.at[1, 0, rows_of(c)], sx, rx.at[c], xn)

    def to_y(c):
        return remote(c_hbm.at[rows_of(c)], cost.at[2, 0, rows_of(c)], sy, ry.at[c], yn)

    def relay_y(c):
        return remote(cost.at[1, 0, span(c, 0)], cost.at[3, 0, span(c, 0)], sry, rdy.at[c], yn)

    def relay_x(c):
        return remote(cost.at[2, 0, span(c, 1)], cost.at[3, 0, span(c, 1)], srx, rdx.at[c], xn)

    def to_core(i, c):
        return remote(cost.at[i, 0, rows_of(c)], cost.at[i, 1, rows_of(c)], sc, rc.at[i, c], cn)

    def keep(i, k, c):
        return pltpu.make_async_copy(cost.at[i, k, rows_of(c)], out_cost.at[i, k, rows_of(c)], keep_sem)

    for c in range(CHUNKS):
        to_x(c).start()
        to_y(c).start()
    own_copy.wait()
    for c in range(CHUNKS):
        to_core(0, c).start()

    angle_copy.wait()
    g1, g2, beta1, beta2 = [angles[k] for k in range(4)]
    for k, v in enumerate(((g1, g2), (beta1, beta2))):
        mine[k + 1] = jnp.concatenate([jnp.full((1, LANES), u) for u in v], axis=0)
    keep_angles = pltpu.make_async_copy(mine.at[pl.ds(1, 2)], out_sums.at[pl.ds(DEVICES, 2)], sums_sem.at[1])
    keep_angles.start()
    ch1, sh1 = cos_sin(0.5 * beta1)
    ch2, sh2 = cos_sin(0.5 * beta2)
    cf1, sf1 = cos_sin(beta1)
    cf2, sf2 = cos_sin(beta2)
    pop = quarter_tables(tab_a, tab_b)
    for k in range(4):
        q = ((pop + k) & 3).astype(jnp.float32)
        tab_q[k] = 0.25 * q
        tab_o[k] = q * float(np.float32(0.5 * math.pi))
    signed1, signed2 = signed_sines(sh1), signed_sines(sh2)

    w1[...] = rotation_power(ch1[0:1, 0:1], -sh1[0:1, 0:1], 8, 2.0 ** -6)
    w2[...] = rotation_power(ch2[0:1, 0:1], -sh2[0:1, 0:1], 8, 2.0 ** -3)
    cmax[...] = jnp.zeros(tile, jnp.float32)

    xf, yf, kf = x.astype(jnp.float32), qy.astype(jnp.float32), core.astype(jnp.float32)
    sign_x, sign_y, sign_k = 2.0 * xf - 1.0, 2.0 * yf - 1.0, 2.0 * kf - 1.0
    flip = sign_x * sign_y
    sx1 = -sign_x * sf1
    sx2, sy2 = sign_x * sh2, sign_y * sh2
    contract = [ch2 * ch2, sx2 * ch2, flip * (ch2 * sy2), flip * (sx2 * sy2)]
    spread = [1.0, 1.0, flip, flip]

    consts1 = (ch1, signed1, cf1, sf1)
    consts2 = (ch2, signed2, cf2, sf2)

    def phases(i, c, own=True, other=True):
        base = c % 2 + c // 2 + (x if i % 2 == 0 else 1 - x) + (qy if i < 2 else 1 - qy)
        ca, cb = spread[i] * ch1, spread[i] * sign_k * sh1
        def body(n, carry):
            r = pl.ds(pl.multiple_of(c * chunk + n * PART, PART), PART)
            spot = (pl.ds(pl.multiple_of(rest(n, 4) * PART, PART), PART), half_lanes(quot(n, 4)))
            terms = []
            for flag, side, coef in ((own, 0, ca), (other, 1, cb)):
                if flag:
                    q = lax.rem(base + popcount_small(n, 3) + (core if side == 0 else 1 - core), 4)
                    terms.append(double_phase(cost[i, side, r].reshape(three), g1, coef,
                                              tab_q[q].reshape(three), tab_o[q].reshape(three)))
            if not own:
                terms.append([psi[k, i, c, *spot].reshape(three) for k in BOTH])
            for k in BOTH:
                u = terms[0][k] if len(terms) == 1 else terms[0][k] + terms[1][k]
                psi[k, i, c, *spot] = u.reshape(PART, LANES)
            if own:
                v = cost[i, 0, r].reshape(three)
                for k, u in enumerate(double_phase(v, g2, contract[i])):
                    trig[k, i, r] = u.reshape(PART, LANES)
                if i == 0:
                    cmax[...] = jnp.maximum(cmax[...], jnp.abs(v).max(axis=0))
            return carry

        loop(0, chunk // PART, body, 0, 4)

    def rows_loop(i, c):
        def body(n, carry):
            run_rows(psi.at[quot(n, 2), i, c], rest(n, 2), consts1)
            return carry
        lax.fori_loop(0, 4, body, 0)

    def place(p):
        return pl.ds(pl.multiple_of(rest(p, half // 8) * 8, 8), 8), half_lanes(quot(p, half // 8))

    def chunk_bits(p, carry, blocks=(1, 2)):
        for k in BOTH:
            for i in blocks:
                v = rotate_pair(*[psi[k, i, c, *place(p)] for c in range(CHUNKS)], cf1, sf1)
                for c in range(CHUNKS):
                    psi[k, i, c, *place(p)] = v[c]
        return carry

    def arrived(i, c):
        if i == 1 or i == 2:
            (to_x if i == 1 else to_y)(c).wait_recv()
            (relay_y if i == 1 else relay_x)(c).start()
        if i == 3:
            relay_y(c).wait_recv()
            relay_x(c).wait_recv()
        if i > 0:
            to_core(i, c).start()
        keep(i, 0, c).start()

    def other_arrived(i, c):
        to_core(i, c).wait_recv()
        keep(i, 1, c).start()

    def unit(i, c):
        other_arrived(i, c)
        phases(i, c)
        rows_loop(i, c)

    for c in range(CHUNKS):
        arrived(0, c)
        unit(0, c)
        if c % 2 == 1:
            run_lanes(psi.at[:, 0, pl.ds(c - 1, 2)], w1)
    for c in range(CHUNKS):
        for i in (1, 2):
            arrived(i, c)
        for i in (1, 2):
            unit(i, c)
        if c == CHUNKS - 1:
            arrived(3, 0)
        run_lanes(psi.at[:, pl.ds(1, 2), c], w1)
        if c == 0:
            loop(0, chunk // 8, lambda p, v: chunk_bits(p, v, (0,)), 0, 4)
    loop(0, chunk // 8, chunk_bits, 0, 4)
    arrived(3, 1)
    unit(3, 0)
    unit(3, 1)
    arrived(3, 2)
    run_lanes(psi.at[:, 3, pl.ds(0, 2)], w1)
    unit(3, 2)
    arrived(3, 3)
    run_lanes(psi.at[:, 3, 2], w1)
    phases(3, 3, other=False)
    other_arrived(3, 3)
    phases(3, 3, own=False)
    for k in BOTH:
        for h in BOTH:
            run_rows(psi.at[k, 3, 3], h, consts1)
    run_lanes(psi.at[:, 3, 3], w1)

    def tail(p, carry):
        r = [pl.ds(pl.multiple_of(c * chunk + p * 8, 8), 8) for c in range(CHUNKS)]
        diag = [rotate_pair(*[psi[k, 3, c, *place(p)] for c in range(CHUNKS)], cf1, sf1) for k in BOTH]
        z = [[], []]
        for c in range(CHUNKS):
            v = [rotate_pair(*[psi[k, i, c, *place(p)] for i in (0, 2, 1)], diag[k][c], cf1, sx1) for k in BOTH]
            sums = None
            for n, i in enumerate((0, 2, 1, 3)):
                (re, im), (tr, ti) = (v[0][n], v[1][n]), (trig[0, i, r[c]], trig[1, i, r[c]])
                term = (re * tr - im * ti, re * ti + im * tr)
                sums = term if sums is None else (sums[0] + term[0], sums[1] + term[1])
            z[0].append(sums[0])
            z[1].append(sums[1])
        for k in BOTH:
            for c, value in enumerate(rotate_pair(*z[k], cf2, sf2)):
                wave[quot(p, half // 8), k, c, place(p)[0]] = value
        return carry

    def swap(n):
        spot = (quot(n, 8), slice(None), slice(None), pl.ds(pl.multiple_of(rest(n, 8) * 32, 32), 32))
        return remote(wave.at[*spot], part.at[*spot], swave, rwave.at[quot(n, 8)], cn)

    def piece(n, carry):
        for k in range(4):
            tail(4 * n + k, carry)
        swap(n).start()
        return carry

    lax.fori_loop(0, 2 * DEVICES, piece, 0)

    sk2 = sign_k * sh2
    for h in BOTH:
        remote(wave.at[h], part.at[h], swave, rwave.at[h], cn).wait_recv()

        def turn(n, carry, h=h):
            k, c = quot(n, CHUNKS), rest(n, CHUNKS)
            shape = (half // 8, 8, LANES)
            run_rows(mixed.at[k, c], h, consts2, ch2 * wave[h, k, c].reshape(shape) + sk2 * part[h, k, c].reshape(shape))
            return carry

        loop(0, 2 * CHUNKS, turn, 0, 2)

    energy = jnp.zeros(tile, jnp.float32)
    for c in range(CHUNKS):
        if c == 0:
            run_lanes(mixed, w2)

        def last(p, acc, c=c):
            r = pl.ds(pl.multiple_of(c * chunk + p * PART, PART), PART)
            spot = (pl.ds(pl.multiple_of(rest(p, 4) * PART, PART), PART), half_lanes(quot(p, 4)))
            vr, vi = [mixed[k, c, *spot] for k in BOTH]
            k = lax.rem(popcount_small(p, 3) + c % 2 + c // 2 + x + qy + core, 4)
            final[0, r] = tab_a[k] * vr + tab_b[k] * vi
            final[1, r] = tab_a[k] * vi - tab_b[k] * vr
            return acc + (cost[0, 0, r] * (vr * vr + vi * vi)).reshape(three).sum(axis=0)

        energy = loop(0, chunk // PART, last, energy, 4)
        for k, out in enumerate((out_re, out_im)):
            pltpu.make_async_copy(final.at[k, rows_of(c)], out.at[rows_of(c)], out_sem.at[k]).start()

    me = qy * 4 + qx
    largest = cmax[...].max(axis=0, keepdims=True) * jnp.maximum(jnp.abs(g1), jnp.abs(g2))
    mine[0] = jnp.concatenate([energy.sum(axis=0, keepdims=True), largest], axis=0)
    sends = [remote(mine.at[0], out_sums.at[me], se, re_sem, dev(n // 4, (n // 2) % 2, n % 2))
             for n in range(1, DEVICES)]
    for cp in sends:
        cp.start()
    keep_mine = pltpu.make_async_copy(mine.at[0], out_sums.at[me], sums_sem.at[0])
    keep_mine.start()
    outs = [keep_mine, keep_angles, pltpu.make_async_copy(cost, out_cost, keep_sem)]
    outs += [pltpu.make_async_copy(final.at[k], out, out_sem.at[k]) for k, out in enumerate((out_re, out_im))]
    spot, others = pl.ds(0, rows // 2), out_sums.at[pl.ds(0, DEVICES - 1)]
    for src, dst, sem in ((c_hbm, cost.at[1, 0], sx), (c_hbm, cost.at[2, 0], sy),
                          (cost.at[1, 0, spot], cost.at[3, 0, spot], sry),
                          (cost.at[2, 0, spot], cost.at[3, 0, spot], srx),
                          (cost.at[:, 0], cost.at[:, 1], sc), (wave, part, swave)):
        remote(src, dst, sem, re_sem, cn).wait_send()
    for cp in outs:
        cp.wait()
    remote(others, others, se, re_sem, cn).wait()


def final_kernel(in_re, in_im, in_cost, in_sums, out_re, out_im, out_energy,
                 state, cost, psi, w, tab_a, tab_b, sums, energy, out_sem, cost_sem, small_sem):
    rows = in_re.shape[0]
    chunk = rows // CHUNKS
    parts, spots = rows // PART, chunk // 8
    outs = (out_re, out_im)

    def put_all(srcs):
        return [pltpu.make_async_copy(srcs[k], outs[k], out_sem.at[k]) for k in BOTH]

    def put_energy(total):
        energy[0] = total * (1.0 / (DEVICES * rows * LANES))
        return pltpu.make_async_copy(energy, out_energy, small_sem.at[1])

    def run(copies):
        for cp in copies:
            cp.start()
        return copies

    def finish(copies):
        for cp in copies:
            cp.wait()

    moves = run(put_all((in_re, in_im)))
    finish(run([pltpu.make_async_copy(in_sums, sums, small_sem.at[0])]))
    both = [sums[n] for n in range(DEVICES)]
    total = sum(v[:1] for v in both[1:]) + both[0][:1]
    moves += run([put_energy(jnp.sum(total))])
    small = jnp.max(jnp.stack(both)[:, 1:]) <= ANGLE_MAX
    finish(moves)

    @pl.when(jnp.logical_not(small))
    def _():
        qx, qy = lax.axis_index("qx"), lax.axis_index("qy")
        fetch = []
        for a in range(DEVICES):
            i = lax.rem(a // 4 + qx // 2, 2) + 2 * lax.rem(a % 2 + qy, 2)
            fetch.append(pltpu.make_async_copy(in_cost.at[i, lax.rem(a // 2 + qx, 2)], cost.at[a], cost_sem.at[a]))
        run(fetch)
        quarter_tables(tab_a, tab_b)
        finish(fetch)

        def part_of(n):
            a, p = quot(n, parts), rest(n, parts)
            c, q = quot(p, chunk // PART), rest(p, chunk // PART)
            spot = (a, c, pl.ds(pl.multiple_of(rest(q, 4) * PART, PART), PART), half_lanes(quot(q, 4)))
            k = lax.rem(popcount_small(p, 5) + popcount_small(a, 3), 4)
            return a, pl.ds(pl.multiple_of(p * PART, PART), PART), spot, k

        def tile_of(p):
            return pl.ds(pl.multiple_of(rest(p, spots // 2) * 8, 8), 8), half_lanes(quot(p, spots // 2))

        for layer in BOTH:
            gamma, beta = [jnp.max(sums[DEVICES + k][layer:layer + 1]) for k in BOTH]
            ch, sh = cos_sin(0.5 * beta)
            cf, sf = cos_sin(beta)

            def phase(n, carry):
                a, r, spot, k = part_of(n)
                t = gamma * cost[a, r]
                vr, vi = jnp.cos(t), -jnp.sin(t)
                qr, qi = (tab_a[k], tab_b[k]) if layer == 0 else (psi[0, *spot], psi[1, *spot])
                psi[0, *spot] = vr * qr - vi * qi
                psi[1, *spot] = vr * qi + vi * qr
                return carry

            lax.fori_loop(0, DEVICES * parts, phase, 0)
            w[...] = rotation_power(ch[0:1, 0:1], -sh[0:1, 0:1], 8, 2.0 ** -4)
            consts = (ch, signed_sines(sh), cf, sf)

            def within(n, carry):
                ref = psi.at[rest(n, 2), quot(n, 2 * CHUNKS), rest(quot(n, 2), CHUNKS)]
                for h in BOTH:
                    run_rows(ref, h, consts)
                run_lanes(ref, w)
                return carry

            lax.fori_loop(0, 16 * CHUNKS, within, 0)

            def chunk_bits(n, carry):
                a, p = quot(n, spots), rest(n, spots)
                for k in BOTH:
                    v = [psi[k, a, c, *tile_of(p)] for c in range(CHUNKS)]
                    for c, value in enumerate(rotate_pair(*v, cf, sf)):
                        psi[k, a, c, *tile_of(p)] = value
                return carry

            lax.fori_loop(0, DEVICES * spots, chunk_bits, 0)

            def top_bits(n, carry):
                c, p = quot(n, spots), rest(n, spots)
                for k in BOTH:
                    v = [psi[k, a, c, *tile_of(p)] for a in range(8)]
                    v = rotate_pair(*v[:4], cf, sf) + rotate_pair(*v[4:], cf, sf)
                    for a in range(4):
                        psi[k, a, c, *tile_of(p)] = ch * v[a] - sh * v[a + 4]
                        psi[k, a + 4, c, *tile_of(p)] = sh * v[a] + ch * v[a + 4]
                return carry

            lax.fori_loop(0, CHUNKS * spots, top_bits, 0)

        def add(n, acc):
            a, r, spot, _ = part_of(n)
            vr, vi = psi[0, *spot], psi[1, *spot]
            return acc + (cost[a, r] * (vr * vr + vi * vi)).reshape(PART // 8, 8, LANES).sum(axis=0)

        total = jnp.sum(lax.fori_loop(0, DEVICES * parts, add, jnp.zeros((8, LANES), jnp.float32)))
        def turn(p, carry):
            _, r, spot, k = part_of((qx * 2 + qy) * parts + p)
            vr, vi, ta, tb = psi[0, *spot], psi[1, *spot], tab_a[k], tab_b[k]
            state[0, r] = ta * vr + tb * vi
            state[1, r] = ta * vi - tb * vr
            return carry

        lax.fori_loop(0, parts, turn, 0)
        finish(run(put_all((state.at[0], state.at[1])) + [put_energy(total)]))


def simulate(cost_rows, gammas, betas):
    rows = cost_rows.shape[0]
    f32 = jnp.float32
    state = jax.ShapeDtypeStruct((rows, LANES), f32)
    near = pl.BlockSpec(memory_space=pl.ANY)
    dma = pltpu.SemaphoreType.DMA
    full = pltpu.VMEM((2, rows, LANES), f32)
    blocks = pltpu.VMEM((2, 4, rows, LANES), f32)
    table = pltpu.VMEM((4, PART, LANES), f32)
    two, four = dma((2,)), dma((CHUNKS,))
    tiles = pltpu.VMEM((DEVICES + 2, 2, LANES), f32)
    halves = pltpu.VMEM((2, 2, CHUNKS, 2 * LANES, LANES), f32)

    def square(*lead):
        return pltpu.VMEM(lead + (2 * LANES, 2 * LANES), f32)

    s_re, s_im, costs, sums = pl.pallas_call(
        gather_kernel,
        out_shape=(state, state, jax.ShapeDtypeStruct((4, 2, rows, LANES), f32),
                   jax.ShapeDtypeStruct((DEVICES + 2, 2, LANES), f32)),
        in_specs=[near] * 2,
        out_specs=(near,) * 4,
        scratch_shapes=[
            pltpu.VMEM((4, 2, rows, LANES), f32), square(2, 4, CHUNKS), blocks,
            halves, square(2, CHUNKS), halves, full, square(), square(),
            table, table, table, table, pltpu.VMEM((8, LANES), f32), pltpu.VMEM((3, 2, LANES), f32), pltpu.SMEM((4,), f32),
            dma, two, dma, dma, dma, dma, dma, dma, four, four, four, four, dma((4, CHUNKS)),
            dma, two, dma, dma, two, dma],
        compiler_params=pltpu.CompilerParams(collective_id=0, has_side_effects=True,
                                             vmem_limit_bytes=52736 << 10),
    )(cost_rows, jnp.concatenate([gammas, betas]))
    return pl.pallas_call(
        final_kernel,
        out_shape=(state, state, jax.ShapeDtypeStruct((1,), f32)),
        in_specs=[near] * 4,
        out_specs=(near,) * 3,
        scratch_shapes=[
            full, pltpu.VMEM((8, rows, LANES), f32), square(2, 8, CHUNKS), square(), table, table,
            tiles, pltpu.SMEM((1,), f32), two, dma((DEVICES,)), two],
        compiler_params=pltpu.CompilerParams(vmem_limit_bytes=52224 << 10),
    )(s_re, s_im, costs, sums)


def popcount(values, bits):
    return sum((values >> b) & 1 for b in range(bits))


def solution(mesh):
    state_spec = P(('inst', 'qx', 'qy'))

    def device_body(cost_local, gammas, betas):
        local_len = cost_local.shape[0]
        s_re, s_im, energy = simulate(cost_local.reshape(local_len // LANES, LANES), gammas, betas)
        return energy, s_re.reshape(local_len), s_im.reshape(local_len)

    return jax.shard_map(device_body, mesh=mesh, in_specs=(state_spec, P(), P()),
                         out_specs=(P('inst'), state_spec, state_spec), check_vma=False)
```
